32 devices in a mesh: groups: 2 (over x), expert: 16 (over z, y, core).
Axes of the slice: x: 2, y: 2, z: 4, core: 2. Of those that a mesh axis runs over, the one named last changes fastest.
Arguments:
- tokens: bfloat16 [4096, 7168], P(('groups', 'expert')), parts along dimension 0, may hold values from -6 to 6
- route_ids: int32 [4096, 2], P(('groups', 'expert')), parts along dimension 0, may hold values from 0 to 3, all different within a row; in each aligned block of 128 rows (0 to 127, 128 to 255, ...) at most 80 rows name the same one
- levels: int32 [4096, 2], P(('groups', 'expert')), parts along dimension 0, may hold values from 1 to 64
- w_gate: bfloat16 [16, 7168, 512], P('expert'), may hold values from -0.0625 to 0.0625
- w_up: bfloat16 [16, 7168, 512], P('expert'), may hold values from -0.0625 to 0.0625
- w_down: bfloat16 [16, 512, 7168], P('expert'), may hold values from -0.125 to 0.125
Outputs:
- combined: bfloat16 [4096, 7168], P(('groups', 'expert')), parts along dimension 0
The draws below stay inside these ranges and needn't reach their ends.
There are 2 independent parts, one for each index of `groups`. The reference program is written for one: setup_inputs(seed, part) draws one part's arguments, and reference() takes and returns one part's arrays. A program takes and returns all parts, laid end to end along the dimension named above; an argument that names none is the same for every part. Nothing has to cross between parts.
Inputs may be any that keep to these rules, and one draw needn't show every extreme that they name: `route_ids`: each row names 2 different experts; among the rows of one device no expert is named more than 80 times, a bound that some block reaches.
All inputs are finite; a program needn't handle non-finite values.
Results may differ from the reference program's by a relative error of at most 0.013.
Values may be sent and summed in bfloat16 or wider, within the bound.
A program may use at most 192 MiB of HBM per device.

```python
import math
import jax
import jax.numpy as jnp
import numpy as np
from jax import lax

D = 7168
FF_WIN = 2048
SHARDS = 4
FF_DEV = 512
TOK_DEV = 128
TOP = 2
EXPERTS = 4
CAP = 80
TOKENS = 2048
N_EXPERT = 16


def set_ends(values, rng, smallest, high):
    spot = [jax.random.randint(jax.random.fold_in(rng, axis), (), 0, length) for axis, length in enumerate(values.shape)]
    longest = values.shape.index(max(values.shape))
    neighbour = spot[:longest] + [(spot[longest] + 1) % values.shape[longest]] + spot[longest + 1:]
    return values.at[tuple(spot)].set(smallest).at[tuple(neighbour)].set(high)


def steps_of(own_key, extent, split, low, high):
    level, own = 1.0, jax.random.fold_in(own_key, 6)
    for position, shards_of in split:
        heights = jnp.exp(jax.random.uniform(jax.random.fold_in(own, position), (shards_of,), jnp.float32, low / len(split), high / len(split)))
        level = level * jnp.repeat(heights, extent[position] // shards_of).reshape([-1 if axis == position else 1 for axis in range(len(extent))])
    return level


def shared_out(key, own, number, rows, count, top, limit, slope):
    sequence = jax.random.permutation(key, count)
    packed, usual = portions_of(count, rows * top, limit, slope, True), portions_of(count, rows * top, limit, slope, False)
    places = jnp.arange(count)

    def named(tallies, offset_by):
        used = int((tallies > 0).sum())
        fixed = max(1, used // 4)
        shifted = fixed + (places - fixed + offset_by * (used - fixed)) % max(1, count - fixed)
        return jnp.zeros((count,), jnp.int32).at[sequence[jnp.where(places < fixed, places, shifted)]].set(jnp.asarray(tallies, jnp.int32))

    tallies = jnp.where(number % 4 == 0, named(packed, number // 4), named(usual, number - number // 4 - 1))
    mixed = jax.random.permutation(jax.random.fold_in(own, 3), count)
    donor, sink = mixed[0:count // 2 * 2:2], mixed[1:count // 2 * 2:2]
    margin = jnp.minimum(tallies[donor] - 1, limit - tallies[sink]) // 2
    margin = jnp.where((donor == sequence[0]) | (sink == sequence[0]) | (tallies[sink] == 0), 0, jnp.maximum(margin, 0))
    shifted = jax.random.randint(jax.random.fold_in(own, 4), (count // 2,), 0, 1 << 20) % (margin + 1)
    tallies = tallies.at[donor].add(-shifted).at[sink].add(shifted)
    members = jnp.searchsorted(jnp.cumsum(tallies), jnp.arange(rows * top), side="right").astype(jnp.int32)
    table = members.reshape(top, rows).T
    table = table[jax.random.permutation(jax.random.fold_in(own, 1), rows)]
    offset_by = jax.random.randint(jax.random.fold_in(own, 2), (rows, 1), 0, top)
    return jnp.take_along_axis(table, (jnp.arange(top)[None, :] + offset_by) % top, axis=1)


def portions_of(number_of, total, limit, slope, full):
    weights = [(1 << 20) // math.isqrt(grade ** slope) + 1 for grade in range(1, number_of + 1)]
    largest = limit if full else min(limit, max(-(-total // number_of), total * weights[0] // sum(weights)))
    least = 1 if total - largest >= number_of - 1 else 0
    given, spare = [largest] + [least] * (number_of - 1), total - largest - least * (number_of - 1)
    while spare > 0:
        candidates = [i for i in range(1, number_of) if given[i] < largest] or [i for i in range(1, number_of) if given[i] < limit]
        whole, budget = sum([weights[i] for i in candidates]), spare
        for i in candidates:
            addition = min(limit - given[i], max(1, budget * weights[i] // whole), spare)
            given[i] = given[i] + addition
            spare = spare - addition
    return np.array(given)


def bell_draw(rng, extent, scale, limit, cuts=(), held_as=jnp.bfloat16):
    values = jax.random.normal(rng, extent, jnp.float32) * scale
    if len(cuts) > 0:
        values = steps_of(rng, extent, cuts, -0.22, 0.18) * values
    return jnp.clip(values, min=-limit, max=limit).astype(held_as)


def setup_inputs(seed: int = 0, part: int = 0) -> dict:
    keys = jax.random.split(jax.random.key(seed), 7)
    own_keys = jax.random.split(jax.random.fold_in(keys[6], part), 7)
    tokens = bell_draw(own_keys[0], (TOKENS, D), 1.0, 6.0, ((0, 16),))
    route_ids_keys = jax.random.split(jax.random.fold_in(own_keys[1], 1), TOKENS // TOK_DEV)
    route_ids_turns = jax.random.permutation(jax.random.fold_in(own_keys[1], 3), TOKENS // TOK_DEV)
    route_ids = jax.vmap(lambda own, number: shared_out(jax.random.fold_in(own_keys[1], 2), own, number, TOK_DEV, EXPERTS, TOP, CAP, 2))(route_ids_keys, route_ids_turns).reshape((TOKENS, TOP))
    levels = set_ends(jax.random.randint(own_keys[2], (TOKENS, TOP), 1, 65), jax.random.fold_in(own_keys[2], 1), 1, 64).astype(jnp.int32)
    w_gate = bell_draw(keys[3], (N_EXPERT, D, FF_DEV), D ** -0.5, 0.0625, ((0, 16),))
    w_up = bell_draw(keys[4], (N_EXPERT, D, FF_DEV), D ** -0.5, 0.0625, ((0, 16),))
    w_down = bell_draw(keys[5], (N_EXPERT, FF_DEV, D), FF_WIN ** -0.5, 0.125, ((0, 16),))
    return {"tokens": tokens, "route_ids": route_ids, "levels": levels, "w_gate": w_gate, "w_up": w_up, "w_down": w_down}


def reference(tokens, route_ids, levels, w_gate, w_up, w_down):
    total, width = tokens.shape
    top = route_ids.shape[1]
    experts = w_gate.shape[0] // SHARDS
    room = N_EXPERT * CAP
    flat_ids = route_ids.reshape(-1)
    count = flat_ids.shape[0]
    level_f = levels.astype(jnp.float32)
    weights = level_f / jnp.sum(level_f, axis=1, keepdims=True)
    flat_w = weights.reshape(-1)
    padded = jnp.concatenate([tokens, jnp.zeros((1, width), tokens.dtype)], axis=0)
    source = (jnp.arange(count, dtype=jnp.int32) // top).astype(jnp.int32)
    gates = w_gate.reshape(experts, SHARDS, width, FF_DEV)
    ups = w_up.reshape(experts, SHARDS, width, FF_DEV)
    downs = w_down.reshape(experts, SHARDS, FF_DEV, width)

    def one_expert(carry, index):
        chosen = flat_ids == index
        rank = (jnp.cumsum(chosen.astype(jnp.int32)) - 1).astype(jnp.int32)
        place = jnp.where(chosen, rank, room).astype(jnp.int32)
        owner = jnp.full((room,), total, jnp.int32).at[place].set(source, mode="drop")
        rows = padded[owner]
        summed = jnp.zeros((room, width), jnp.float32)
        for shard in range(SHARDS):
            gate = jnp.dot(rows, gates[index, shard], preferred_element_type=jnp.float32)
            up = jnp.dot(rows, ups[index, shard], preferred_element_type=jnp.float32)
            hidden = (jax.nn.silu(gate) * up).astype(jnp.bfloat16)
            part = jnp.dot(hidden, downs[index, shard], preferred_element_type=jnp.float32).astype(jnp.bfloat16)
            part = lax.optimization_barrier(part)
            summed = summed + part.astype(jnp.float32)
        rounded = summed.astype(jnp.bfloat16)
        rounded = lax.optimization_barrier(rounded)
        out_e = rounded.astype(jnp.float32)
        safe = jnp.clip(rank, 0, room - 1).astype(jnp.int32)
        picked = out_e[safe] * jnp.where(chosen, flat_w, jnp.float32(0.0))[:, None]
        return carry + jnp.sum(picked.reshape(total, top, width), axis=1), None

    start = jnp.zeros((total, width), jnp.float32)
    result, unused = lax.scan(one_expert, start, jnp.arange(experts, dtype=jnp.int32))
    return result.astype(jnp.bfloat16)
```

```python
import functools

import jax
import jax.numpy as jnp
from jax import lax
from jax.experimental import pallas as pl
from jax.experimental.pallas import tpu as pltpu
from jax.sharding import PartitionSpec as P

SHARDS = 4
MESH = pl.DeviceIdType.MESH


def tile_of(length, most):
    size = most
    while length % size:
        size //= 2
    return size


def xor(a, mask, count):
    total, bit = 0, 1
    while bit < count:
        total += (a // bit + mask // bit) % 2 * bit
        bit *= 2
    return total


def layer_kernel(
    planes, out_ref, gate_hbm, up_hbm, down_hbm, ret_ref,
    x, gate, up, down, acc, hidden, pair, cross,
    w_sem, z_send, z_recv, y_send, y_recv, p_send, p_recv,
    rp_send, rp_recv, ry_send, ry_recv, rz_send, rz_recv,
):
    me = lax.axis_index("expert")
    plane, s = me // SHARDS, me % SHARDS
    base = plane * SHARDS
    core, row = s % 2, s // 2
    partner_s = row * 2 + (1 - core)
    cross_s = (1 - row) * 2 + core
    diag_s = (1 - row) * 2 + (1 - core)
    partner, neighbour = base + partner_s, base + cross_s
    cap, width = x.shape[2], x.shape[3]
    rows = SHARDS * cap
    tile = tile_of(width, 1024)
    chunks = width // tile

    barrier = pltpu.get_barrier_semaphore()
    peers = [partner, neighbour]
    peers += [xor(plane, j, planes) * SHARDS + s for j in range(1, planes)]
    for peer in peers:
        pl.semaphore_signal(barrier, inc=1, device_id={"expert": peer}, device_id_type=MESH)
    pl.semaphore_wait(barrier, planes + 1)

    def remote(src, dst, send, recv, device):
        return pltpu.make_async_remote_copy(
            src_ref=src, dst_ref=dst, send_sem=send, recv_sem=recv,
            device_id={"expert": device}, device_id_type=MESH,
        )

    def columns(q):
        return pl.ds(pl.multiple_of(q * tile, tile), tile)

    def out_copy(j):
        to = xor(plane, j, planes)
        return remote(out_ref.at[to], x.at[j, s], z_send.at[j], z_recv.at[j], to * SHARDS + s)

    def own_copy():
        return pltpu.make_async_copy(out_ref.at[plane], x.at[0, s], z_recv.at[0])

    def y_copy(j):
        return remote(x.at[j, s], x.at[j, s], y_send.at[j], y_recv.at[j], neighbour)

    def y_arrival(j):
        return remote(x.at[j, cross_s], x.at[j, cross_s], y_send.at[j], y_recv.at[j], neighbour)

    def p_copy(j, k, slot):
        return remote(x.at[j, slot], x.at[j, slot], p_send.at[j, k], p_recv.at[j, k], partner)

    def rp_copy(j, q, k, slot):
        cols = columns(q)
        return remote(
            x.at[j, slot, :, cols], pair.at[j, k, :, cols],
            rp_send.at[j, q, k], rp_recv.at[j, q, k], partner,
        )

    def ry_copy(j, q):
        cols = columns(q)
        return remote(
            x.at[j, cross_s, :, cols], cross.at[j, :, cols],
            ry_send.at[j, q], ry_recv.at[j, q], neighbour,
        )

    def rz_copy(j, q):
        cols, to = columns(q), xor(plane, j, planes)
        return remote(
            x.at[j, s, :, cols], ret_ref.at[plane, :, cols],
            rz_send.at[j, q], rz_recv.at[j, q], to * SHARDS + s,
        )

    def keep_copy(q):
        cols = columns(q)
        return pltpu.make_async_copy(x.at[0, s, :, cols], ret_ref.at[plane, :, cols], rz_send.at[0, q])

    own_copy().start()
    for distance in range(1, planes):
        for to in (plane + distance, plane - distance):
            @pl.when((to >= 0) & (to < planes))
            def _():
                mask = xor(plane, to, planes)
                remote(
                    out_ref.at[to], x.at[mask, s], z_send.at[mask], z_recv.at[mask], to * SHARDS + s
                ).start()
    loads = [
        pltpu.make_async_copy(gate_hbm.at[0], gate, w_sem.at[0]),
        pltpu.make_async_copy(up_hbm.at[0], up, w_sem.at[1]),
        pltpu.make_async_copy(down_hbm.at[0], down, w_sem.at[2]),
    ]
    for load in loads:
        load.start()

    def arrive(j):
        if j == 0:
            own_copy().wait()
        else:
            out_copy(j).wait_recv()
        y_copy(j).start()
        p_copy(j, 0, s).start()

    def gather(j):
        y_arrival(j).wait_recv()
        p_copy(j, 1, cross_s).start()
        p_copy(j, 0, partner_s).wait_recv()
        p_copy(j, 1, diag_s).wait_recv()

    def expand(j):
        @pl.loop(0, chunks)
        def _(q):
            cols = columns(q)
            part = x[j, :, :, cols].reshape(rows, tile)

            @pl.when(q == 0)
            def _():
                acc[...] = jnp.zeros_like(acc)

            acc[0] += jnp.dot(part, gate[cols, :], preferred_element_type=jnp.float32)
            acc[1] += jnp.dot(part, up[cols, :], preferred_element_type=jnp.float32)

        value = acc[0]
        hidden[...] = (value / (1.0 + jnp.exp(-value)) * acc[1]).astype(hidden.dtype)

    def contract(j):
        y_copy(j).wait_send()
        p_copy(j, 0, s).wait_send()
        p_copy(j, 1, cross_s).wait_send()

        @pl.loop(0, chunks + 1)
        def _(q):
            @pl.when(q < chunks)
            def _():
                cols = columns(q)
                part = jnp.dot(hidden[...], down[:, cols], preferred_element_type=jnp.float32)
                x[j, :, :, cols] = part.astype(x.dtype).reshape(SHARDS, cap, tile)
                rp_copy(j, q, 1 - row, diag_s).start()
                rp_copy(j, q, row, partner_s).start()

            @pl.when(q > 0)
            def _():
                cols = columns(q - 1)
                rp_copy(j, q - 1, 1 - row, diag_s).wait_recv()
                total = x[j, cross_s, :, cols].astype(jnp.float32)
                total += pair[j, 1 - row, :, cols].astype(jnp.float32)
                x[j, cross_s, :, cols] = total.astype(x.dtype)
                ry_copy(j, q - 1).start()

    def finish(j):
        @pl.loop(0, chunks)
        def _(q):
            cols = columns(q)
            rp_copy(j, q, row, partner_s).wait_recv()
            total = x[j, s, :, cols].astype(jnp.float32) + pair[j, row, :, cols].astype(jnp.float32)
            ry_copy(j, q).wait_recv()
            x[j, s, :, cols] = (total + cross[j, :, cols].astype(jnp.float32)).astype(x.dtype)
            if j > 0:
                rz_copy(j, q).start()
            else:
                keep_copy(q).start()

    order = [0, *range(2, planes), 1]
    arrive(0)
    arrive(1)
    for i, j in enumerate(order):
        gather(j)
        if 0 < i < planes - 2:
            arrive(order[i + 1])
        if i == 0:
            for load in loads:
                load.wait()
        expand(j)
        contract(j)
        if i == 0:
            arrive(order[1])
        else:
            finish(order[i - 1])
    finish(order[-1])

    for j in range(planes):
        @pl.loop(0, chunks)
        def _(q):
            rp_copy(j, q, 1 - row, diag_s).wait_send()
            rp_copy(j, q, row, partner_s).wait_send()
            ry_copy(j, q).wait_send()
            if j > 0:
                rz_copy(j, q).wait()
            else:
                keep_copy(q).wait()
        if j > 0:
            out_copy(j).wait_send()


def routed_kernel(
    tokens, ids, levels, gate_hbm, up_hbm, down_hbm, out_hbm,
    x, gate, up, down, acc, hidden, pair, cross, raw, raw_y, raw_f,
    near_stage, far_stage, near_ret, outer_ret, far_ret, table, picks, mix,
    w_sem, raw_sem, out_sem, table_send, table_recv,
    cross_send, cross_recv, far_send, far_recv, near_send, near_recv,
    fwd_send, fwd_recv, y_send, y_recv, d_send, d_recv,
    rp_send, rp_recv, ry_send, ry_recv,
    nr_send, nr_recv, or_send, or_recv, fr_send, fr_recv,
    pair_free, cross_free,
):
    me = lax.axis_index("expert")
    plane, s = me // SHARDS, me % SHARDS
    core, row = s % 2, s // 2
    half, near_plane = plane // 2, xor(plane, 1, 4)
    far_plane = 2 * (1 - half) + half
    kind = (plane + half + 1) % 2
    inner, outer = kind == 0, kind == 1
    cross_s = (1 - row) * 2 + core
    partner_s = row * 2 + (1 - core)
    diag_s = (1 - row) * 2 + (1 - core)
    partner, neighbour = plane * SHARDS + partner_s, plane * SHARDS + cross_s
    near, far = near_plane * SHARDS + s, far_plane * SHARDS + s
    far_b = xor(far_plane, 1, 4) * SHARDS + s
    cap, width = x.shape[2], x.shape[3]
    tok_rows = raw.shape[0]
    rows = SHARDS * cap
    tile = tile_of(width, 1024)
    chunks = width // tile
    own_j, near_j = 0, 1

    def columns(q):
        return pl.ds(pl.multiple_of(q * tile, tile), tile)

    def remote(src, dst, send, recv, device):
        return pltpu.make_async_remote_copy(
            src_ref=src, dst_ref=dst, send_sem=send, recv_sem=recv,
            device_id={"expert": device}, device_id_type=MESH,
        )

    def each(body):
        pl.loop(0, chunks)(body)

    raw_load = pltpu.make_async_copy(tokens, raw, raw_sem)
    loads = [
        pltpu.make_async_copy(gate_hbm.at[0], gate, w_sem.at[0]),
        pltpu.make_async_copy(up_hbm.at[0], up, w_sem.at[1]),
        pltpu.make_async_copy(down_hbm.at[0], down, w_sem.at[2]),
    ]
    raw_load.start()

    barrier = pltpu.get_barrier_semaphore()
    peers = [partner, neighbour, near, far, far_b]
    for peer in peers:
        pl.semaphore_signal(barrier, inc=1, device_id={"expert": peer}, device_id_type=MESH)

    lane = lax.broadcasted_iota(jnp.int32, (tok_rows, tok_rows), 1)
    line = lax.broadcasted_iota(jnp.int32, (tok_rows, tok_rows), 0)
    first, second = ids[:, 0:1] == lane, ids[:, 1:2] == lane
    level_0, level_1 = levels[:, 0:1].astype(jnp.float32), levels[:, 1:2].astype(jnp.float32)
    named = jnp.where(first | second, 1.0, 0.0)
    earlier = jnp.where(line > lane, 1.0, 0.0).astype(jnp.bfloat16)
    rank = jnp.dot(earlier, named.astype(jnp.bfloat16), preferred_element_type=jnp.float32)
    place = jnp.where(named > 0.0, rank, 2.0 * tok_rows)
    share = jnp.where(first, level_0 / (level_0 + level_1), 0.0)
    share += jnp.where(second, level_1 / (level_0 + level_1), 0.0)
    table[0, 0:8, :] = jnp.transpose(place)[0:8, :]
    table[0, 8:16, :] = jnp.transpose(share)[0:8, :]

    def matches(k, expert):
        spot = lax.broadcasted_iota(jnp.int32, (cap, tok_rows), 0).astype(jnp.float32)
        return table[k, pl.ds(expert, 1), :] == spot

    def set_pick(k):
        for i, expert in enumerate((plane, near_plane)):
            pick = jnp.where(matches(k, expert), 1.0, 0.0)
            picks[k, i * cap:(i + 1) * cap, :] = pick.astype(picks.dtype)

    def set_mix(k, spot):
        parts = []
        for expert in (plane, near_plane):
            weight = table[k, pl.ds(8 + expert, 1), :]
            parts.append(jnp.where(matches(k, expert), weight, 0.0))
        weight = jnp.transpose(jnp.concatenate(parts, axis=0))
        high = weight.astype(jnp.bfloat16)
        mix[spot, 0] = high
        mix[spot, 1] = (weight - high.astype(jnp.float32)).astype(jnp.bfloat16)

    def select(k, block):
        return jnp.dot(picks[k], block, preferred_element_type=jnp.float32).astype(x.dtype)

    def mixed(spot, own, other):
        both = jnp.concatenate([own, other], axis=0)
        total = jnp.dot(mix[spot, 0], both, preferred_element_type=jnp.float32)
        return total + jnp.dot(mix[spot, 1], both, preferred_element_type=jnp.float32)

    set_pick(0)
    set_mix(0, 0)
    pl.semaphore_wait(barrier, len(peers))

    table_y = remote(table.at[0], table.at[1], table_send.at[0], table_recv.at[0], neighbour)
    table_f = remote(table.at[0], table.at[2 + kind], table_send.at[1], table_recv.at[1 + kind], far)
    table_y.start()
    table_f.start()

    def table_arrival(k):
        return remote(table.at[0], table.at[k], table_send.at[0], table_recv.at[k - 1], far)

    def cross_copy(q):
        cols = columns(q)
        return remote(tokens.at[:, cols], raw_y.at[:, cols], cross_send.at[q], cross_recv.at[q], neighbour)

    def far_copy(q, k):
        cols = columns(q)
        return remote(tokens.at[:, cols], raw_f.at[k, :, cols], far_send.at[q], far_recv.at[k, q], far)

    def near_copy(k, q):
        cols, slot = columns(q), s if k == 0 else cross_s
        return remote(
            near_stage.at[:, cols], x.at[near_j, slot, :, cols],
            near_send.at[k, q], near_recv.at[k, q], near,
        )

    def fwd_copy(i, q):
        cols = columns(q)
        return remote(
            far_stage.at[:, cols], x.at[2 + i, s, :, cols], fwd_send.at[i, q], fwd_recv.at[i, q], near
        )

    def y_copy(i, q):
        cols = columns(q)
        return remote(
            x.at[2 + i, s, :, cols], x.at[2 + i, s, :, cols], y_send.at[i, q], y_recv.at[i, q], neighbour
        )

    def y_arrival(i, q):
        cols = columns(q)
        return remote(
            x.at[2 + i, s, :, cols], x.at[2 + i, cross_s, :, cols],
            y_send.at[i, q], y_recv.at[i, q], neighbour,
        )

    def d_copy(j, r, q):
        cols, slot = columns(q), r * 2 + core
        return remote(
            x.at[j, slot, :, cols], x.at[j, slot, :, cols], d_send.at[j, r], d_recv.at[j, r], partner
        )

    def d_whole(j, r, lane_core):
        slot = r * 2 + lane_core
        return remote(x.at[j, slot], x.at[j, slot], d_send.at[j, r], d_recv.at[j, r], partner)

    def gathered(j):
        for r in range(2):
            d_whole(j, r, 1 - core).wait_recv()

    def rp_copy(j, t, q, k, slot):
        cols = columns(q)
        return remote(
            x.at[j, slot, :, cols], pair.at[t, k, :, cols],
            rp_send.at[j, q, k], rp_recv.at[j, q, k], partner,
        )

    def ry_copy(j, t, q):
        cols = columns(q)
        return remote(
            x.at[j, cross_s, :, cols], cross.at[t, :, cols],
            ry_send.at[j, q], ry_recv.at[j, q], neighbour,
        )

    def nr_copy(q):
        cols = columns(q)
        return remote(x.at[near_j, s, :, cols], near_ret.at[:, cols], nr_send.at[q], nr_recv.at[q], near)

    def or_copy(i, q):
        cols = columns(q)
        return remote(
            x.at[2 + i, s, :, cols], outer_ret.at[i, :, cols], or_send.at[i, q], or_recv.at[i, q], near
        )

    def fr_copy(i, q):
        cols = columns(q)
        return remote(
            raw_f.at[i, :, cols], far_ret.at[:, cols], fr_send.at[i, q], fr_recv.at[q],
            far if i == 0 else far_b,
        )

    def out_copy(q):
        cols = columns(q)
        return pltpu.make_async_copy(raw.at[:, cols], out_hbm.at[:, cols], out_sem.at[q])

    def expand(j, spot):
        @each
        def _(q):
            cols = columns(q)
            part = x[j, :, :, cols].reshape(rows, tile)

            @pl.when(q == 0)
            def _():
                acc[...] = jnp.zeros_like(acc)

            acc[0] += jnp.dot(part, gate[cols, :], preferred_element_type=jnp.float32)
            acc[1] += jnp.dot(part, up[cols, :], preferred_element_type=jnp.float32)

        value = acc[0]
        hidden[spot] = (value / (1.0 + jnp.exp(-value)) * acc[1]).astype(hidden.dtype)

    def contract(j, t, spot, credit):
        for r in range(2):
            d_whole(j, r, core).wait_send()
        if j >= 2:
            @each
            def _(q):
                y_copy(j - 2, q).wait_send()
        if credit:
            pl.semaphore_wait(pair_free, 1)
            pl.semaphore_wait(cross_free, 1)

        @pl.loop(0, chunks + 1)
        def _(q):
            @pl.when(q < chunks)
            def _():
                cols = columns(q)
                part = jnp.dot(hidden[spot], down[:, cols], preferred_element_type=jnp.float32)
                x[j, :, :, cols] = part.astype(x.dtype).reshape(SHARDS, cap, tile)
                rp_copy(j, t, q, 1 - row, diag_s).start()
                rp_copy(j, t, q, row, partner_s).start()

            @pl.when(q > 0)
            def _():
                cols = columns(q - 1)
                rp_copy(j, t, q - 1, 1 - row, diag_s).wait_recv()
                total = x[j, cross_s, :, cols].astype(jnp.float32)
                total += pair[t, 1 - row, :, cols].astype(jnp.float32)
                x[j, cross_s, :, cols] = total.astype(x.dtype)
                ry_copy(j, t, q - 1).start()

    def finish(j, t, credit, then):
        @each
        def _(q):
            cols = columns(q)
            rp_copy(j, t, q, row, partner_s).wait_recv()
            total = x[j, s, :, cols].astype(jnp.float32) + pair[t, row, :, cols].astype(jnp.float32)
            ry_copy(j, t, q).wait_recv()
            x[j, s, :, cols] = (total + cross[t, :, cols].astype(jnp.float32)).astype(x.dtype)
            then(q)

        if credit:
            pl.semaphore_signal(pair_free, inc=1, device_id={"expert": partner}, device_id_type=MESH)
            pl.semaphore_signal(cross_free, inc=1, device_id={"expert": neighbour}, device_id_type=MESH)

    def to_inner(i):
        def then(q):
            @pl.when(outer)
            def _():
                or_copy(i, q).start()

        return then

    def merge(i):
        @pl.when(inner)
        def _():
            @each
            def _(q):
                cols = columns(q)
                or_copy(i, q).wait_recv()
                total = mixed(1 + i, x[2 + i, s, :, cols], outer_ret[i, :, cols])
                raw_f[i, :, cols] = total.astype(raw_f.dtype)
                fr_copy(i, q).start()

    def enter(i, q):
        cols = columns(q)

        @pl.when(inner)
        def _():
            far_copy(q, i).wait_recv()
            taken = select(2 + i, raw_f[i, :, cols])
            x[2 + i, s, :, cols] = taken[:cap]
            if i > 0:
                fwd_copy(i - 1, q).wait_send()
            far_stage[:, cols] = taken[cap:]
            fwd_copy(i, q).start()

        @pl.when(outer)
        def _():
            fwd_copy(i, q).wait_recv()

        y_copy(i, q).start()
        d_copy(2 + i, row, q).start()

    each(lambda q: cross_copy(q).start())

    @pl.when(inner)
    def _():
        each(lambda q: far_copy(q, 0).start())

    for load in loads:
        load.start()
    raw_load.wait()

    @each
    def _(q):
        cols = columns(q)
        taken = select(0, raw[:, cols])
        near_stage[:, cols] = taken[cap:]
        near_copy(0, q).start()
        x[own_j, s, :, cols] = taken[:cap]
        d_copy(own_j, row, q).start()

    @pl.when(outer)
    def _():
        each(lambda q: far_copy(q, 1).start())

    table_arrival(1).wait_recv()
    set_pick(1)

    @pl.when(inner)
    def _():
        for i in range(2):
            table_arrival(2 + i).wait_recv()
            set_pick(2 + i)
            set_mix(2 + i, 1 + i)

    @each
    def _(q):
        cols = columns(q)
        cross_copy(q).wait_recv()
        taken = select(1, raw_y[:, cols])
        near_copy(0, q).wait_send()
        near_stage[:, cols] = taken[cap:]
        near_copy(1, q).start()
        x[own_j, cross_s, :, cols] = taken[:cap]
        d_copy(own_j, 1 - row, q).start()
        enter(0, q)

    loads[0].wait()
    loads[1].wait()
    gathered(own_j)
    expand(own_j, 0)

    @each
    def _(q):
        enter(1, q)
        y_arrival(0, q).wait_recv()
        d_copy(2, 1 - row, q).start()

    gathered(2)
    expand(2, 1)
    loads[2].wait()
    contract(2, 0, 1, False)

    @each
    def _(q):
        y_arrival(1, q).wait_recv()
        d_copy(3, 1 - row, q).start()

    gathered(3)
    expand(3, 1)
    contract(3, 1, 1, False)
    finish(2, 0, True, to_inner(0))
    contract(own_j, 0, 0, True)
    merge(0)

    @each
    def _(q):
        for k in range(2):
            near_copy(k, q).wait_recv()
            d_copy(near_j, row if k == 0 else 1 - row, q).start()

    gathered(near_j)
    expand(near_j, 1)
    finish(3, 1, True, to_inner(1))
    contract(near_j, 1, 1, True)
    merge(1)
    finish(own_j, 0, False, lambda q: None)
    finish(near_j, 1, False, lambda q: nr_copy(q).start())

    @each
    def _(q):
        cols = columns(q)
        nr_copy(q).wait_recv()
        fr_copy(0, q).wait_recv()
        total = mixed(0, x[own_j, s, :, cols], near_ret[:, cols])
        raw[:, cols] = (total + far_ret[:, cols].astype(jnp.float32)).astype(raw.dtype)
        out_copy(q).start()

    table_y.wait_send()
    table_f.wait_send()

    @each
    def _(q):
        cross_copy(q).wait_send()
        far_copy(q, 0).wait_send()
        near_copy(1, q).wait_send()
        nr_copy(q).wait_send()
        for j, t in ((0, 0), (1, 1), (2, 0), (3, 1)):
            rp_copy(j, t, q, 1 - row, diag_s).wait_send()
            rp_copy(j, t, q, row, partner_s).wait_send()
            ry_copy(j, t, q).wait_send()

        @pl.when(inner)
        def _():
            fwd_copy(1, q).wait_send()
            fr_copy(0, q).wait_send()
            fr_copy(1, q).wait_send()

        @pl.when(outer)
        def _():
            or_copy(0, q).wait_send()
            or_copy(1, q).wait_send()

        out_copy(q).wait()


def routed(tokens, route_ids, levels, w_gate, w_up, w_down, cap):
    tok_rows, width = tokens.shape
    ff, dtype = w_gate.shape[2], tokens.dtype
    rows, chunks = SHARDS * cap, width // tile_of(width, 1024)
    dma, vmem = pltpu.SemaphoreType.DMA, pltpu.VMEM
    anywhere, local = pl.BlockSpec(memory_space=pl.ANY), pl.BlockSpec(memory_space=pltpu.VMEM)
    return pl.pallas_call(
        routed_kernel,
        out_shape=jax.ShapeDtypeStruct((tok_rows, width), dtype),
        in_specs=[anywhere, local, local, anywhere, anywhere, anywhere],
        out_specs=anywhere,
        scratch_shapes=[
            vmem((4, SHARDS, cap, width), dtype),
            vmem((width, ff), dtype),
            vmem((width, ff), dtype),
            vmem((ff, width), dtype),
            vmem((2, rows, ff), jnp.float32),
            vmem((2, rows, ff), dtype),
            vmem((2, 2, cap, width), dtype),
            vmem((2, cap, width), dtype),
            vmem((tok_rows, width), dtype),
            vmem((tok_rows, width), dtype),
            vmem((2, tok_rows, width), dtype),
            vmem((cap, width), dtype),
            vmem((cap, width), dtype),
            vmem((cap, width), dtype),
            vmem((2, cap, width), dtype),
            vmem((tok_rows, width), dtype),
            vmem((4, 16, tok_rows), jnp.float32),
            vmem((4, 2 * cap, tok_rows), dtype),
            vmem((3, 2, tok_rows, 2 * cap), dtype),
            dma((3,)), dma, dma((chunks,)), dma((2,)), dma((3,)),
            dma((chunks,)), dma((chunks,)), dma((chunks,)), dma((2, chunks)),
            dma((2, chunks)), dma((2, chunks)),
            dma((2, chunks)), dma((2, chunks)),
            dma((2, chunks)), dma((2, chunks)),
            dma((4, 2)), dma((4, 2)),
            dma((4, chunks, 2)), dma((4, chunks, 2)),
            dma((4, chunks)), dma((4, chunks)),
            dma((chunks,)), dma((chunks,)),
            dma((2, chunks)), dma((2, chunks)),
            dma((2, chunks)), dma((chunks,)),
            pltpu.SemaphoreType.REGULAR, pltpu.SemaphoreType.REGULAR,
        ],
        compiler_params=pltpu.CompilerParams(
            collective_id=0, has_side_effects=True, vmem_limit_bytes=67_000_000
        ),
    )(tokens, route_ids, levels, w_gate, w_up, w_down)


def combine_kernel(weight_ref, ret_ref, out_ref):
    weight = weight_ref[...]
    high = weight.astype(jnp.bfloat16)
    low = (weight - high.astype(jnp.float32)).astype(jnp.bfloat16)
    total = jnp.dot(high, ret_ref[...], preferred_element_type=jnp.float32)
    total += jnp.dot(low, ret_ref[...], preferred_element_type=jnp.float32)
    out_ref[...] = total.astype(out_ref.dtype)


def on_device(tokens, route_ids, levels, w_gate, w_up, w_down):
    tok_rows, width = tokens.shape
    top = route_ids.shape[1]
    ff = w_gate.shape[2]
    experts = lax.axis_size("expert") // SHARDS
    capacity = 5 * tok_rows * top // (4 * experts)
    cap = -(-capacity // 16) * 16
    slots = experts * cap
    dtype = tokens.dtype
    if experts == 4 and top == 2 and tok_rows < 2 * cap:
        return routed(tokens, route_ids, levels, w_gate, w_up, w_down, cap)

    chosen = route_ids[:, :, None] == jnp.arange(experts, dtype=jnp.int32)
    named = jnp.any(chosen, axis=1)
    index = jnp.arange(tok_rows, dtype=jnp.int32)
    earlier = (index[:, None] > index[None, :]).astype(jnp.bfloat16)
    rank = jnp.dot(earlier, named.astype(jnp.bfloat16), preferred_element_type=jnp.float32)
    place = jnp.where(named, rank.astype(jnp.int32), cap)
    level_f = levels.astype(jnp.float32)
    weights = level_f / jnp.sum(level_f, axis=1, keepdims=True)
    weight_e = jnp.sum(jnp.where(chosen, weights[:, :, None], 0.0), axis=1)
    spot = jnp.arange(cap, dtype=jnp.int32)
    pick = (place[:, :, None] == spot).reshape(tok_rows, slots)
    weight_m = jnp.where(pick, jnp.repeat(weight_e, cap, axis=1), 0.0)
    outgoing = lax.dot_general(
        pick.astype(dtype), tokens, (((0,), (0,)), ((), ())), preferred_element_type=jnp.float32
    ).astype(dtype).reshape(experts, cap, width)

    dma, anywhere = pltpu.SemaphoreType.DMA, pl.BlockSpec(memory_space=pl.ANY)
    rows, chunks = SHARDS * cap, width // tile_of(width, 1024)
    returned = pl.pallas_call(
        functools.partial(layer_kernel, experts),
        out_shape=jax.ShapeDtypeStruct((experts, cap, width), dtype),
        in_specs=[anywhere] * 4,
        out_specs=anywhere,
        scratch_shapes=[
            pltpu.VMEM((experts, SHARDS, cap, width), dtype),
            pltpu.VMEM((width, ff), dtype),
            pltpu.VMEM((width, ff), dtype),
            pltpu.VMEM((ff, width), dtype),
            pltpu.VMEM((2, rows, ff), jnp.float32),
            pltpu.VMEM((rows, ff), dtype),
            pltpu.VMEM((experts, 2, cap, width), dtype),
            pltpu.VMEM((experts, cap, width), dtype),
            dma((3,)),
            dma((experts,)), dma((experts,)),
            dma((experts,)), dma((experts,)),
            dma((experts, 2)), dma((experts, 2)),
            dma((experts, chunks, 2)), dma((experts, chunks, 2)),
            dma((experts, chunks)), dma((experts, chunks)),
            dma((experts, chunks)), dma((experts, chunks)),
        ],
        compiler_params=pltpu.CompilerParams(
            collective_id=0, has_side_effects=True, vmem_limit_bytes=67_000_000
        ),
    )(outgoing, w_gate, w_up, w_down)

    tile = tile_of(width, 1024)
    return pl.pallas_call(
        combine_kernel,
        out_shape=jax.ShapeDtypeStruct((tok_rows, width), dtype),
        grid=(width // tile,),
        in_specs=[
            pl.BlockSpec((tok_rows, slots), lambda n: (0, 0)),
            pl.BlockSpec((slots, tile), lambda n: (0, n)),
        ],
        out_specs=pl.BlockSpec((tok_rows, tile), lambda n: (0, n)),
    )(weight_m, returned.reshape(slots, width))


def solution(mesh):
    return jax.shard_map(
        on_device,
        mesh=mesh,
        in_specs=(
            P(("groups", "expert"), None),
            P(("groups", "expert"), None),
            P(("groups", "expert"), None),
            P("expert", None, None),
            P("expert", None, None),
            P("expert", None, None),
        ),
        out_specs=P(("groups", "expert"), None),
        check_vma=False,
    )
```

```python
import functools

import jax
import jax.numpy as jnp
from jax import lax
from jax.experimental import pallas as pl
from jax.experimental.pallas import tpu as pltpu
from jax.sharding import PartitionSpec as P

SHARDS = 4
MESH = pl.DeviceIdType.MESH


def tile_of(length, most):
    size = most
    while length % size:
        size //= 2
    return size


def xor(a, mask, count):
    total, bit = 0, 1
    while bit < count:
        total += (a // bit + mask // bit) % 2 * bit
        bit *= 2
    return total


def layer_kernel(
    planes, out_ref, gate_hbm, up_hbm, down_hbm, ret_ref,
    x, gate, up, down, acc, hidden, pair, cross,
    w_sem, z_send, z_recv, y_send, y_recv, p_send, p_recv,
    rp_send, rp_recv, ry_send, ry_recv, rz_send, rz_recv,
):
    me = lax.axis_index("expert")
    plane, s = me // SHARDS, me % SHARDS
    base = plane * SHARDS
    core, row = s % 2, s // 2
    partner_s = row * 2 + (1 - core)
    cross_s = (1 - row) * 2 + core
    diag_s = (1 - row) * 2 + (1 - core)
    partner, neighbour = base + partner_s, base + cross_s
    cap, width = x.shape[2], x.shape[3]
    rows = SHARDS * cap
    tile = tile_of(width, 1024)
    chunks = width // tile

    barrier = pltpu.get_barrier_semaphore()
    peers = [partner, neighbour]
    peers += [xor(plane, j, planes) * SHARDS + s for j in range(1, planes)]
    for peer in peers:
        pl.semaphore_signal(barrier, inc=1, device_id={"expert": peer}, device_id_type=MESH)
    pl.semaphore_wait(barrier, planes + 1)

    def remote(src, dst, send, recv, device):
        return pltpu.make_async_remote_copy(
            src_ref=src, dst_ref=dst, send_sem=send, recv_sem=recv,
            device_id={"expert": device}, device_id_type=MESH,
        )

    def columns(q):
        return pl.ds(pl.multiple_of(q * tile, tile), tile)

    def out_copy(j):
        to = xor(plane, j, planes)
        return remote(out_ref.at[to], x.at[j, s], z_send.at[j], z_recv.at[j], to * SHARDS + s)

    def own_copy():
        return pltpu.make_async_copy(out_ref.at[plane], x.at[0, s], z_recv.at[0])

    def y_copy(j):
        return remote(x.at[j, s], x.at[j, s], y_send.at[j], y_recv.at[j], neighbour)

    def y_arrival(j):
        return remote(x.at[j, cross_s], x.at[j, cross_s], y_send.at[j], y_recv.at[j], neighbour)

    def p_copy(j, k, slot):
        return remote(x.at[j, slot], x.at[j, slot], p_send.at[j, k], p_recv.at[j, k], partner)

    def rp_copy(j, q, k, slot):
        cols = columns(q)
        return remote(
            x.at[j, slot, :, cols], pair.at[j, k, :, cols],
            rp_send.at[j, q, k], rp_recv.at[j, q, k], partner,
        )

    def ry_copy(j, q):
        cols = columns(q)
        return remote(
            x.at[j, cross_s, :, cols], cross.at[j, :, cols],
            ry_send.at[j, q], ry_recv.at[j, q], neighbour,
        )

    def rz_copy(j, q):
        cols, to = columns(q), xor(plane, j, planes)
        return remote(
            x.at[j, s, :, cols], ret_ref.at[plane, :, cols],
            rz_send.at[j, q], rz_recv.at[j, q], to * SHARDS + s,
        )

    def keep_copy(q):
        cols = columns(q)
        return pltpu.make_async_copy(x.at[0, s, :, cols], ret_ref.at[plane, :, cols], rz_send.at[0, q])

    own_copy().start()
    for distance in range(1, planes):
        for to in (plane + distance, plane - distance):
            @pl.when((to >= 0) & (to < planes))
            def _():
                mask = xor(plane, to, planes)
                remote(
                    out_ref.at[to], x.at[mask, s], z_send.at[mask], z_recv.at[mask], to * SHARDS + s
                ).start()
    loads = [
        pltpu.make_async_copy(gate_hbm.at[0], gate, w_sem.at[0]),
        pltpu.make_async_copy(up_hbm.at[0], up, w_sem.at[1]),
        pltpu.make_async_copy(down_hbm.at[0], down, w_sem.at[2]),
    ]
    for load in loads:
        load.start()

    def arrive(j):
        if j == 0:
            own_copy().wait()
        else:
            out_copy(j).wait_recv()
        y_copy(j).start()
        p_copy(j, 0, s).start()

    def gather(j):
        y_arrival(j).wait_recv()
        p_copy(j, 1, cross_s).start()
        p_copy(j, 0, partner_s).wait_recv()
        p_copy(j, 1, diag_s).wait_recv()

    def expand(j):
        @pl.loop(0, chunks)
        def _(q):
            cols = columns(q)
            part = x[j, :, :, cols].reshape(rows, tile)

            @pl.when(q == 0)
            def _():
                acc[...] = jnp.zeros_like(acc)

            acc[0] += jnp.dot(part, gate[cols, :], preferred_element_type=jnp.float32)
            acc[1] += jnp.dot(part, up[cols, :], preferred_element_type=jnp.float32)

        value = acc[0]
        hidden[...] = (value / (1.0 + jnp.exp(-value)) * acc[1]).astype(hidden.dtype)

    def contract(j):
        y_copy(j).wait_send()
        p_copy(j, 0, s).wait_send()
        p_copy(j, 1, cross_s).wait_send()

        @pl.loop(0, chunks + 1)
        def _(q):
            @pl.when(q < chunks)
            def _():
                cols = columns(q)
                part = jnp.dot(hidden[...], down[:, cols], preferred_element_type=jnp.float32)
                x[j, :, :, cols] = part.astype(x.dtype).reshape(SHARDS, cap, tile)
                rp_copy(j, q, 1 - row, diag_s).start()
                rp_copy(j, q, row, partner_s).start()

            @pl.when(q > 0)
            def _():
                cols = columns(q - 1)
                rp_copy(j, q - 1, 1 - row, diag_s).wait_recv()
                total = x[j, cross_s, :, cols].astype(jnp.float32)
                total += pair[j, 1 - row, :, cols].astype(jnp.float32)
                x[j, cross_s, :, cols] = total.astype(x.dtype)
                ry_copy(j, q - 1).start()

    def finish(j):
        @pl.loop(0, chunks)
        def _(q):
            cols = columns(q)
            rp_copy(j, q, row, partner_s).wait_recv()
            total = x[j, s, :, cols].astype(jnp.float32) + pair[j, row, :, cols].astype(jnp.float32)
            ry_copy(j, q).wait_recv()
            x[j, s, :, cols] = (total + cross[j, :, cols].astype(jnp.float32)).astype(x.dtype)
            if j > 0:
                rz_copy(j, q).start()
            else:
                keep_copy(q).start()

    order = [0, *range(2, planes), 1]
    arrive(0)
    arrive(1)
    for i, j in enumerate(order):
        gather(j)
        if 0 < i < planes - 2:
            arrive(order[i + 1])
        if i == 0:
            for load in loads:
                load.wait()
        expand(j)
        contract(j)
        if i == 0:
            arrive(order[1])
        else:
            finish(order[i - 1])
    finish(order[-1])

    for j in range(planes):
        @pl.loop(0, chunks)
        def _(q):
            rp_copy(j, q, 1 - row, diag_s).wait_send()
            rp_copy(j, q, row, partner_s).wait_send()
            ry_copy(j, q).wait_send()
            if j > 0:
                rz_copy(j, q).wait()
            else:
                keep_copy(q).wait()
        if j > 0:
            out_copy(j).wait_send()


def routed_kernel(
    tokens, ids, levels, gate_hbm, up_hbm, down_hbm, out_hbm,
    x, gate, up, down, acc, hidden, pair, cross, raw, raw_y, raw_f,
    near_stage, near_ret, outer_ret, far_ret, table, picks, mix,
    w_sem, raw_sem, out_sem, table_send, table_recv,
    cross_send, cross_recv, far_send, far_recv, near_send, near_recv,
    fwd_send, fwd_recv, y_send, y_recv, d_send, d_recv,
    rp_send, rp_recv, ry_send, ry_recv,
    nr_send, nr_recv, or_send, or_recv, fr_send, fr_recv,
    pair_free, cross_free,
):
    me = lax.axis_index("expert")
    plane, s = me // SHARDS, me % SHARDS
    core, row = s % 2, s // 2
    half, near_plane = plane // 2, xor(plane, 1, 4)
    far_plane = 2 * (1 - half) + half
    kind = (plane + half + 1) % 2
    inner, outer = kind == 0, kind == 1
    cross_s = (1 - row) * 2 + core
    partner_s = row * 2 + (1 - core)
    diag_s = (1 - row) * 2 + (1 - core)
    partner, neighbour = plane * SHARDS + partner_s, plane * SHARDS + cross_s
    near, far = near_plane * SHARDS + s, far_plane * SHARDS + s
    far_b = xor(far_plane, 1, 4) * SHARDS + s
    cap, width = x.shape[2], x.shape[3]
    tok_rows = raw.shape[0]
    rows = SHARDS * cap
    tile = tile_of(width, 1024)
    chunks = width // tile
    own_j, near_j = 0, 1

    def columns(q):
        return pl.ds(pl.multiple_of(q * tile, tile), tile)

    def remote(src, dst, send, recv, device):
        return pltpu.make_async_remote_copy(
            src_ref=src, dst_ref=dst, send_sem=send, recv_sem=recv,
            device_id={"expert": device}, device_id_type=MESH,
        )

    def each(body):
        pl.loop(0, chunks)(body)

    raw_load = pltpu.make_async_copy(tokens, raw, raw_sem)
    loads = [
        pltpu.make_async_copy(gate_hbm.at[0], gate, w_sem.at[0]),
        pltpu.make_async_copy(up_hbm.at[0], up, w_sem.at[1]),
        pltpu.make_async_copy(down_hbm.at[0], down, w_sem.at[2]),
    ]
    raw_load.start()

    barrier = pltpu.get_barrier_semaphore()
    peers = [partner, neighbour, near, far, far_b]
    for peer in peers:
        pl.semaphore_signal(barrier, inc=1, device_id={"expert": peer}, device_id_type=MESH)

    lane = lax.broadcasted_iota(jnp.int32, (tok_rows, tok_rows), 1)
    line = lax.broadcasted_iota(jnp.int32, (tok_rows, tok_rows), 0)
    expert_of = lax.broadcasted_iota(jnp.int32, (8, tok_rows), 0)
    first, second = ids[0:1, :] == expert_of, ids[1:2, :] == expert_of
    level_0, level_1 = levels[0:1, :].astype(jnp.float32), levels[1:2, :].astype(jnp.float32)
    named = jnp.where(first | second, 1.0, 0.0)
    earlier = jnp.where(line < lane, 1.0, 0.0).astype(jnp.bfloat16)
    rank = jnp.dot(named.astype(jnp.bfloat16), earlier, preferred_element_type=jnp.float32)
    share = jnp.where(first, level_0 / (level_0 + level_1), 0.0)
    share += jnp.where(second, level_1 / (level_0 + level_1), 0.0)
    table[0, 0:8, :] = jnp.where(named > 0.0, rank, 2.0 * tok_rows)
    table[0, 8:16, :] = share

    def matches(k, expert):
        spot = lax.broadcasted_iota(jnp.int32, (cap, tok_rows), 0).astype(jnp.float32)
        return table[k, pl.ds(expert, 1), :] == spot

    def set_pick(k):
        for i, expert in enumerate((plane, near_plane)):
            pick = jnp.where(matches(k, expert), 1.0, 0.0)
            picks[k, i * cap:(i + 1) * cap, :] = pick.astype(picks.dtype)

    def set_mix(k, spot):
        parts = []
        for expert in (plane, near_plane):
            weight = table[k, pl.ds(8 + expert, 1), :]
            parts.append(jnp.where(matches(k, expert), weight, 0.0))
        weight = jnp.transpose(jnp.concatenate(parts, axis=0))
        high = weight.astype(jnp.bfloat16)
        mix[spot, 0] = high
        mix[spot, 1] = (weight - high.astype(jnp.float32)).astype(jnp.bfloat16)

    def select(k, block):
        return jnp.dot(picks[k], block, preferred_element_type=jnp.float32).astype(x.dtype)

    def mixed(spot, own, other):
        both = jnp.concatenate([own, other], axis=0)
        total = jnp.dot(mix[spot, 0], both, preferred_element_type=jnp.float32)
        return total + jnp.dot(mix[spot, 1], both, preferred_element_type=jnp.float32)

    set_pick(0)
    set_mix(0, 0)
    pl.semaphore_wait(barrier, len(peers))

    table_y = remote(table.at[0], table.at[1], table_send.at[0], table_recv.at[0], neighbour)
    table_f = remote(table.at[0], table.at[3 - kind], table_send.at[1], table_recv.at[2 - kind], far)
    table_y.start()
    table_f.start()

    def table_arrival(k):
        return remote(table.at[0], table.at[k], table_send.at[0], table_recv.at[k - 1], far)

    def cross_copy(q):
        cols = columns(q)
        return remote(raw.at[:, cols], raw_y.at[:, cols], cross_send.at[q], cross_recv.at[q], neighbour)

    def far_copy(q, k):
        cols = columns(q)
        return remote(raw.at[:, cols], raw_f.at[k, :, cols], far_send.at[q], far_recv.at[k, q], far)

    def near_copy(k, q):
        cols, slot = columns(q), s if k == 0 else cross_s
        return remote(
            near_stage.at[k, :, cols], x.at[near_j, slot, :, cols],
            near_send.at[k, q], near_recv.at[k, q], near,
        )

    def fwd_copy(i, q):
        cols = columns(q)
        return remote(
            raw_f.at[i, pl.ds(0, cap), cols], x.at[2 + i, s, :, cols], fwd_send.at[i, q], fwd_recv.at[i, q], near
        )

    def y_copy(i, q):
        cols = columns(q)
        return remote(
            x.at[2 + i, s, :, cols], x.at[2 + i, s, :, cols], y_send.at[i, q], y_recv.at[i, q], neighbour
        )

    def y_arrival(i, q):
        cols = columns(q)
        return remote(
            x.at[2 + i, s, :, cols], x.at[2 + i, cross_s, :, cols],
            y_send.at[i, q], y_recv.at[i, q], neighbour,
        )

    def d_copy(j, r, q):
        cols, slot = columns(q), r * 2 + core
        return remote(
            x.at[j, slot, :, cols], x.at[j, slot, :, cols], d_send.at[j, r], d_recv.at[j, r], partner
        )

    def d_whole(j, r, lane_core):
        slot = r * 2 + lane_core
        return remote(x.at[j, slot], x.at[j, slot], d_send.at[j, r], d_recv.at[j, r], partner)

    def gathered(j):
        for r in range(2):
            d_whole(j, r, 1 - core).wait_recv()

    def rp_copy(j, t, q, k, slot):
        cols = columns(q)
        return remote(
            x.at[j, slot, :, cols], pair.at[t, k, :, cols],
            rp_send.at[j, q, k], rp_recv.at[j, q, k], partner,
        )

    def ry_copy(j, t, q):
        cols = columns(q)
        return remote(
            x.at[j, cross_s, :, cols], cross.at[t, :, cols],
            ry_send.at[j, q], ry_recv.at[j, q], neighbour,
        )

    def nr_copy(q):
        cols = columns(q)
        return remote(x.at[near_j, s, :, cols], near_ret.at[:, cols], nr_send.at[q], nr_recv.at[q], near)

    def or_copy(i, q):
        cols = columns(q)
        return remote(
            x.at[2 + i, s, :, cols], outer_ret.at[i, :, cols], or_send.at[i, q], or_recv.at[i, q], near
        )

    def fr_copy(i, q):
        cols = columns(q)
        return remote(
            raw_f.at[i, :, cols], far_ret.at[:, cols], fr_send.at[i, q], fr_recv.at[q],
            far_b if i == 0 else far,
        )

    def out_copy(q):
        cols = columns(q)
        return pltpu.make_async_copy(raw.at[:, cols], out_hbm.at[:, cols], out_sem.at[q])

    def expand(j, spot):
        @each
        def _(q):
            cols = columns(q)
            part = x[j, :, :, cols].reshape(rows, tile)

            @pl.when(q == 0)
            def _():
                acc[...] = jnp.zeros_like(acc)

            acc[0] += jnp.dot(part, gate[cols, :], preferred_element_type=jnp.float32)
            acc[1] += jnp.dot(part, up[cols, :], preferred_element_type=jnp.float32)

        value = acc[0]
        hidden[spot] = (value / (1.0 + jnp.exp(-value)) * acc[1]).astype(hidden.dtype)

    def contract(j, t, spot, credit, also):
        for r in range(2):
            d_whole(j, r, core).wait_send()
        if j >= 2:
            @each
            def _(q):
                y_copy(j - 2, q).wait_send()
        if credit:
            pl.semaphore_wait(pair_free, 1)
            pl.semaphore_wait(cross_free, 1)

        @pl.loop(0, chunks + 1)
        def _(q):
            @pl.when(q < chunks)
            def _():
                cols = columns(q)
                part = jnp.dot(hidden[spot], down[:, cols], preferred_element_type=jnp.float32)
                x[j, :, :, cols] = part.astype(x.dtype).reshape(SHARDS, cap, tile)
                rp_copy(j, t, q, 1 - row, diag_s).start()
                rp_copy(j, t, q, row, partner_s).start()
                for step in also:
                    step(q)

            @pl.when(q > 0)
            def _():
                cols = columns(q - 1)
                rp_copy(j, t, q - 1, 1 - row, diag_s).wait_recv()
                total = x[j, cross_s, :, cols].astype(jnp.float32)
                total += pair[t, 1 - row, :, cols].astype(jnp.float32)
                x[j, cross_s, :, cols] = total.astype(x.dtype)
                ry_copy(j, t, q - 1).start()

    def finish(j, t):
        def step(q):
            cols = columns(q)
            rp_copy(j, t, q, row, partner_s).wait_recv()
            total = x[j, s, :, cols].astype(jnp.float32) + pair[t, row, :, cols].astype(jnp.float32)
            ry_copy(j, t, q).wait_recv()
            x[j, s, :, cols] = (total + cross[t, :, cols].astype(jnp.float32)).astype(x.dtype)
            if j >= 2:
                @pl.when(outer)
                def _():
                    or_copy(j - 2, q).start()
            elif j == near_j:
                nr_copy(q).start()

        return step

    def release():
        pl.semaphore_signal(pair_free, inc=1, device_id={"expert": partner}, device_id_type=MESH)
        pl.semaphore_signal(cross_free, inc=1, device_id={"expert": neighbour}, device_id_type=MESH)

    def merge(i):
        def step(q):
            @pl.when(inner)
            def _():
                cols = columns(q)
                or_copy(i, q).wait_recv()
                total = mixed(1 + i, x[2 + i, s, :, cols], outer_ret[i, :, cols])
                fwd_copy(i, q).wait_send()
                raw_f[i, :, cols] = total.astype(raw_f.dtype)
                fr_copy(i, q).start()

        return step

    def lagged(i):
        def step(q):
            pl.when(q >= 2)(lambda: merge(i)(q - 2))

        return step

    def merge_rest(i):
        pl.loop(chunks - 2, chunks)(merge(i))

    def enter(i, q):
        cols = columns(q)

        @pl.when(inner)
        def _():
            with jax.named_scope("w_far"):
                far_copy(q, i).wait_recv()
            taken = select(2 + i, raw_f[i, :, cols])
            x[2 + i, s, :, cols] = taken[:cap]
            raw_f[i, 0:cap, cols] = taken[cap:]
            fwd_copy(i, q).start()

        @pl.when(outer)
        def _():
            with jax.named_scope("w_fwd"):
                fwd_copy(i, q).wait_recv()

        y_copy(i, q).start()
        d_copy(2 + i, row, q).start()

    def far_table(i):
        @pl.when(inner)
        def _():
            table_arrival(2 + i).wait_recv()
            set_pick(2 + i)
            set_mix(2 + i, 1 + i)

    raw_load.wait()
    each(lambda q: cross_copy(q).start())
    each(lambda q: far_copy(q, 1 - kind).start())
    for load in loads:
        load.start()

    with jax.named_scope("take_own"):
        @each
        def _(q):
            cols = columns(q)
            taken = select(0, raw[:, cols])
            near_stage[0, :, cols] = taken[cap:]
            x[own_j, s, :, cols] = taken[:cap]
            d_copy(own_j, row, q).start()

            @pl.when(outer | (q < 2))
            def _():
                near_copy(0, q).start()

    with jax.named_scope("tables"):
        table_arrival(1).wait_recv()
        set_pick(1)

        far_table(0)

    with jax.named_scope("enter_b"):
        @each
        def _(q):
            cols = columns(q)
            with jax.named_scope("w_cross"):
                cross_copy(q).wait_recv()
            taken = select(1, raw_y[:, cols])
            near_stage[1, :, cols] = taken[cap:]
            x[own_j, cross_s, :, cols] = taken[:cap]
            d_copy(own_j, 1 - row, q).start()
            enter(0, q)

            pl.when(outer)(lambda: near_copy(1, q).start())
            pl.when(inner & (q % 2 == 1))(lambda: near_copy(0, 2 + q // 2).start())

    with jax.named_scope("wait_own"):
        loads[0].wait()
        loads[1].wait()
        gathered(own_j)
    with jax.named_scope("expand_own"):
        expand(own_j, 0)

    with jax.named_scope("enter_a"):
        far_table(1)

        @each
        def _(q):
            enter(1, q)
            with jax.named_scope("w_yb"):
                y_arrival(0, q).wait_recv()
            d_copy(2, 1 - row, q).start()

            late = 2 + chunks // 2 + q // 2

            @pl.when(inner & (q % 2 == 1) & (late < chunks))
            def _():
                near_copy(0, late).start()

    pl.when(inner)(lambda: each(lambda q: near_copy(1, q).start()))

    with jax.named_scope("wait_b"):
        gathered(2)
    with jax.named_scope("expand_b"):
        expand(2, 1)
    loads[2].wait()
    with jax.named_scope("contract_b"):
        contract(2, 0, 1, False, ())

    with jax.named_scope("wait_a"):
        @each
        def _(q):
            y_arrival(1, q).wait_recv()
            d_copy(3, 1 - row, q).start()

        gathered(3)
    with jax.named_scope("expand_a"):
        expand(3, 1)
    with jax.named_scope("contract_a"):
        contract(3, 1, 1, False, (finish(2, 0), lagged(0)))
        release()
    with jax.named_scope("merge_b"):
        merge_rest(0)

    with jax.named_scope("contract_own"):
        contract(own_j, 0, 0, True, (finish(3, 1), lagged(1)))
        release()
    with jax.named_scope("merge_a"):
        merge_rest(1)

    with jax.named_scope("wait_near"):
        @each
        def _(q):
            for k in range(2):
                near_copy(k, q).wait_recv()
                d_copy(near_j, row if k == 0 else 1 - row, q).start()

        gathered(near_j)
    with jax.named_scope("expand_near"):
        expand(near_j, 1)
    with jax.named_scope("contract_near"):
        contract(near_j, 1, 1, True, (finish(own_j, 0),))

    with jax.named_scope("finish_near"):
        each(finish(near_j, 1))

    with jax.named_scope("combine"):
        @each
        def _(q):
            cols = columns(q)
            cross_copy(q).wait_send()
            far_copy(q, 0).wait_send()
            with jax.named_scope("w_nr"):
                nr_copy(q).wait_recv()
            with jax.named_scope("w_fr"):
                fr_copy(0, q).wait_recv()
            total = mixed(0, x[own_j, s, :, cols], near_ret[:, cols])
            raw[:, cols] = (total + far_ret[:, cols].astype(jnp.float32)).astype(raw.dtype)
            out_copy(q).start()

    table_y.wait_send()
    table_f.wait_send()

    @each
    def _(q):
        near_copy(0, q).wait_send()
        near_copy(1, q).wait_send()
        nr_copy(q).wait_send()
        for j, t in ((0, 0), (1, 1), (2, 0), (3, 1)):
            rp_copy(j, t, q, 1 - row, diag_s).wait_send()
            rp_copy(j, t, q, row, partner_s).wait_send()
            ry_copy(j, t, q).wait_send()

        @pl.when(inner)
        def _():
            fr_copy(0, q).wait_send()
            fr_copy(1, q).wait_send()

        @pl.when(outer)
        def _():
            or_copy(0, q).wait_send()
            or_copy(1, q).wait_send()

        out_copy(q).wait()


def routed(tokens, route_ids, levels, w_gate, w_up, w_down, cap):
    tok_rows, width = tokens.shape
    ff, dtype = w_gate.shape[2], tokens.dtype
    rows, chunks = SHARDS * cap, width // tile_of(width, 1024)
    dma, vmem = pltpu.SemaphoreType.DMA, pltpu.VMEM
    anywhere, local = pl.BlockSpec(memory_space=pl.ANY), pl.BlockSpec(memory_space=pltpu.VMEM)
    return pl.pallas_call(
        routed_kernel,
        out_shape=jax.ShapeDtypeStruct((tok_rows, width), dtype),
        in_specs=[anywhere, local, local, anywhere, anywhere, anywhere],
        out_specs=anywhere,
        scratch_shapes=[
            vmem((4, SHARDS, cap, width), dtype),
            vmem((width, ff), dtype),
            vmem((width, ff), dtype),
            vmem((ff, width), dtype),
            vmem((2, rows, ff), jnp.float32),
            vmem((2, rows, ff), dtype),
            vmem((2, 2, cap, width), dtype),
            vmem((2, cap, width), dtype),
            vmem((tok_rows, width), dtype),
            vmem((tok_rows, width), dtype),
            vmem((2, tok_rows, width), dtype),
            vmem((2, cap, width), dtype),
            vmem((cap, width), dtype),
            vmem((2, cap, width), dtype),
            vmem((tok_rows, width), dtype),
            vmem((4, 16, tok_rows), jnp.float32),
            vmem((4, 2 * cap, tok_rows), dtype),
            vmem((3, 2, tok_rows, 2 * cap), dtype),
            dma((3,)), dma, dma((chunks,)), dma((2,)), dma((3,)),
            dma((chunks,)), dma((chunks,)), dma((chunks,)), dma((2, chunks)),
            dma((2, chunks)), dma((2, chunks)),
            dma((2, chunks)), dma((2, chunks)),
            dma((2, chunks)), dma((2, chunks)),
            dma((4, 2)), dma((4, 2)),
            dma((4, chunks, 2)), dma((4, chunks, 2)),
            dma((4, chunks)), dma((4, chunks)),
            dma((chunks,)), dma((chunks,)),
            dma((2, chunks)), dma((2, chunks)),
            dma((2, chunks)), dma((chunks,)),
            pltpu.SemaphoreType.REGULAR, pltpu.SemaphoreType.REGULAR,
        ],
        compiler_params=pltpu.CompilerParams(
            collective_id=0, has_side_effects=True, vmem_limit_bytes=67_000_000
        ),
    )(tokens, route_ids.T, levels.T, w_gate, w_up, w_down)


def combine_kernel(weight_ref, ret_ref, out_ref):
    weight = weight_ref[...]
    high = weight.astype(jnp.bfloat16)
    low = (weight - high.astype(jnp.float32)).astype(jnp.bfloat16)
    total = jnp.dot(high, ret_ref[...], preferred_element_type=jnp.float32)
    total += jnp.dot(low, ret_ref[...], preferred_element_type=jnp.float32)
    out_ref[...] = total.astype(out_ref.dtype)


def on_device(tokens, route_ids, levels, w_gate, w_up, w_down):
    tok_rows, width = tokens.shape
    top = route_ids.shape[1]
    ff = w_gate.shape[2]
    experts = lax.axis_size("expert") // SHARDS
    capacity = 5 * tok_rows * top // (4 * experts)
    cap = -(-capacity // 16) * 16
    slots = experts * cap
    dtype = tokens.dtype
    if experts == 4 and top == 2 and tok_rows < 2 * cap:
        return routed(tokens, route_ids, levels, w_gate, w_up, w_down, cap)

    chosen = route_ids[:, :, None] == jnp.arange(experts, dtype=jnp.int32)
    named = jnp.any(chosen, axis=1)
    index = jnp.arange(tok_rows, dtype=jnp.int32)
    earlier = (index[:, None] > index[None, :]).astype(jnp.bfloat16)
    rank = jnp.dot(earlier, named.astype(jnp.bfloat16), preferred_element_type=jnp.float32)
    place = jnp.where(named, rank.astype(jnp.int32), cap)
    level_f = levels.astype(jnp.float32)
    weights = level_f / jnp.sum(level_f, axis=1, keepdims=True)
    weight_e = jnp.sum(jnp.where(chosen, weights[:, :, None], 0.0), axis=1)
    spot = jnp.arange(cap, dtype=jnp.int32)
    pick = (place[:, :, None] == spot).reshape(tok_rows, slots)
    weight_m = jnp.where(pick, jnp.repeat(weight_e, cap, axis=1), 0.0)
    outgoing = lax.dot_general(
        pick.astype(dtype), tokens, (((0,), (0,)), ((), ())), preferred_element_type=jnp.float32
    ).astype(dtype).reshape(experts, cap, width)

    dma, anywhere = pltpu.SemaphoreType.DMA, pl.BlockSpec(memory_space=pl.ANY)
    rows, chunks = SHARDS * cap, width // tile_of(width, 1024)
    returned = pl.pallas_call(
        functools.partial(layer_kernel, experts),
        out_shape=jax.ShapeDtypeStruct((experts, cap, width), dtype),
        in_specs=[anywhere] * 4,
        out_specs=anywhere,
        scratch_shapes=[
            pltpu.VMEM((experts, SHARDS, cap, width), dtype),
            pltpu.VMEM((width, ff), dtype),
            pltpu.VMEM((width, ff), dtype),
            pltpu.VMEM((ff, width), dtype),
            pltpu.VMEM((2, rows, ff), jnp.float32),
            pltpu.VMEM((rows, ff), dtype),
            pltpu.VMEM((experts, 2, cap, width), dtype),
            pltpu.VMEM((experts, cap, width), dtype),
            dma((3,)),
            dma((experts,)), dma((experts,)),
            dma((experts,)), dma((experts,)),
            dma((experts, 2)), dma((experts, 2)),
            dma((experts, chunks, 2)), dma((experts, chunks, 2)),
            dma((experts, chunks)), dma((experts, chunks)),
            dma((experts, chunks)), dma((experts, chunks)),
        ],
        compiler_params=pltpu.CompilerParams(
            collective_id=0, has_side_effects=True, vmem_limit_bytes=67_000_000
        ),
    )(outgoing, w_gate, w_up, w_down)

    tile = tile_of(width, 1024)
    return pl.pallas_call(
        combine_kernel,
        out_shape=jax.ShapeDtypeStruct((tok_rows, width), dtype),
        grid=(width // tile,),
        in_specs=[
            pl.BlockSpec((tok_rows, slots), lambda n: (0, 0)),
            pl.BlockSpec((slots, tile), lambda n: (0, n)),
        ],
        out_specs=pl.BlockSpec((tok_rows, tile), lambda n: (0, n)),
    )(weight_m, returned.reshape(slots, width))


def solution(mesh):
    return jax.shard_map(
        on_device,
        mesh=mesh,
        in_specs=(
            P(("groups", "expert"), None),
            P(("groups", "expert"), None),
            P(("groups", "expert"), None),
            P("expert", None, None),
            P("expert", None, None),
            P("expert", None, None),
        ),
        out_specs=P(("groups", "expert"), None),
        check_vma=False,
    )
```

```python
import functools

import jax
import jax.numpy as jnp
from jax import lax
from jax.experimental import pallas as pl
from jax.experimental.pallas import tpu as pltpu
from jax.sharding import PartitionSpec as P

SHARDS = 4
MESH = pl.DeviceIdType.MESH


def tile_of(length, most):
    size = most
    while length % size:
        size //= 2
    return size


def xor(a, mask, count):
    total, bit = 0, 1
    while bit < count:
        total += (a // bit + mask // bit) % 2 * bit
        bit *= 2
    return total


def layer_kernel(
    planes, out_ref, gate_hbm, up_hbm, down_hbm, ret_ref,
    x, gate, up, down, acc, hidden, pair, cross,
    w_sem, z_send, z_recv, y_send, y_recv, p_send, p_recv,
    rp_send, rp_recv, ry_send, ry_recv, rz_send, rz_recv,
):
    me = lax.axis_index("expert")
    plane, s = me // SHARDS, me % SHARDS
    base = plane * SHARDS
    core, row = s % 2, s // 2
    partner_s = row * 2 + (1 - core)
    cross_s = (1 - row) * 2 + core
    diag_s = (1 - row) * 2 + (1 - core)
    partner, neighbour = base + partner_s, base + cross_s
    cap, width = x.shape[2], x.shape[3]
    rows = SHARDS * cap
    tile = tile_of(width, 1024)
    chunks = width // tile

    barrier = pltpu.get_barrier_semaphore()
    peers = [partner, neighbour]
    peers += [xor(plane, j, planes) * SHARDS + s for j in range(1, planes)]
    for peer in peers:
        pl.semaphore_signal(barrier, inc=1, device_id={"expert": peer}, device_id_type=MESH)
    pl.semaphore_wait(barrier, planes + 1)

    def remote(src, dst, send, recv, device):
        return pltpu.make_async_remote_copy(
            src_ref=src, dst_ref=dst, send_sem=send, recv_sem=recv,
            device_id={"expert": device}, device_id_type=MESH,
        )

    def columns(q):
        return pl.ds(pl.multiple_of(q * tile, tile), tile)

    def out_copy(j):
        to = xor(plane, j, planes)
        return remote(out_ref.at[to], x.at[j, s], z_send.at[j], z_recv.at[j], to * SHARDS + s)

    def own_copy():
        return pltpu.make_async_copy(out_ref.at[plane], x.at[0, s], z_recv.at[0])

    def y_copy(j):
        return remote(x.at[j, s], x.at[j, s], y_send.at[j], y_recv.at[j], neighbour)

    def y_arrival(j):
        return remote(x.at[j, cross_s], x.at[j, cross_s], y_send.at[j], y_recv.at[j], neighbour)

    def p_copy(j, k, slot):
        return remote(x.at[j, slot], x.at[j, slot], p_send.at[j, k], p_recv.at[j, k], partner)

    def rp_copy(j, q, k, slot):
        cols = columns(q)
        return remote(
            x.at[j, slot, :, cols], pair.at[j, k, :, cols],
            rp_send.at[j, q, k], rp_recv.at[j, q, k], partner,
        )

    def ry_copy(j, q):
        cols = columns(q)
        return remote(
            x.at[j, cross_s, :, cols], cross.at[j, :, cols],
            ry_send.at[j, q], ry_recv.at[j, q], neighbour,
        )

    def rz_copy(j, q):
        cols, to = columns(q), xor(plane, j, planes)
        return remote(
            x.at[j, s, :, cols], ret_ref.at[plane, :, cols],
            rz_send.at[j, q], rz_recv.at[j, q], to * SHARDS + s,
        )

    def keep_copy(q):
        cols = columns(q)
        return pltpu.make_async_copy(x.at[0, s, :, cols], ret_ref.at[plane, :, cols], rz_send.at[0, q])

    own_copy().start()
    for distance in range(1, planes):
        for to in (plane + distance, plane - distance):
            @pl.when((to >= 0) & (to < planes))
            def _():
                mask = xor(plane, to, planes)
                remote(
                    out_ref.at[to], x.at[mask, s], z_send.at[mask], z_recv.at[mask], to * SHARDS + s
                ).start()
    loads = [
        pltpu.make_async_copy(gate_hbm.at[0], gate, w_sem.at[0]),
        pltpu.make_async_copy(up_hbm.at[0], up, w_sem.at[1]),
        pltpu.make_async_copy(down_hbm.at[0], down, w_sem.at[2]),
    ]
    for load in loads:
        load.start()

    def arrive(j):
        if j == 0:
            own_copy().wait()
        else:
            out_copy(j).wait_recv()
        y_copy(j).start()
        p_copy(j, 0, s).start()

    def gather(j):
        y_arrival(j).wait_recv()
        p_copy(j, 1, cross_s).start()
        p_copy(j, 0, partner_s).wait_recv()
        p_copy(j, 1, diag_s).wait_recv()

    def expand(j):
        @pl.loop(0, chunks)
        def _(q):
            cols = columns(q)
            part = x[j, :, :, cols].reshape(rows, tile)

            @pl.when(q == 0)
            def _():
                acc[...] = jnp.zeros_like(acc)

            acc[0] += jnp.dot(part, gate[cols, :], preferred_element_type=jnp.float32)
            acc[1] += jnp.dot(part, up[cols, :], preferred_element_type=jnp.float32)

        value = acc[0]
        hidden[...] = (value / (1.0 + jnp.exp(-value)) * acc[1]).astype(hidden.dtype)

    def contract(j):
        y_copy(j).wait_send()
        p_copy(j, 0, s).wait_send()
        p_copy(j, 1, cross_s).wait_send()

        @pl.loop(0, chunks + 1)
        def _(q):
            @pl.when(q < chunks)
            def _():
                cols = columns(q)
                part = jnp.dot(hidden[...], down[:, cols], preferred_element_type=jnp.float32)
                x[j, :, :, cols] = part.astype(x.dtype).reshape(SHARDS, cap, tile)
                rp_copy(j, q, 1 - row, diag_s).start()
                rp_copy(j, q, row, partner_s).start()

            @pl.when(q > 0)
            def _():
                cols = columns(q - 1)
                rp_copy(j, q - 1, 1 - row, diag_s).wait_recv()
                total = x[j, cross_s, :, cols].astype(jnp.float32)
                total += pair[j, 1 - row, :, cols].astype(jnp.float32)
                x[j, cross_s, :, cols] = total.astype(x.dtype)
                ry_copy(j, q - 1).start()

    def finish(j):
        @pl.loop(0, chunks)
        def _(q):
            cols = columns(q)
            rp_copy(j, q, row, partner_s).wait_recv()
            total = x[j, s, :, cols].astype(jnp.float32) + pair[j, row, :, cols].astype(jnp.float32)
            ry_copy(j, q).wait_recv()
            x[j, s, :, cols] = (total + cross[j, :, cols].astype(jnp.float32)).astype(x.dtype)
            if j > 0:
                rz_copy(j, q).start()
            else:
                keep_copy(q).start()

    order = [0, *range(2, planes), 1]
    arrive(0)
    arrive(1)
    for i, j in enumerate(order):
        gather(j)
        if 0 < i < planes - 2:
            arrive(order[i + 1])
        if i == 0:
            for load in loads:
                load.wait()
        expand(j)
        contract(j)
        if i == 0:
            arrive(order[1])
        else:
            finish(order[i - 1])
    finish(order[-1])

    for j in range(planes):
        @pl.loop(0, chunks)
        def _(q):
            rp_copy(j, q, 1 - row, diag_s).wait_send()
            rp_copy(j, q, row, partner_s).wait_send()
            ry_copy(j, q).wait_send()
            if j > 0:
                rz_copy(j, q).wait()
            else:
                keep_copy(q).wait()
        if j > 0:
            out_copy(j).wait_send()


def routed_kernel(
    tokens, ids, levels, gate_hbm, up_hbm, down_hbm, out_hbm,
    x, gate, up, down, acc, hidden, pair, cross, raw, raw_y, raw_f,
    near_stage, near_ret, outer_ret, far_ret, table, picks, mix,
    w_sem, raw_sem, out_sem, table_send, table_recv,
    cross_send, cross_recv, far_send, far_recv, near_send, near_recv,
    fwd_send, fwd_recv, y_send, y_recv, d_send, d_recv,
    rp_send, rp_recv, ry_send, ry_recv,
    nr_send, nr_recv, or_send, or_recv, fr_send, fr_recv,
    pair_free, cross_free,
):
    me = lax.axis_index("expert")
    plane, s = me // SHARDS, me % SHARDS
    core, row = s % 2, s // 2
    half, near_plane = plane // 2, xor(plane, 1, 4)
    far_plane = 2 * (1 - half) + half
    kind = (plane + half + 1) % 2
    inner, outer = kind == 0, kind == 1
    cross_s = (1 - row) * 2 + core
    partner_s = row * 2 + (1 - core)
    diag_s = (1 - row) * 2 + (1 - core)
    partner, neighbour = plane * SHARDS + partner_s, plane * SHARDS + cross_s
    near, far = near_plane * SHARDS + s, far_plane * SHARDS + s
    far_b = xor(far_plane, 1, 4) * SHARDS + s
    cap, width = x.shape[2], x.shape[3]
    tok_rows = raw.shape[0]
    rows = SHARDS * cap
    tile = tile_of(width, 1024)
    chunks = width // tile
    own_j, near_j = 0, 1

    def columns(q):
        return pl.ds(pl.multiple_of(q * tile, tile), tile)

    def remote(src, dst, send, recv, device):
        return pltpu.make_async_remote_copy(
            src_ref=src, dst_ref=dst, send_sem=send, recv_sem=recv,
            device_id={"expert": device}, device_id_type=MESH,
        )

    def each(body):
        pl.loop(0, chunks)(body)

    raw_load = pltpu.make_async_copy(tokens, raw, raw_sem)
    loads = [
        pltpu.make_async_copy(gate_hbm.at[0], gate, w_sem.at[0]),
        pltpu.make_async_copy(up_hbm.at[0], up, w_sem.at[1]),
        pltpu.make_async_copy(down_hbm.at[0], down, w_sem.at[2]),
    ]
    raw_load.start()

    barrier = pltpu.get_barrier_semaphore()
    peers = [partner, neighbour, near, far]
    for peer in peers:
        pl.semaphore_signal(barrier, inc=1, device_id={"expert": peer}, device_id_type=MESH)

    @pl.when(inner)
    def _():
        pl.semaphore_signal(barrier, inc=1, device_id={"expert": far_b}, device_id_type=MESH)

    lane = lax.broadcasted_iota(jnp.int32, (tok_rows, tok_rows), 1)
    line = lax.broadcasted_iota(jnp.int32, (tok_rows, tok_rows), 0)
    expert_of = lax.broadcasted_iota(jnp.int32, (8, tok_rows), 0)
    first, second = ids[0:1, :] == expert_of, ids[1:2, :] == expert_of
    level_0, level_1 = levels[0:1, :].astype(jnp.float32), levels[1:2, :].astype(jnp.float32)
    named = jnp.where(first | second, 1.0, 0.0)
    earlier = jnp.where(line < lane, 1.0, 0.0).astype(jnp.bfloat16)
    rank = jnp.dot(named.astype(jnp.bfloat16), earlier, preferred_element_type=jnp.float32)
    share = jnp.where(first, level_0 / (level_0 + level_1), 0.0)
    share += jnp.where(second, level_1 / (level_0 + level_1), 0.0)
    table[0, 0:8, :] = jnp.where(named > 0.0, rank, 2.0 * tok_rows)
    table[0, 8:16, :] = share

    def matches(k, expert):
        spot = lax.broadcasted_iota(jnp.int32, (cap, tok_rows), 0).astype(jnp.float32)
        return table[k, pl.ds(expert, 1), :] == spot

    def set_pick(k):
        for i, expert in enumerate((plane, near_plane)):
            pick = jnp.where(matches(k, expert), 1.0, 0.0)
            picks[k, i * cap:(i + 1) * cap, :] = pick.astype(picks.dtype)

    def set_mix(k, spot):
        parts = []
        for expert in (plane, near_plane):
            weight = table[k, pl.ds(8 + expert, 1), :]
            parts.append(jnp.where(matches(k, expert), weight, 0.0))
        weight = jnp.transpose(jnp.concatenate(parts, axis=0))
        high = weight.astype(jnp.bfloat16)
        mix[spot, 0] = high
        mix[spot, 1] = (weight - high.astype(jnp.float32)).astype(jnp.bfloat16)

    def select(k, block):
        return jnp.dot(picks[k], block, preferred_element_type=jnp.float32).astype(x.dtype)

    def mixed(spot, own, other):
        both = jnp.concatenate([own, other], axis=0)
        total = jnp.dot(mix[spot, 0], both, preferred_element_type=jnp.float32)
        return total + jnp.dot(mix[spot, 1], both, preferred_element_type=jnp.float32)

    set_pick(0)
    set_mix(0, 0)
    with jax.named_scope("barrier"):
        pl.semaphore_wait(barrier, len(peers) + 1 - kind)

    table_y = remote(table.at[0], table.at[1], table_send.at[0], table_recv.at[0], neighbour)
    table_f = remote(table.at[0], table.at[3 - kind], table_send.at[1], table_recv.at[2 - kind], far)
    table_y.start()
    table_f.start()

    def table_arrival(k):
        return remote(table.at[0], table.at[k], table_send.at[0], table_recv.at[k - 1], far)

    def cross_copy(q):
        cols = columns(q)
        return remote(raw.at[:, cols], raw_y.at[:, cols], cross_send, cross_recv.at[q], neighbour)

    def far_copy(q, k):
        cols = columns(q)
        return remote(raw.at[:, cols], raw_f.at[k, :, cols], far_send, far_recv.at[k, q], far)

    def near_copy(k, q):
        cols, slot = columns(q), s if k == 0 else cross_s
        return remote(
            near_stage.at[k, :, cols], x.at[near_j, slot, :, cols],
            near_send.at[k], near_recv.at[k], near,
        )

    def fwd_copy(i, q):
        cols = columns(q)
        return remote(
            raw_f.at[i, pl.ds(0, cap), cols], x.at[2 + i, s, :, cols], fwd_send.at[i], fwd_recv.at[i, q], near
        )

    def y_copy(i, q):
        cols = columns(q)
        return remote(
            x.at[2 + i, s, :, cols], x.at[2 + i, s, :, cols], y_send.at[i], y_recv.at[i, q], neighbour
        )

    def y_arrival(i, q):
        cols = columns(q)
        return remote(
            x.at[2 + i, s, :, cols], x.at[2 + i, cross_s, :, cols],
            y_send.at[i], y_recv.at[i, q], neighbour,
        )

    def d_copy(j, r, q):
        cols, slot = columns(q), r * 2 + core
        return remote(
            x.at[j, slot, :, cols], x.at[j, slot, :, cols], d_send.at[j, r], d_recv.at[j, r], partner
        )

    def d_whole(j, r, lane_core):
        slot = r * 2 + lane_core
        return remote(x.at[j, slot], x.at[j, slot], d_send.at[j, r], d_recv.at[j, r], partner)

    def gathered(j):
        for r in range(2):
            d_whole(j, r, 1 - core).wait_recv()

    def rp_copy(j, t, q, k, slot):
        cols = columns(q)
        return remote(
            x.at[j, slot, :, cols], pair.at[t, k, :, cols],
            rp_send.at[j], rp_recv.at[t, q, k], partner,
        )

    def ry_copy(j, t, q):
        cols = columns(q)
        return remote(
            x.at[j, cross_s, :, cols], cross.at[t, :, cols],
            ry_send.at[j], ry_recv.at[t, q], neighbour,
        )

    def nr_copy(q):
        cols = columns(q)
        return remote(x.at[near_j, s, :, cols], near_ret.at[:, cols], nr_send, nr_recv.at[q], near)

    def or_copy(i, q):
        cols = columns(q)
        return remote(
            x.at[2 + i, s, :, cols], outer_ret.at[i, :, cols], or_send.at[i], or_recv.at[i, q], near
        )

    def fr_copy(i, q):
        cols = columns(q)
        return remote(
            raw_f.at[i, :, cols], far_ret.at[:, cols], fr_send.at[i], fr_recv.at[q],
            far_b if i == 0 else far,
        )

    def out_copy(q):
        cols = columns(q)
        return pltpu.make_async_copy(raw.at[:, cols], out_hbm.at[:, cols], out_sem)

    def expand(j, spot):
        @each
        def _(q):
            cols = columns(q)
            part = x[j, :, :, cols].reshape(rows, tile)

            @pl.when(q == 0)
            def _():
                acc[...] = jnp.zeros_like(acc)

            acc[0] += jnp.dot(part, gate[cols, :], preferred_element_type=jnp.float32)
            acc[1] += jnp.dot(part, up[cols, :], preferred_element_type=jnp.float32)

        value = acc[0]
        hidden[spot] = (value / (1.0 + jnp.exp(-value)) * acc[1]).astype(hidden.dtype)

    def contract(j, t, spot, credit, also):
        for r in range(2):
            d_whole(j, r, core).wait_send()
        if j >= 2:
            remote(x.at[j, s], x.at[j, s], y_send.at[j - 2], d_recv.at[j, 0], neighbour).wait_send()
        if credit:
            pl.semaphore_wait(pair_free, 1)
            pl.semaphore_wait(cross_free, 1)

        @pl.loop(0, chunks + 1)
        def _(q):
            @pl.when(q < chunks)
            def _():
                cols = columns(q)
                part = jnp.dot(hidden[spot], down[:, cols], preferred_element_type=jnp.float32)
                x[j, :, :, cols] = part.astype(x.dtype).reshape(SHARDS, cap, tile)
                rp_copy(j, t, q, 1 - row, diag_s).start()
                rp_copy(j, t, q, row, partner_s).start()
                for step in also:
                    step(q)

            @pl.when(q > 0)
            def _():
                cols = columns(q - 1)
                rp_copy(j, t, q - 1, 1 - row, diag_s).wait_recv()
                total = x[j, cross_s, :, cols].astype(jnp.float32)
                total += pair[t, 1 - row, :, cols].astype(jnp.float32)
                x[j, cross_s, :, cols] = total.astype(x.dtype)
                ry_copy(j, t, q - 1).start()

    def finish(j, t):
        def step(q):
            cols = columns(q)
            rp_copy(j, t, q, row, partner_s).wait_recv()
            total = x[j, s, :, cols].astype(jnp.float32) + pair[t, row, :, cols].astype(jnp.float32)
            ry_copy(j, t, q).wait_recv()
            x[j, s, :, cols] = (total + cross[t, :, cols].astype(jnp.float32)).astype(x.dtype)
            if j >= 2:
                @pl.when(outer)
                def _():
                    or_copy(j - 2, q).start()
            elif j == near_j:
                nr_copy(q).start()

        return step

    def release():
        pl.semaphore_signal(pair_free, inc=1, device_id={"expert": partner}, device_id_type=MESH)
        pl.semaphore_signal(cross_free, inc=1, device_id={"expert": neighbour}, device_id_type=MESH)

    def sent(src, dst, send):
        remote(src, dst, send, nr_recv.at[0], near).wait_send()

    def merge(i):
        def step(q):
            @pl.when(inner)
            def _():
                cols = columns(q)

                @pl.when(q == 0)
                def _():
                    sent(raw_f.at[i, pl.ds(0, cap)], near_ret, fwd_send.at[i])
                    if i == 0:
                        sent(near_stage.at[1], near_ret, near_send.at[1])

                or_copy(i, q).wait_recv()
                total = mixed(1 + i, x[2 + i, s, :, cols], outer_ret[i, :, cols])
                raw_f[i, :, cols] = total.astype(raw_f.dtype)
                fr_copy(i, q).start()

        return step

    def lagged(i):
        def step(q):
            pl.when(q >= 2)(lambda: merge(i)(q - 2))

        return step

    def merge_rest(i):
        pl.loop(chunks - 2, chunks)(merge(i))

    def enter(i, q):
        cols = columns(q)

        @pl.when(inner)
        def _():
            with jax.named_scope("w_far"):
                far_copy(q, i).wait_recv()
            taken = select(2 + i, raw_f[i, :, cols])
            x[2 + i, s, :, cols] = taken[:cap]
            raw_f[i, 0:cap, cols] = taken[cap:]
            fwd_copy(i, q).start()

        @pl.when(outer)
        def _():
            with jax.named_scope("w_fwd"):
                fwd_copy(i, q).wait_recv()

        y_copy(i, q).start()
        d_copy(2 + i, row, q).start()

    def far_table(i):
        @pl.when(inner)
        def _():
            table_arrival(2 + i).wait_recv()
            set_pick(2 + i)
            set_mix(2 + i, 1 + i)

    with jax.named_scope("w_raw"):
        raw_load.wait()
    each(lambda q: cross_copy(q).start())
    each(lambda q: far_copy(q, 1 - kind).start())
    for load in loads:
        load.start()

    with jax.named_scope("take_own"):
        @each
        def _(q):
            cols = columns(q)
            taken = select(0, raw[:, cols])
            near_stage[0, :, cols] = taken[cap:]
            x[own_j, s, :, cols] = taken[:cap]
            d_copy(own_j, row, q).start()

            @pl.when(outer | (q < 2))
            def _():
                near_copy(0, q).start()

    with jax.named_scope("tables"):
        table_arrival(1).wait_recv()
        set_pick(1)

        far_table(0)

    with jax.named_scope("enter_b"):
        @each
        def _(q):
            cols = columns(q)
            with jax.named_scope("w_cross"):
                cross_copy(q).wait_recv()
            taken = select(1, raw_y[:, cols])
            near_stage[1, :, cols] = taken[cap:]
            x[own_j, cross_s, :, cols] = taken[:cap]
            d_copy(own_j, 1 - row, q).start()
            enter(0, q)

            pl.when(outer)(lambda: near_copy(1, q).start())
            pl.when(inner & (q % 2 == 1))(lambda: near_copy(0, 2 + q // 2).start())

    with jax.named_scope("wait_own"):
        loads[0].wait()
        loads[1].wait()
        gathered(own_j)
    with jax.named_scope("expand_own"):
        expand(own_j, 0)

    def enter_a(q):
        enter(1, q)
        y_arrival(0, q).wait_recv()
        d_copy(2, 1 - row, q).start()
        late = 2 + chunks // 2 + q // 2

        @pl.when(inner & (q % 2 == 1) & (late < chunks))
        def _():
            near_copy(0, late).start()

    middle = chunks // 2 + 1
    with jax.named_scope("enter_a"):
        far_table(1)
        pl.loop(0, middle)(enter_a)

        @pl.loop(middle, chunks)
        def _(q):
            y_arrival(0, q).wait_recv()
            d_copy(2, 1 - row, q).start()

    with jax.named_scope("wait_b"):
        gathered(2)
    with jax.named_scope("expand_b"):
        expand(2, 1)
    with jax.named_scope("enter_a2"):
        @pl.loop(middle, chunks)
        def _(q):
            enter(1, q)
            late = 2 + chunks // 2 + q // 2

            @pl.when(inner & (q % 2 == 1) & (late < chunks))
            def _():
                near_copy(0, late).start()

        pl.when(inner)(lambda: each(lambda q: near_copy(1, q).start()))

    loads[2].wait()
    with jax.named_scope("contract_b"):
        contract(2, 0, 1, False, ())

    with jax.named_scope("wait_a"):
        @each
        def _(q):
            y_arrival(1, q).wait_recv()
            d_copy(3, 1 - row, q).start()

        gathered(3)
    with jax.named_scope("expand_a"):
        expand(3, 1)
    with jax.named_scope("contract_a"):
        contract(3, 1, 1, False, (finish(2, 0), lagged(0)))
        release()
    with jax.named_scope("merge_b"):
        merge_rest(0)

    with jax.named_scope("wait_near"):
        for k, r in ((0, row), (1, 1 - row)):
            slot = r * 2 + core
            remote(near_stage.at[k], x.at[near_j, slot], near_send.at[k], near_recv.at[k], near).wait_recv()
            d_whole(near_j, r, core).start()

        gathered(near_j)
    with jax.named_scope("expand_near"):
        expand(near_j, 1)
    with jax.named_scope("contract_near"):
        contract(near_j, 0, 1, True, (finish(3, 1), lagged(1)))
        release()
    with jax.named_scope("merge_a"):
        merge_rest(1)
    with jax.named_scope("contract_own"):
        contract(own_j, 1, 0, True, (finish(near_j, 0),))

    with jax.named_scope("combine"):
        remote(raw, raw_y, cross_send, cross_recv.at[0], neighbour).wait_send()
        remote(raw, raw_y, far_send, cross_recv.at[0], neighbour).wait_send()

        @each
        def _(q):
            cols = columns(q)
            with jax.named_scope("w_own"):
                finish(own_j, 1)(q)
            with jax.named_scope("w_nr"):
                nr_copy(q).wait_recv()
            with jax.named_scope("w_fr"):
                fr_copy(0, q).wait_recv()
            total = mixed(0, x[own_j, s, :, cols], near_ret[:, cols])
            raw[:, cols] = (total + far_ret[:, cols].astype(jnp.float32)).astype(raw.dtype)
            out_copy(q).start()

    with jax.named_scope("tail_sends"):
        table_y.wait_send()
        table_f.wait_send()
        sent(near_stage.at[0], near_ret, near_send.at[0])
        sent(x.at[near_j, s], near_ret, nr_send)
        for j in range(4):
            sent(x.at[j, pl.ds(0, 2)], pair.at[0], rp_send.at[j])
            sent(x.at[j, cross_s], near_ret, ry_send.at[j])

        @pl.when(inner)
        def _():
            for i in range(2):
                sent(raw_f.at[i], far_ret, fr_send.at[i])

        @pl.when(outer)
        def _():
            sent(near_stage.at[1], near_ret, near_send.at[1])
            for i in range(2):
                sent(x.at[2 + i, s], near_ret, or_send.at[i])

    with jax.named_scope("tail_out"):
        pltpu.make_async_copy(raw, out_hbm, out_sem).wait()


def routed(tokens, route_ids, levels, w_gate, w_up, w_down, cap):
    tok_rows, width = tokens.shape
    ff, dtype = w_gate.shape[2], tokens.dtype
    rows, chunks = SHARDS * cap, width // tile_of(width, 1024)
    dma, vmem = pltpu.SemaphoreType.DMA, pltpu.VMEM
    anywhere, local = pl.BlockSpec(memory_space=pl.ANY), pl.BlockSpec(memory_space=pltpu.VMEM)
    return pl.pallas_call(
        routed_kernel,
        out_shape=jax.ShapeDtypeStruct((tok_rows, width), dtype),
        in_specs=[anywhere, local, local, anywhere, anywhere, anywhere],
        out_specs=anywhere,
        scratch_shapes=[
            vmem((4, SHARDS, cap, width), dtype),
            vmem((width, ff), dtype),
            vmem((width, ff), dtype),
            vmem((ff, width), dtype),
            vmem((2, rows, ff), jnp.float32),
            vmem((2, rows, ff), dtype),
            vmem((2, 2, cap, width), dtype),
            vmem((2, cap, width), dtype),
            vmem((tok_rows, width), dtype),
            vmem((tok_rows, width), dtype),
            vmem((2, tok_rows, width), dtype),
            vmem((2, cap, width), dtype),
            vmem((cap, width), dtype),
            vmem((2, cap, width), dtype),
            vmem((tok_rows, width), dtype),
            vmem((4, 16, tok_rows), jnp.float32),
            vmem((4, 2 * cap, tok_rows), dtype),
            vmem((3, 2, tok_rows, 2 * cap), dtype),
            dma((3,)), dma, dma, dma((2,)), dma((3,)),
            dma, dma((chunks,)), dma, dma((2, chunks)),
            dma((2,)), dma((2,)),
            dma((2,)), dma((2, chunks)),
            dma((2,)), dma((2, chunks)),
            dma((4, 2)), dma((4, 2)),
            dma((4,)), dma((2, chunks, 2)),
            dma((4,)), dma((2, chunks)),
            dma, dma((chunks,)),
            dma((2,)), dma((2, chunks)),
            dma((2,)), dma((chunks,)),
            pltpu.SemaphoreType.REGULAR, pltpu.SemaphoreType.REGULAR,
        ],
        compiler_params=pltpu.CompilerParams(
            collective_id=0, has_side_effects=True, vmem_limit_bytes=67_000_000
        ),
    )(tokens, route_ids.T, levels.T, w_gate, w_up, w_down)


def combine_kernel(weight_ref, ret_ref, out_ref):
    weight = weight_ref[...]
    high = weight.astype(jnp.bfloat16)
    low = (weight - high.astype(jnp.float32)).astype(jnp.bfloat16)
    total = jnp.dot(high, ret_ref[...], preferred_element_type=jnp.float32)
    total += jnp.dot(low, ret_ref[...], preferred_element_type=jnp.float32)
    out_ref[...] = total.astype(out_ref.dtype)


def on_device(tokens, route_ids, levels, w_gate, w_up, w_down):
    tok_rows, width = tokens.shape
    top = route_ids.shape[1]
    ff = w_gate.shape[2]
    experts = lax.axis_size("expert") // SHARDS
    capacity = 5 * tok_rows * top // (4 * experts)
    cap = -(-capacity // 16) * 16
    slots = experts * cap
    dtype = tokens.dtype
    if experts == 4 and top == 2 and tok_rows < 2 * cap:
        return routed(tokens, route_ids, levels, w_gate, w_up, w_down, cap)

    chosen = route_ids[:, :, None] == jnp.arange(experts, dtype=jnp.int32)
    named = jnp.any(chosen, axis=1)
    index = jnp.arange(tok_rows, dtype=jnp.int32)
    earlier = (index[:, None] > index[None, :]).astype(jnp.bfloat16)
    rank = jnp.dot(earlier, named.astype(jnp.bfloat16), preferred_element_type=jnp.float32)
    place = jnp.where(named, rank.astype(jnp.int32), cap)
    level_f = levels.astype(jnp.float32)
    weights = level_f / jnp.sum(level_f, axis=1, keepdims=True)
    weight_e = jnp.sum(jnp.where(chosen, weights[:, :, None], 0.0), axis=1)
    spot = jnp.arange(cap, dtype=jnp.int32)
    pick = (place[:, :, None] == spot).reshape(tok_rows, slots)
    weight_m = jnp.where(pick, jnp.repeat(weight_e, cap, axis=1), 0.0)
    outgoing = lax.dot_general(
        pick.astype(dtype), tokens, (((0,), (0,)), ((), ())), preferred_element_type=jnp.float32
    ).astype(dtype).reshape(experts, cap, width)

    dma, anywhere = pltpu.SemaphoreType.DMA, pl.BlockSpec(memory_space=pl.ANY)
    rows, chunks = SHARDS * cap, width // tile_of(width, 1024)
    returned = pl.pallas_call(
        functools.partial(layer_kernel, experts),
        out_shape=jax.ShapeDtypeStruct((experts, cap, width), dtype),
        in_specs=[anywhere] * 4,
        out_specs=anywhere,
        scratch_shapes=[
            pltpu.VMEM((experts, SHARDS, cap, width), dtype),
            pltpu.VMEM((width, ff), dtype),
            pltpu.VMEM((width, ff), dtype),
            pltpu.VMEM((ff, width), dtype),
            pltpu.VMEM((2, rows, ff), jnp.float32),
            pltpu.VMEM((rows, ff), dtype),
            pltpu.VMEM((experts, 2, cap, width), dtype),
            pltpu.VMEM((experts, cap, width), dtype),
            dma((3,)),
            dma((experts,)), dma((experts,)),
            dma((experts,)), dma((experts,)),
            dma((experts, 2)), dma((experts, 2)),
            dma((experts, chunks, 2)), dma((experts, chunks, 2)),
            dma((experts, chunks)), dma((experts, chunks)),
            dma((experts, chunks)), dma((experts, chunks)),
        ],
        compiler_params=pltpu.CompilerParams(
            collective_id=0, has_side_effects=True, vmem_limit_bytes=67_000_000
        ),
    )(outgoing, w_gate, w_up, w_down)

    tile = tile_of(width, 1024)
    return pl.pallas_call(
        combine_kernel,
        out_shape=jax.ShapeDtypeStruct((tok_rows, width), dtype),
        grid=(width // tile,),
        in_specs=[
            pl.BlockSpec((tok_rows, slots), lambda n: (0, 0)),
            pl.BlockSpec((slots, tile), lambda n: (0, n)),
        ],
        out_specs=pl.BlockSpec((tok_rows, tile), lambda n: (0, n)),
    )(weight_m, returned.reshape(slots, width))


def solution(mesh):
    return jax.shard_map(
        on_device,
        mesh=mesh,
        in_specs=(
            P(("groups", "expert"), None),
            P(("groups", "expert"), None),
            P(("groups", "expert"), None),
            P("expert", None, None),
            P("expert", None, None),
            P("expert", None, None),
        ),
        out_specs=P(("groups", "expert"), None),
        check_vma=False,
    )
```

```python
import functools

import jax
import jax.numpy as jnp
from jax import lax
from jax.experimental import pallas as pl
from jax.experimental.pallas import tpu as pltpu
from jax.sharding import PartitionSpec as P

SHARDS = 4
MESH = pl.DeviceIdType.MESH


def tile_of(length, most):
    size = most
    while length % size:
        size //= 2
    return size


def xor(a, mask, count):
    total, bit = 0, 1
    while bit < count:
        total += (a // bit + mask // bit) % 2 * bit
        bit *= 2
    return total


def layer_kernel(
    planes, out_ref, gate_hbm, up_hbm, down_hbm, ret_ref,
    x, gate, up, down, acc, hidden, pair, cross,
    w_sem, z_send, z_recv, y_send, y_recv, p_send, p_recv,
    rp_send, rp_recv, ry_send, ry_recv, rz_send, rz_recv,
):
    me = lax.axis_index("expert")
    plane, s = me // SHARDS, me % SHARDS
    base = plane * SHARDS
    core, row = s % 2, s // 2
    partner_s = row * 2 + (1 - core)
    cross_s = (1 - row) * 2 + core
    diag_s = (1 - row) * 2 + (1 - core)
    partner, neighbour = base + partner_s, base + cross_s
    cap, width = x.shape[2], x.shape[3]
    rows = SHARDS * cap
    tile = tile_of(width, 1024)
    chunks = width // tile

    barrier = pltpu.get_barrier_semaphore()
    peers = [partner, neighbour]
    peers += [xor(plane, j, planes) * SHARDS + s for j in range(1, planes)]
    for peer in peers:
        pl.semaphore_signal(barrier, inc=1, device_id={"expert": peer}, device_id_type=MESH)
    pl.semaphore_wait(barrier, planes + 1)

    def remote(src, dst, send, recv, device):
        return pltpu.make_async_remote_copy(
            src_ref=src, dst_ref=dst, send_sem=send, recv_sem=recv,
            device_id={"expert": device}, device_id_type=MESH,
        )

    def columns(q):
        return pl.ds(pl.multiple_of(q * tile, tile), tile)

    def out_copy(j):
        to = xor(plane, j, planes)
        return remote(out_ref.at[to], x.at[j, s], z_send.at[j], z_recv.at[j], to * SHARDS + s)

    def own_copy():
        return pltpu.make_async_copy(out_ref.at[plane], x.at[0, s], z_recv.at[0])

    def y_copy(j):
        return remote(x.at[j, s], x.at[j, s], y_send.at[j], y_recv.at[j], neighbour)

    def y_arrival(j):
        return remote(x.at[j, cross_s], x.at[j, cross_s], y_send.at[j], y_recv.at[j], neighbour)

    def p_copy(j, k, slot):
        return remote(x.at[j, slot], x.at[j, slot], p_send.at[j, k], p_recv.at[j, k], partner)

    def rp_copy(j, q, k, slot):
        cols = columns(q)
        return remote(
            x.at[j, slot, :, cols], pair.at[j, k, :, cols],
            rp_send.at[j, q, k], rp_recv.at[j, q, k], partner,
        )

    def ry_copy(j, q):
        cols = columns(q)
        return remote(
            x.at[j, cross_s, :, cols], cross.at[j, :, cols],
            ry_send.at[j, q], ry_recv.at[j, q], neighbour,
        )

    def rz_copy(j, q):
        cols, to = columns(q), xor(plane, j, planes)
        return remote(
            x.at[j, s, :, cols], ret_ref.at[plane, :, cols],
            rz_send.at[j, q], rz_recv.at[j, q], to * SHARDS + s,
        )

    def keep_copy(q):
        cols = columns(q)
        return pltpu.make_async_copy(x.at[0, s, :, cols], ret_ref.at[plane, :, cols], rz_send.at[0, q])

    own_copy().start()
    for distance in range(1, planes):
        for to in (plane + distance, plane - distance):
            @pl.when((to >= 0) & (to < planes))
            def _():
                mask = xor(plane, to, planes)
                remote(
                    out_ref.at[to], x.at[mask, s], z_send.at[mask], z_recv.at[mask], to * SHARDS + s
                ).start()
    loads = [
        pltpu.make_async_copy(gate_hbm.at[0], gate, w_sem.at[0]),
        pltpu.make_async_copy(up_hbm.at[0], up, w_sem.at[1]),
        pltpu.make_async_copy(down_hbm.at[0], down, w_sem.at[2]),
    ]
    for load in loads:
        load.start()

    def arrive(j):
        if j == 0:
            own_copy().wait()
        else:
            out_copy(j).wait_recv()
        y_copy(j).start()
        p_copy(j, 0, s).start()

    def gather(j):
        y_arrival(j).wait_recv()
        p_copy(j, 1, cross_s).start()
        p_copy(j, 0, partner_s).wait_recv()
        p_copy(j, 1, diag_s).wait_recv()

    def expand(j):
        @pl.loop(0, chunks)
        def _(q):
            cols = columns(q)
            part = x[j, :, :, cols].reshape(rows, tile)

            @pl.when(q == 0)
            def _():
                acc[...] = jnp.zeros_like(acc)

            acc[0] += jnp.dot(part, gate[cols, :], preferred_element_type=jnp.float32)
            acc[1] += jnp.dot(part, up[cols, :], preferred_element_type=jnp.float32)

        value = acc[0]
        hidden[...] = (value / (1.0 + jnp.exp(-value)) * acc[1]).astype(hidden.dtype)

    def contract(j):
        y_copy(j).wait_send()
        p_copy(j, 0, s).wait_send()
        p_copy(j, 1, cross_s).wait_send()

        @pl.loop(0, chunks + 1)
        def _(q):
            @pl.when(q < chunks)
            def _():
                cols = columns(q)
                part = jnp.dot(hidden[...], down[:, cols], preferred_element_type=jnp.float32)
                x[j, :, :, cols] = part.astype(x.dtype).reshape(SHARDS, cap, tile)
                rp_copy(j, q, 1 - row, diag_s).start()
                rp_copy(j, q, row, partner_s).start()

            @pl.when(q > 0)
            def _():
                cols = columns(q - 1)
                rp_copy(j, q - 1, 1 - row, diag_s).wait_recv()
                total = x[j, cross_s, :, cols].astype(jnp.float32)
                total += pair[j, 1 - row, :, cols].astype(jnp.float32)
                x[j, cross_s, :, cols] = total.astype(x.dtype)
                ry_copy(j, q - 1).start()

    def finish(j):
        @pl.loop(0, chunks)
        def _(q):
            cols = columns(q)
            rp_copy(j, q, row, partner_s).wait_recv()
            total = x[j, s, :, cols].astype(jnp.float32) + pair[j, row, :, cols].astype(jnp.float32)
            ry_copy(j, q).wait_recv()
            x[j, s, :, cols] = (total + cross[j, :, cols].astype(jnp.float32)).astype(x.dtype)
            if j > 0:
                rz_copy(j, q).start()
            else:
                keep_copy(q).start()

    order = [0, *range(2, planes), 1]
    arrive(0)
    arrive(1)
    for i, j in enumerate(order):
        gather(j)
        if 0 < i < planes - 2:
            arrive(order[i + 1])
        if i == 0:
            for load in loads:
                load.wait()
        expand(j)
        contract(j)
        if i == 0:
            arrive(order[1])
        else:
            finish(order[i - 1])
    finish(order[-1])

    for j in range(planes):
        @pl.loop(0, chunks)
        def _(q):
            rp_copy(j, q, 1 - row, diag_s).wait_send()
            rp_copy(j, q, row, partner_s).wait_send()
            ry_copy(j, q).wait_send()
            if j > 0:
                rz_copy(j, q).wait()
            else:
                keep_copy(q).wait()
        if j > 0:
            out_copy(j).wait_send()


def routed_kernel(
    tokens, ids, levels, gate_hbm, up_hbm, down_hbm, out_hbm,
    x, gate, up, down, acc, hidden, pair, cross, raw, raw_y, raw_f,
    near_stage, near_ret, near_cross, outer_ret, far_ret, table, picks, mix,
    w_sem, raw_sem, out_sem, table_send, table_recv,
    cross_send, cross_recv, far_send, far_recv, near_send, near_recv,
    fwd_send, fwd_recv, y_send, y_recv, d_send, d_recv,
    rp_send, rp_recv, ry_send, ry_recv,
    nr_send, nr_recv, or_send, or_recv, fr_send, fr_recv,
    nx_send, nx_recv, fin_send, fin_recv,
    pair_free, cross_free,
):
    me = lax.axis_index("expert")
    plane, s = me // SHARDS, me % SHARDS
    core, row = s % 2, s // 2
    half, near_plane = plane // 2, xor(plane, 1, 4)
    far_plane = 2 * (1 - half) + half
    kind = (plane + half + 1) % 2
    inner, outer = kind == 0, kind == 1
    cross_s = (1 - row) * 2 + core
    partner_s = row * 2 + (1 - core)
    diag_s = (1 - row) * 2 + (1 - core)
    partner, neighbour = plane * SHARDS + partner_s, plane * SHARDS + cross_s
    near, far = near_plane * SHARDS + s, far_plane * SHARDS + s
    far_b = xor(far_plane, 1, 4) * SHARDS + s
    cap, width = x.shape[2], x.shape[3]
    tok_rows = raw.shape[0]
    rows = SHARDS * cap
    tile = tile_of(width, 1024)
    chunks = width // tile
    own_j, near_j = 0, 1
    folds = near_cross.shape[0]

    def columns(q):
        return pl.ds(pl.multiple_of(q * tile, tile), tile)

    def remote(src, dst, send, recv, device):
        return pltpu.make_async_remote_copy(
            src_ref=src, dst_ref=dst, send_sem=send, recv_sem=recv,
            device_id={"expert": device}, device_id_type=MESH,
        )

    def each(body):
        pl.loop(0, chunks)(body)

    raw_load = pltpu.make_async_copy(tokens, raw, raw_sem)
    loads = [
        pltpu.make_async_copy(gate_hbm.at[0], gate, w_sem.at[0]),
        pltpu.make_async_copy(up_hbm.at[0], up, w_sem.at[1]),
        pltpu.make_async_copy(down_hbm.at[0], down, w_sem.at[2]),
    ]
    raw_load.start()

    barrier = pltpu.get_barrier_semaphore()
    peers = [partner, neighbour, near, far]
    for peer in peers:
        pl.semaphore_signal(barrier, inc=1, device_id={"expert": peer}, device_id_type=MESH)

    @pl.when(inner)
    def _():
        pl.semaphore_signal(barrier, inc=1, device_id={"expert": far_b}, device_id_type=MESH)

    lane = lax.broadcasted_iota(jnp.int32, (tok_rows, tok_rows), 1)
    line = lax.broadcasted_iota(jnp.int32, (tok_rows, tok_rows), 0)
    expert_of = lax.broadcasted_iota(jnp.int32, (8, tok_rows), 0)
    first, second = ids[0:1, :] == expert_of, ids[1:2, :] == expert_of
    level_0, level_1 = levels[0:1, :].astype(jnp.float32), levels[1:2, :].astype(jnp.float32)
    named = jnp.where(first | second, 1.0, 0.0)
    earlier = jnp.where(line < lane, 1.0, 0.0).astype(jnp.bfloat16)
    rank = jnp.dot(named.astype(jnp.bfloat16), earlier, preferred_element_type=jnp.float32)
    share = jnp.where(first, level_0 / (level_0 + level_1), 0.0)
    share += jnp.where(second, level_1 / (level_0 + level_1), 0.0)
    table[0, 0:8, :] = jnp.where(named > 0.0, rank, 2.0 * tok_rows)
    table[0, 8:16, :] = share

    def matches(k, expert):
        spot = lax.broadcasted_iota(jnp.int32, (cap, tok_rows), 0).astype(jnp.float32)
        return table[k, pl.ds(expert, 1), :] == spot

    def set_pick(k):
        for i, expert in enumerate((plane, near_plane)):
            pick = jnp.where(matches(k, expert), 1.0, 0.0)
            picks[k, i * cap:(i + 1) * cap, :] = pick.astype(picks.dtype)

    def set_mix(k, spot):
        parts = []
        for expert in (plane, near_plane):
            weight = table[k, pl.ds(8 + expert, 1), :]
            parts.append(jnp.where(matches(k, expert), weight, 0.0))
        weight = jnp.transpose(jnp.concatenate(parts, axis=0))
        high = weight.astype(jnp.bfloat16)
        mix[spot, 0] = high
        mix[spot, 1] = (weight - high.astype(jnp.float32)).astype(jnp.bfloat16)

    def select(k, block):
        return jnp.dot(picks[k], block, preferred_element_type=jnp.float32).astype(x.dtype)

    def mixed(spot, own, other):
        both = jnp.concatenate([own, other], axis=0)
        total = jnp.dot(mix[spot, 0], both, preferred_element_type=jnp.float32)
        return total + jnp.dot(mix[spot, 1], both, preferred_element_type=jnp.float32)

    set_pick(0)
    set_mix(0, 0)
    with jax.named_scope("barrier"):
        pl.semaphore_wait(barrier, len(peers) + 1 - kind)

    table_y = remote(table.at[0], table.at[1], table_send.at[0], table_recv.at[0], neighbour)
    table_f = remote(table.at[0], table.at[3 - kind], table_send.at[1], table_recv.at[2 - kind], far)
    table_y.start()
    table_f.start()

    def table_arrival(k):
        return remote(table.at[0], table.at[k], table_send.at[0], table_recv.at[k - 1], far)

    def cross_copy(q):
        cols = columns(q)
        return remote(raw.at[:, cols], raw_y.at[:, cols], cross_send, cross_recv.at[q], neighbour)

    def far_copy(q, k):
        cols = columns(q)
        return remote(raw.at[:, cols], raw_f.at[k, :, cols], far_send, far_recv.at[k, q], far)

    def near_copy(k, q):
        cols, slot = columns(q), s if k == 0 else cross_s
        return remote(
            near_stage.at[k, :, cols], x.at[near_j, slot, :, cols],
            near_send.at[k], near_recv.at[k], near,
        )

    def fwd_copy(i, q):
        cols = columns(q)
        return remote(
            raw_f.at[i, pl.ds(0, cap), cols], x.at[2 + i, s, :, cols], fwd_send.at[i], fwd_recv.at[i, q], near
        )

    def y_copy(i, q):
        cols = columns(q)
        return remote(
            x.at[2 + i, s, :, cols], x.at[2 + i, s, :, cols], y_send.at[i], y_recv.at[i, q], neighbour
        )

    def y_arrival(i, q):
        cols = columns(q)
        return remote(
            x.at[2 + i, s, :, cols], x.at[2 + i, cross_s, :, cols],
            y_send.at[i], y_recv.at[i, q], neighbour,
        )

    def d_copy(j, r, q):
        cols, slot = columns(q), r * 2 + core
        return remote(
            x.at[j, slot, :, cols], x.at[j, slot, :, cols], d_send.at[j, r], d_recv.at[j, r], partner
        )

    def d_whole(j, r, lane_core):
        slot = r * 2 + lane_core
        return remote(x.at[j, slot], x.at[j, slot], d_send.at[j, r], d_recv.at[j, r], partner)

    def gathered(j):
        for r in range(2):
            d_whole(j, r, 1 - core).wait_recv()

    def rp_copy(j, t, q, k, slot):
        cols = columns(q)
        return remote(
            x.at[j, slot, :, cols], pair.at[t, k, :, cols],
            rp_send.at[j], rp_recv.at[t, q, k], partner,
        )

    def ry_copy(j, t, q):
        cols = columns(q)
        return remote(
            x.at[j, cross_s, :, cols], cross.at[t, :, cols],
            ry_send.at[j], ry_recv.at[t, q], neighbour,
        )

    def nr_copy(q):
        cols = columns(q)
        return remote(x.at[near_j, s, :, cols], near_ret.at[:, cols], nr_send, nr_recv.at[q], near)

    def or_copy(i, q):
        cols = columns(q)
        return remote(
            x.at[2 + i, s, :, cols], outer_ret.at[i, :, cols], or_send.at[i], or_recv.at[i, q], near
        )

    def fr_copy(i, q):
        cols = columns(q)
        return remote(
            raw_f.at[i, :, cols], far_ret.at[:, cols], fr_send.at[i], fr_recv.at[q],
            far_b if i == 0 else far,
        )

    def out_copy(q):
        cols = columns(q)
        return pltpu.make_async_copy(raw.at[:, cols], out_hbm.at[:, cols], out_sem)

    def folded(q):
        return (q >= 2) & (q < 2 + folds)

    def nx_copy(q):
        return remote(
            x.at[near_j, cross_s, :, columns(q)], near_cross.at[q - 2], nx_send, nx_recv.at[q - 2], near
        )

    def fin_copy(q):
        return remote(
            raw_y.at[:, columns(q)], raw_y.at[:, columns((q + folds) % chunks)],
            fin_send, fin_recv.at[q - 2], neighbour,
        )

    def fold(q):
        cols = columns(q)
        with jax.named_scope("w_nx"):
            nx_copy(q).wait_recv()
        total = mixed(3, x[own_j, cross_s, :, cols], near_cross[q - 2])
        raw_y[:, cols] = total.astype(raw_y.dtype)
        fin_copy(q).start()

    def expand(j, spot, also=()):
        @each
        def _(q):
            cols = columns(q)
            part = x[j, :, :, cols].reshape(rows, tile)

            @pl.when(q == 0)
            def _():
                acc[...] = jnp.zeros_like(acc)

            acc[0] += jnp.dot(part, gate[cols, :], preferred_element_type=jnp.float32)
            acc[1] += jnp.dot(part, up[cols, :], preferred_element_type=jnp.float32)
            for step in also:
                step(q)

        value = acc[0]
        hidden[spot] = (value / (1.0 + jnp.exp(-value)) * acc[1]).astype(hidden.dtype)

    def contract(j, t, spot, credit, also):
        for r in range(2):
            d_whole(j, r, core).wait_send()
        if j >= 2:
            remote(x.at[j, s], x.at[j, s], y_send.at[j - 2], d_recv.at[j, 0], neighbour).wait_send()
        if credit:
            pl.semaphore_wait(pair_free, 1)
            pl.semaphore_wait(cross_free, 1)

        @pl.loop(0, chunks + 1)
        def _(q):
            @pl.when(q < chunks)
            def _():
                cols = columns(q)
                part = jnp.dot(hidden[spot], down[:, cols], preferred_element_type=jnp.float32)
                x[j, :, :, cols] = part.astype(x.dtype).reshape(SHARDS, cap, tile)
                rp_copy(j, t, q, 1 - row, diag_s).start()
                rp_copy(j, t, q, row, partner_s).start()
                for step in also:
                    step(q)

            @pl.when(q > 0)
            def _():
                cols = columns(q - 1)
                rp_copy(j, t, q - 1, 1 - row, diag_s).wait_recv()
                total = x[j, cross_s, :, cols].astype(jnp.float32)
                total += pair[t, 1 - row, :, cols].astype(jnp.float32)
                x[j, cross_s, :, cols] = total.astype(x.dtype)
                if j >= 2:
                    ry_copy(j, t, q - 1).start()
                else:
                    pl.when(~folded(q - 1))(lambda: ry_copy(j, t, q - 1).start())

                    @pl.when(folded(q - 1))
                    def _():
                        nx_copy(q - 1).start() if j == near_j else fold(q - 1)

    def finish(j, t):
        def step(q):
            cols = columns(q)
            with jax.named_scope("w_rp"):
                rp_copy(j, t, q, row, partner_s).wait_recv()
            total = x[j, s, :, cols].astype(jnp.float32) + pair[t, row, :, cols].astype(jnp.float32)

            def whole():
                with jax.named_scope("w_ry"):
                    ry_copy(j, t, q).wait_recv()
                x[j, s, :, cols] = (total + cross[t, :, cols].astype(jnp.float32)).astype(x.dtype)

            def column_sum():
                x[j, s, :, cols] = total.astype(x.dtype)

            if j >= 2:
                whole()
            else:
                pl.when(~folded(q))(whole)
                pl.when(folded(q))(column_sum)
            if j >= 2:
                @pl.when(outer)
                def _():
                    or_copy(j - 2, q).start()
            elif j == near_j:
                nr_copy(q).start()

        return step

    def release():
        pl.semaphore_signal(pair_free, inc=1, device_id={"expert": partner}, device_id_type=MESH)
        pl.semaphore_signal(cross_free, inc=1, device_id={"expert": neighbour}, device_id_type=MESH)

    def sent(src, dst, send):
        remote(src, dst, send, nr_recv.at[0], near).wait_send()

    def merge(i):
        def step(q):
            @pl.when(inner)
            def _():
                cols = columns(q)

                @pl.when(q == 0)
                def _():
                    sent(raw_f.at[i, pl.ds(0, cap)], near_ret, fwd_send.at[i])
                    if i == 0:
                        sent(near_stage.at[1], near_ret, near_send.at[1])

                with jax.named_scope("w_or"):
                    or_copy(i, q).wait_recv()
                total = mixed(1 + i, x[2 + i, s, :, cols], outer_ret[i, :, cols])
                raw_f[i, :, cols] = total.astype(raw_f.dtype)
                fr_copy(i, q).start()

        return step

    def early(j, t):
        def step(q):
            pl.when(q == chunks // 2)(lambda: finish(j, t)(0))
            pl.when(q == chunks - 1)(lambda: finish(j, t)(1))

        return step

    def ahead(j, t):
        def step(q):
            pl.when(q < chunks - 2)(lambda: finish(j, t)(q + 2))

        return step

    def merge_most(i):
        def step(q):
            pl.when(q < chunks - 2)(lambda: merge(i)(q))

        return step

    def merge_last(i):
        def step(q):
            pl.when(q < 2)(lambda: merge(i)(chunks - 2 + q))

        return step

    def near_nth(n):
        pl.when(n < chunks)(lambda: near_copy(0, n).start())
        pl.when(n >= chunks)(lambda: near_copy(1, n - chunks).start())

    def enter(i, q):
        cols = columns(q)

        @pl.when(inner)
        def _():
            with jax.named_scope("w_far"):
                far_copy(q, i).wait_recv()
            taken = select(2 + i, raw_f[i, :, cols])
            x[2 + i, s, :, cols] = taken[:cap]
            raw_f[i, 0:cap, cols] = taken[cap:]
            fwd_copy(i, q).start()

        @pl.when(outer)
        def _():
            with jax.named_scope("w_fwd"):
                fwd_copy(i, q).wait_recv()

        y_copy(i, q).start()
        d_copy(2 + i, row, q).start()

    def far_table(i):
        @pl.when(inner)
        def _():
            table_arrival(2 + i).wait_recv()
            set_pick(2 + i)
            set_mix(2 + i, 1 + i)

    with jax.named_scope("w_raw"):
        raw_load.wait()
    each(lambda q: cross_copy(q).start())
    each(lambda q: far_copy(q, 1 - kind).start())
    for load in loads:
        load.start()

    with jax.named_scope("take_own"):
        @each
        def _(q):
            cols = columns(q)
            taken = select(0, raw[:, cols])
            near_stage[0, :, cols] = taken[cap:]
            x[own_j, s, :, cols] = taken[:cap]
            d_copy(own_j, row, q).start()

            @pl.when(outer | (q < 2))
            def _():
                near_copy(0, q).start()

    with jax.named_scope("tables"):
        table_arrival(1).wait_recv()
        set_pick(1)
        set_mix(1, 3)

        far_table(0)

    with jax.named_scope("enter_b"):
        @each
        def _(q):
            cols = columns(q)
            with jax.named_scope("w_cross"):
                cross_copy(q).wait_recv()
            taken = select(1, raw_y[:, cols])
            near_stage[1, :, cols] = taken[cap:]
            x[own_j, cross_s, :, cols] = taken[:cap]
            d_copy(own_j, 1 - row, q).start()
            enter(0, q)

            pl.when(outer)(lambda: near_copy(1, q).start())
            pl.when(inner & (q % 2 == 1))(lambda: near_copy(0, 2 + q // 2).start())

    pl.when(inner)(lambda: near_nth(2 + chunks // 2))

    with jax.named_scope("wait_own"):
        loads[0].wait()
        loads[1].wait()
        gathered(own_j)
    with jax.named_scope("expand_own"):
        expand(own_j, 0)

    def enter_a(q):
        enter(1, q)
        y_arrival(0, q).wait_recv()
        d_copy(2, 1 - row, q).start()
        pl.when(inner & (q % 2 == 1))(lambda: near_nth(3 + chunks // 2 + q // 2))

    middle = chunks // 2 + 1
    with jax.named_scope("enter_a"):
        far_table(1)
        pl.loop(0, middle)(enter_a)

        @pl.loop(middle, chunks)
        def _(q):
            y_arrival(0, q).wait_recv()
            d_copy(2, 1 - row, q).start()

    with jax.named_scope("wait_b"):
        gathered(2)
    with jax.named_scope("expand_b"):
        expand(2, 1)
    with jax.named_scope("enter_a2"):
        @pl.loop(middle, chunks)
        def _(q):
            enter(1, q)

        @pl.when(inner)
        def _():
            pl.loop(3 + chunks // 2 + middle // 2, 2 * chunks)(near_nth)

    loads[2].wait()
    with jax.named_scope("contract_b"):
        contract(2, 0, 1, False, ())

    with jax.named_scope("wait_a"):
        @each
        def _(q):
            y_arrival(1, q).wait_recv()
            d_copy(3, 1 - row, q).start()

        gathered(3)
    with jax.named_scope("expand_a"):
        expand(3, 1, (early(2, 0),))
    def spread_near(q):
        @pl.when(q == chunks - 1)
        def _():
            for k, r in ((0, row), (1, 1 - row)):
                slot = r * 2 + core
                remote(near_stage.at[k], x.at[near_j, slot], near_send.at[k], near_recv.at[k], near).wait_recv()
                d_whole(near_j, r, core).start()

    with jax.named_scope("contract_a"):
        contract(3, 1, 1, False, (ahead(2, 0), merge_most(0), spread_near))
        release()

    with jax.named_scope("wait_near"):
        gathered(near_j)
    with jax.named_scope("expand_near"):
        expand(near_j, 1, (early(3, 1),))
    with jax.named_scope("contract_near"):
        contract(near_j, 0, 1, True, (merge_last(0), ahead(3, 1), merge_most(1)))
        release()
    def merge_late(q):
        pl.when(q >= chunks - 2)(lambda: merge(1)(q))

    with jax.named_scope("contract_own"):
        contract(own_j, 1, 0, True, (finish(near_j, 0), merge_late))

    with jax.named_scope("combine"):
        remote(raw, raw_y, cross_send, cross_recv.at[0], neighbour).wait_send()
        remote(raw, raw_y, far_send, cross_recv.at[0], neighbour).wait_send()

        @each
        def _(q):
            cols = columns(q)
            with jax.named_scope("w_own"):
                finish(own_j, 1)(q)
            with jax.named_scope("w_nr"):
                nr_copy(q).wait_recv()
            with jax.named_scope("w_fr"):
                fr_copy(0, q).wait_recv()
            total = mixed(0, x[own_j, s, :, cols], near_ret[:, cols])
            total += far_ret[:, cols].astype(jnp.float32)

            @pl.when(~folded(q))
            def _():
                raw[:, cols] = total.astype(raw.dtype)

            @pl.when(folded(q))
            def _():
                with jax.named_scope("w_fin"):
                    fin_copy(q).wait_recv()
                rest = raw_y[:, columns((q + folds) % chunks)]
                raw[:, cols] = (total + rest.astype(jnp.float32)).astype(raw.dtype)

            out_copy(q).start()

    with jax.named_scope("tail_sends"):
        table_y.wait_send()
        table_f.wait_send()
        sent(near_stage.at[0], near_ret, near_send.at[0])
        sent(x.at[near_j, s], near_ret, nr_send)
        for j in range(4):
            sent(x.at[j, pl.ds(0, 2)], pair.at[0], rp_send.at[j])
            part = pl.ds(0, width if j >= 2 else width - folds * tile)
            sent(x.at[j, cross_s, :, part], near_ret.at[:, part], ry_send.at[j])
        sent(near_cross, near_cross, nx_send)
        part = pl.ds(0, folds * tile)
        sent(raw_y.at[:, part], far_ret.at[:, part], fin_send)

        @pl.when(inner)
        def _():
            for i in range(2):
                sent(raw_f.at[i], far_ret, fr_send.at[i])

        @pl.when(outer)
        def _():
            sent(near_stage.at[1], near_ret, near_send.at[1])
            for i in range(2):
                sent(x.at[2 + i, s], near_ret, or_send.at[i])

    with jax.named_scope("tail_out"):
        pltpu.make_async_copy(raw, out_hbm, out_sem).wait()


def routed(tokens, route_ids, levels, w_gate, w_up, w_down, cap):
    tok_rows, width = tokens.shape
    ff, dtype = w_gate.shape[2], tokens.dtype
    rows, chunks = SHARDS * cap, width // tile_of(width, 1024)
    folds = chunks * 3 // 7
    dma, vmem = pltpu.SemaphoreType.DMA, pltpu.VMEM
    anywhere, local = pl.BlockSpec(memory_space=pl.ANY), pl.BlockSpec(memory_space=pltpu.VMEM)
    return pl.pallas_call(
        routed_kernel,
        out_shape=jax.ShapeDtypeStruct((tok_rows, width), dtype),
        in_specs=[anywhere, local, local, anywhere, anywhere, anywhere],
        out_specs=anywhere,
        scratch_shapes=[
            vmem((4, SHARDS, cap, width), dtype),
            vmem((width, ff), dtype),
            vmem((width, ff), dtype),
            vmem((ff, width), dtype),
            vmem((2, rows, ff), jnp.float32),
            vmem((2, rows, ff), dtype),
            vmem((2, 2, cap, width), dtype),
            vmem((2, cap, width), dtype),
            vmem((tok_rows, width), dtype),
            vmem((tok_rows, width), dtype),
            vmem((2, tok_rows, width), dtype),
            vmem((2, cap, width), dtype),
            vmem((cap, width), dtype),
            vmem((folds, cap, width // chunks), dtype),
            vmem((2, cap, width), dtype),
            vmem((tok_rows, width), dtype),
            vmem((4, 16, tok_rows), jnp.float32),
            vmem((4, 2 * cap, tok_rows), dtype),
            vmem((4, 2, tok_rows, 2 * cap), dtype),
            dma((3,)), dma, dma, dma((2,)), dma((3,)),
            dma, dma((chunks,)), dma, dma((2, chunks)),
            dma((2,)), dma((2,)),
            dma((2,)), dma((2, chunks)),
            dma((2,)), dma((2, chunks)),
            dma((4, 2)), dma((4, 2)),
            dma((4,)), dma((2, chunks, 2)),
            dma((4,)), dma((2, chunks)),
            dma, dma((chunks,)),
            dma((2,)), dma((2, chunks)),
            dma((2,)), dma((chunks,)),
            dma, dma((folds,)), dma, dma((folds,)),
            pltpu.SemaphoreType.REGULAR, pltpu.SemaphoreType.REGULAR,
        ],
        compiler_params=pltpu.CompilerParams(
            collective_id=0, has_side_effects=True, vmem_limit_bytes=67_000_000
        ),
    )(tokens, route_ids.T, levels.T, w_gate, w_up, w_down)


def combine_kernel(weight_ref, ret_ref, out_ref):
    weight = weight_ref[...]
    high = weight.astype(jnp.bfloat16)
    low = (weight - high.astype(jnp.float32)).astype(jnp.bfloat16)
    total = jnp.dot(high, ret_ref[...], preferred_element_type=jnp.float32)
    total += jnp.dot(low, ret_ref[...], preferred_element_type=jnp.float32)
    out_ref[...] = total.astype(out_ref.dtype)


def on_device(tokens, route_ids, levels, w_gate, w_up, w_down):
    tok_rows, width = tokens.shape
    top = route_ids.shape[1]
    ff = w_gate.shape[2]
    experts = lax.axis_size("expert") // SHARDS
    capacity = 5 * tok_rows * top // (4 * experts)
    cap = -(-capacity // 16) * 16
    slots = experts * cap
    dtype = tokens.dtype
    if experts == 4 and top == 2 and tok_rows < 2 * cap:
        return routed(tokens, route_ids, levels, w_gate, w_up, w_down, cap)

    chosen = route_ids[:, :, None] == jnp.arange(experts, dtype=jnp.int32)
    named = jnp.any(chosen, axis=1)
    index = jnp.arange(tok_rows, dtype=jnp.int32)
    earlier = (index[:, None] > index[None, :]).astype(jnp.bfloat16)
    rank = jnp.dot(earlier, named.astype(jnp.bfloat16), preferred_element_type=jnp.float32)
    place = jnp.where(named, rank.astype(jnp.int32), cap)
    level_f = levels.astype(jnp.float32)
    weights = level_f / jnp.sum(level_f, axis=1, keepdims=True)
    weight_e = jnp.sum(jnp.where(chosen, weights[:, :, None], 0.0), axis=1)
    spot = jnp.arange(cap, dtype=jnp.int32)
    pick = (place[:, :, None] == spot).reshape(tok_rows, slots)
    weight_m = jnp.where(pick, jnp.repeat(weight_e, cap, axis=1), 0.0)
    outgoing = lax.dot_general(
        pick.astype(dtype), tokens, (((0,), (0,)), ((), ())), preferred_element_type=jnp.float32
    ).astype(dtype).reshape(experts, cap, width)

    dma, anywhere = pltpu.SemaphoreType.DMA, pl.BlockSpec(memory_space=pl.ANY)
    rows, chunks = SHARDS * cap, width // tile_of(width, 1024)
    returned = pl.pallas_call(
        functools.partial(layer_kernel, experts),
        out_shape=jax.ShapeDtypeStruct((experts, cap, width), dtype),
        in_specs=[anywhere] * 4,
        out_specs=anywhere,
        scratch_shapes=[
            pltpu.VMEM((experts, SHARDS, cap, width), dtype),
            pltpu.VMEM((width, ff), dtype),
            pltpu.VMEM((width, ff), dtype),
            pltpu.VMEM((ff, width), dtype),
            pltpu.VMEM((2, rows, ff), jnp.float32),
            pltpu.VMEM((rows, ff), dtype),
            pltpu.VMEM((experts, 2, cap, width), dtype),
            pltpu.VMEM((experts, cap, width), dtype),
            dma((3,)),
            dma((experts,)), dma((experts,)),
            dma((experts,)), dma((experts,)),
            dma((experts, 2)), dma((experts, 2)),
            dma((experts, chunks, 2)), dma((experts, chunks, 2)),
            dma((experts, chunks)), dma((experts, chunks)),
            dma((experts, chunks)), dma((experts, chunks)),
        ],
        compiler_params=pltpu.CompilerParams(
            collective_id=0, has_side_effects=True, vmem_limit_bytes=67_000_000
        ),
    )(outgoing, w_gate, w_up, w_down)

    tile = tile_of(width, 1024)
    return pl.pallas_call(
        combine_kernel,
        out_shape=jax.ShapeDtypeStruct((tok_rows, width), dtype),
        grid=(width // tile,),
        in_specs=[
            pl.BlockSpec((tok_rows, slots), lambda n: (0, 0)),
            pl.BlockSpec((slots, tile), lambda n: (0, n)),
        ],
        out_specs=pl.BlockSpec((tok_rows, tile), lambda n: (0, n)),
    )(weight_m, returned.reshape(slots, width))


def solution(mesh):
    return jax.shard_map(
        on_device,
        mesh=mesh,
        in_specs=(
            P(("groups", "expert"), None),
            P(("groups", "expert"), None),
            P(("groups", "expert"), None),
            P("expert", None, None),
            P("expert", None, None),
            P("expert", None, None),
        ),
        out_specs=P(("groups", "expert"), None),
        check_vma=False,
    )
```

```python
import functools

import jax
import jax.numpy as jnp
from jax import lax
from jax.experimental import pallas as pl
from jax.experimental.pallas import tpu as pltpu
from jax.sharding import PartitionSpec as P

SHARDS = 4
MESH = pl.DeviceIdType.MESH


def tile_of(length, most):
    size = most
    while length % size:
        size //= 2
    return size


def xor(a, mask, count):
    total, bit = 0, 1
    while bit < count:
        total += (a // bit + mask // bit) % 2 * bit
        bit *= 2
    return total


def layer_kernel(
    planes, out_ref, gate_hbm, up_hbm, down_hbm, ret_ref,
    x, gate, up, down, acc, hidden, pair, cross,
    w_sem, z_send, z_recv, y_send, y_recv, p_send, p_recv,
    rp_send, rp_recv, ry_send, ry_recv, rz_send, rz_recv,
):
    me = lax.axis_index("expert")
    plane, s = me // SHARDS, me % SHARDS
    base = plane * SHARDS
    core, row = s % 2, s // 2
    partner_s = row * 2 + (1 - core)
    cross_s = (1 - row) * 2 + core
    diag_s = (1 - row) * 2 + (1 - core)
    partner, neighbour = base + partner_s, base + cross_s
    cap, width = x.shape[2], x.shape[3]
    rows = SHARDS * cap
    tile = tile_of(width, 1024)
    chunks = width // tile

    barrier = pltpu.get_barrier_semaphore()
    peers = [partner, neighbour]
    peers += [xor(plane, j, planes) * SHARDS + s for j in range(1, planes)]
    for peer in peers:
        pl.semaphore_signal(barrier, inc=1, device_id={"expert": peer}, device_id_type=MESH)
    pl.semaphore_wait(barrier, planes + 1)

    def remote(src, dst, send, recv, device):
        return pltpu.make_async_remote_copy(
            src_ref=src, dst_ref=dst, send_sem=send, recv_sem=recv,
            device_id={"expert": device}, device_id_type=MESH,
        )

    def columns(q):
        return pl.ds(pl.multiple_of(q * tile, tile), tile)

    def out_copy(j):
        to = xor(plane, j, planes)
        return remote(out_ref.at[to], x.at[j, s], z_send.at[j], z_recv.at[j], to * SHARDS + s)

    def own_copy():
        return pltpu.make_async_copy(out_ref.at[plane], x.at[0, s], z_recv.at[0])

    def y_copy(j):
        return remote(x.at[j, s], x.at[j, s], y_send.at[j], y_recv.at[j], neighbour)

    def y_arrival(j):
        return remote(x.at[j, cross_s], x.at[j, cross_s], y_send.at[j], y_recv.at[j], neighbour)

    def p_copy(j, k, slot):
        return remote(x.at[j, slot], x.at[j, slot], p_send.at[j, k], p_recv.at[j, k], partner)

    def rp_copy(j, q, k, slot):
        cols = columns(q)
        return remote(
            x.at[j, slot, :, cols], pair.at[j, k, :, cols],
            rp_send.at[j, q, k], rp_recv.at[j, q, k], partner,
        )

    def ry_copy(j, q):
        cols = columns(q)
        return remote(
            x.at[j, cross_s, :, cols], cross.at[j, :, cols],
            ry_send.at[j, q], ry_recv.at[j, q], neighbour,
        )

    def rz_copy(j, q):
        cols, to = columns(q), xor(plane, j, planes)
        return remote(
            x.at[j, s, :, cols], ret_ref.at[plane, :, cols],
            rz_send.at[j, q], rz_recv.at[j, q], to * SHARDS + s,
        )

    def keep_copy(q):
        cols = columns(q)
        return pltpu.make_async_copy(x.at[0, s, :, cols], ret_ref.at[plane, :, cols], rz_send.at[0, q])

    own_copy().start()
    for distance in range(1, planes):
        for to in (plane + distance, plane - distance):
            @pl.when((to >= 0) & (to < planes))
            def _():
                mask = xor(plane, to, planes)
                remote(
                    out_ref.at[to], x.at[mask, s], z_send.at[mask], z_recv.at[mask], to * SHARDS + s
                ).start()
    loads = [
        pltpu.make_async_copy(gate_hbm.at[0], gate, w_sem.at[0]),
        pltpu.make_async_copy(up_hbm.at[0], up, w_sem.at[1]),
        pltpu.make_async_copy(down_hbm.at[0], down, w_sem.at[2]),
    ]
    for load in loads:
        load.start()

    def arrive(j):
        if j == 0:
            own_copy().wait()
        else:
            out_copy(j).wait_recv()
        y_copy(j).start()
        p_copy(j, 0, s).start()

    def gather(j):
        y_arrival(j).wait_recv()
        p_copy(j, 1, cross_s).start()
        p_copy(j, 0, partner_s).wait_recv()
        p_copy(j, 1, diag_s).wait_recv()

    def expand(j):
        @pl.loop(0, chunks)
        def _(q):
            cols = columns(q)
            part = x[j, :, :, cols].reshape(rows, tile)

            @pl.when(q == 0)
            def _():
                acc[...] = jnp.zeros_like(acc)

            acc[0] += jnp.dot(part, gate[cols, :], preferred_element_type=jnp.float32)
            acc[1] += jnp.dot(part, up[cols, :], preferred_element_type=jnp.float32)

        value = acc[0]
        hidden[...] = (value / (1.0 + jnp.exp(-value)) * acc[1]).astype(hidden.dtype)

    def contract(j):
        y_copy(j).wait_send()
        p_copy(j, 0, s).wait_send()
        p_copy(j, 1, cross_s).wait_send()

        @pl.loop(0, chunks + 1)
        def _(q):
            @pl.when(q < chunks)
            def _():
                cols = columns(q)
                part = jnp.dot(hidden[...], down[:, cols], preferred_element_type=jnp.float32)
                x[j, :, :, cols] = part.astype(x.dtype).reshape(SHARDS, cap, tile)
                rp_copy(j, q, 1 - row, diag_s).start()
                rp_copy(j, q, row, partner_s).start()

            @pl.when(q > 0)
            def _():
                cols = columns(q - 1)
                rp_copy(j, q - 1, 1 - row, diag_s).wait_recv()
                total = x[j, cross_s, :, cols].astype(jnp.float32)
                total += pair[j, 1 - row, :, cols].astype(jnp.float32)
                x[j, cross_s, :, cols] = total.astype(x.dtype)
                ry_copy(j, q - 1).start()

    def finish(j):
        @pl.loop(0, chunks)
        def _(q):
            cols = columns(q)
            rp_copy(j, q, row, partner_s).wait_recv()
            total = x[j, s, :, cols].astype(jnp.float32) + pair[j, row, :, cols].astype(jnp.float32)
            ry_copy(j, q).wait_recv()
            x[j, s, :, cols] = (total + cross[j, :, cols].astype(jnp.float32)).astype(x.dtype)
            if j > 0:
                rz_copy(j, q).start()
            else:
                keep_copy(q).start()

    order = [0, *range(2, planes), 1]
    arrive(0)
    arrive(1)
    for i, j in enumerate(order):
        gather(j)
        if 0 < i < planes - 2:
            arrive(order[i + 1])
        if i == 0:
            for load in loads:
                load.wait()
        expand(j)
        contract(j)
        if i == 0:
            arrive(order[1])
        else:
            finish(order[i - 1])
    finish(order[-1])

    for j in range(planes):
        @pl.loop(0, chunks)
        def _(q):
            rp_copy(j, q, 1 - row, diag_s).wait_send()
            rp_copy(j, q, row, partner_s).wait_send()
            ry_copy(j, q).wait_send()
            if j > 0:
                rz_copy(j, q).wait()
            else:
                keep_copy(q).wait()
        if j > 0:
            out_copy(j).wait_send()


def routed_kernel(
    tokens, ids, levels, gate_hbm, up_hbm, down_hbm, far_ret,
    x, gate, up, down, acc, hidden, pair, cross, raw, raw_y, raw_f,
    near_stage, near_ret, near_cross, outer_ret, table, picks, mix,
    w_sem, raw_sem, table_send, table_recv,
    cross_send, cross_recv, far_send, far_recv, near_send, near_recv,
    fwd_send, fwd_recv, y_send, y_recv, d_send, d_recv,
    rp_send, rp_recv, ry_send, ry_recv,
    nr_send, nr_recv, or_send, or_recv, fr_send, fr_recv,
    nx_send, nx_recv, fin_send, fin_recv,
    pair_free, cross_free,
):
    me = lax.axis_index("expert")
    plane, s = me // SHARDS, me % SHARDS
    core, row = s % 2, s // 2
    half, near_plane = plane // 2, xor(plane, 1, 4)
    far_plane = 2 * (1 - half) + half
    kind = (plane + half + 1) % 2
    inner, outer = kind == 0, kind == 1
    cross_s = (1 - row) * 2 + core
    partner_s = row * 2 + (1 - core)
    diag_s = (1 - row) * 2 + (1 - core)
    partner, neighbour = plane * SHARDS + partner_s, plane * SHARDS + cross_s
    near, far = near_plane * SHARDS + s, far_plane * SHARDS + s
    far_b = xor(far_plane, 1, 4) * SHARDS + s
    cap, width = x.shape[2], x.shape[3]
    tok_rows = raw.shape[0]
    rows = SHARDS * cap
    tile = tile_of(width, 1024)
    chunks = width // tile
    own_j, near_j = 0, 1
    folds = near_cross.shape[0]

    def columns(q):
        return pl.ds(pl.multiple_of(q * tile, tile), tile)

    def remote(src, dst, send, recv, device):
        return pltpu.make_async_remote_copy(
            src_ref=src, dst_ref=dst, send_sem=send, recv_sem=recv,
            device_id={"expert": device}, device_id_type=MESH,
        )

    def each(body):
        pl.loop(0, chunks)(body)

    raw_load = pltpu.make_async_copy(tokens, raw, raw_sem)
    loads = [
        pltpu.make_async_copy(gate_hbm.at[0], gate, w_sem.at[0]),
        pltpu.make_async_copy(up_hbm.at[0], up, w_sem.at[1]),
        pltpu.make_async_copy(down_hbm.at[0], down, w_sem.at[2]),
    ]
    raw_load.start()

    barrier = pltpu.get_barrier_semaphore()
    peers = [partner, neighbour, near, far]
    for peer in peers:
        pl.semaphore_signal(barrier, inc=1, device_id={"expert": peer}, device_id_type=MESH)

    @pl.when(inner)
    def _():
        pl.semaphore_signal(barrier, inc=1, device_id={"expert": far_b}, device_id_type=MESH)

    lane = lax.broadcasted_iota(jnp.int32, (tok_rows, tok_rows), 1)
    line = lax.broadcasted_iota(jnp.int32, (tok_rows, tok_rows), 0)
    expert_of = lax.broadcasted_iota(jnp.int32, (8, tok_rows), 0)
    first, second = ids[0:1, :] == expert_of, ids[1:2, :] == expert_of
    level_0, level_1 = levels[0:1, :].astype(jnp.float32), levels[1:2, :].astype(jnp.float32)
    named = jnp.where(first | second, 1.0, 0.0)
    earlier = jnp.where(line < lane, 1.0, 0.0).astype(jnp.bfloat16)
    rank = jnp.dot(named.astype(jnp.bfloat16), earlier, preferred_element_type=jnp.float32)
    share = jnp.where(first, level_0 / (level_0 + level_1), 0.0)
    share += jnp.where(second, level_1 / (level_0 + level_1), 0.0)
    table[0, 0:8, :] = jnp.where(named > 0.0, rank, 2.0 * tok_rows)
    table[0, 8:16, :] = share

    def matches(k, expert):
        spot = lax.broadcasted_iota(jnp.int32, (cap, tok_rows), 0).astype(jnp.float32)
        return table[k, pl.ds(expert, 1), :] == spot

    def set_pick(k):
        for i, expert in enumerate((plane, near_plane)):
            pick = jnp.where(matches(k, expert), 1.0, 0.0)
            picks[k, i * cap:(i + 1) * cap, :] = pick.astype(picks.dtype)

    def set_mix(k, spot):
        parts = []
        for expert in (plane, near_plane):
            weight = table[k, pl.ds(8 + expert, 1), :]
            parts.append(jnp.where(matches(k, expert), weight, 0.0))
        weight = jnp.transpose(jnp.concatenate(parts, axis=0))
        high = weight.astype(jnp.bfloat16)
        mix[spot, 0] = high
        mix[spot, 1] = (weight - high.astype(jnp.float32)).astype(jnp.bfloat16)

    def select(k, block):
        return jnp.dot(picks[k], block, preferred_element_type=jnp.float32).astype(x.dtype)

    def mixed(spot, own, other):
        both = jnp.concatenate([own, other], axis=0)
        total = jnp.dot(mix[spot, 0], both, preferred_element_type=jnp.float32)
        return total + jnp.dot(mix[spot, 1], both, preferred_element_type=jnp.float32)

    set_pick(0)
    set_mix(0, 0)
    with jax.named_scope("barrier"):
        pl.semaphore_wait(barrier, len(peers) + 1 - kind)

    table_y = remote(table.at[0], table.at[1], table_send.at[0], table_recv.at[0], neighbour)
    table_f = remote(table.at[0], table.at[3 - kind], table_send.at[1], table_recv.at[2 - kind], far)
    table_y.start()
    table_f.start()

    def table_arrival(k):
        return remote(table.at[0], table.at[k], table_send.at[0], table_recv.at[k - 1], far)

    def cross_copy(q):
        cols = columns(q)
        return remote(raw.at[:, cols], raw_y.at[:, cols], cross_send, cross_recv.at[q], neighbour)

    def far_copy(q, k):
        cols = columns(q)
        return remote(raw.at[:, cols], raw_f.at[k, :, cols], far_send, far_recv.at[k, q], far)

    def near_copy(k, q):
        cols, slot = columns(q), s if k == 0 else cross_s
        return remote(
            near_stage.at[k, :, cols], x.at[near_j, slot, :, cols],
            near_send.at[k], near_recv.at[k], near,
        )

    def fwd_copy(i, q):
        cols = columns(q)
        return remote(
            raw_f.at[i, pl.ds(0, cap), cols], x.at[2 + i, s, :, cols], fwd_send.at[i], fwd_recv.at[i, q], near
        )

    def y_copy(i, q):
        cols = columns(q)
        return remote(
            x.at[2 + i, s, :, cols], x.at[2 + i, s, :, cols], y_send.at[i], y_recv.at[i, q], neighbour
        )

    def y_arrival(i, q):
        cols = columns(q)
        return remote(
            x.at[2 + i, s, :, cols], x.at[2 + i, cross_s, :, cols],
            y_send.at[i], y_recv.at[i, q], neighbour,
        )

    def d_copy(j, r, q):
        cols, slot = columns(q), r * 2 + core
        return remote(
            x.at[j, slot, :, cols], x.at[j, slot, :, cols], d_send.at[j, r], d_recv.at[j, r], partner
        )

    def d_whole(j, r, lane_core):
        slot = r * 2 + lane_core
        return remote(x.at[j, slot], x.at[j, slot], d_send.at[j, r], d_recv.at[j, r], partner)

    def gathered(j):
        for r in range(2):
            d_whole(j, r, 1 - core).wait_recv()

    def rp_copy(j, t, q, k, slot):
        cols = columns(q)
        return remote(
            x.at[j, slot, :, cols], pair.at[t, k, :, cols],
            rp_send.at[j], rp_recv.at[t, q, k], partner,
        )

    def ry_copy(j, t, q):
        cols = columns(q)
        return remote(
            x.at[j, cross_s, :, cols], cross.at[t, :, cols],
            ry_send.at[j], ry_recv.at[t, q], neighbour,
        )

    def nr_copy(q):
        cols = columns(q)
        return remote(x.at[near_j, s, :, cols], near_ret.at[:, cols], nr_send, nr_recv.at[q], near)

    def or_copy(i, q):
        cols = columns(q)
        return remote(
            x.at[2 + i, s, :, cols], outer_ret.at[i, :, cols], or_send.at[i], or_recv.at[i, q], near
        )

    def fr_copy(i, q):
        cols = columns(q)
        return remote(
            raw_f.at[i, :, cols], far_ret.at[:, cols], fr_send.at[i], fr_recv.at[q],
            far_b if i == 0 else far,
        )

    def folded(q):
        return (q >= 2) & (q < 2 + folds)

    def nx_copy(q):
        return remote(
            x.at[near_j, cross_s, :, columns(q)], near_cross.at[q - 2], nx_send, nx_recv.at[q - 2], near
        )

    def fin_copy(q):
        return remote(
            raw.at[:, columns(q)], raw_y.at[:, columns(q)],
            fin_send, fin_recv.at[q - 2], neighbour,
        )

    def fold(q):
        cols = columns(q)
        with jax.named_scope("w_nx"):
            nx_copy(q).wait_recv()
        total = mixed(3, x[own_j, cross_s, :, cols], near_cross[q - 2])
        raw[:, cols] = total.astype(raw.dtype)
        fin_copy(q).start()

    def expand(j, spot, also=()):
        @each
        def _(q):
            cols = columns(q)
            part = x[j, :, :, cols].reshape(rows, tile)

            @pl.when(q == 0)
            def _():
                acc[...] = jnp.zeros_like(acc)

            acc[0] += jnp.dot(part, gate[cols, :], preferred_element_type=jnp.float32)
            acc[1] += jnp.dot(part, up[cols, :], preferred_element_type=jnp.float32)
            for step in also:
                step(q)

        value = acc[0]
        hidden[spot] = (value / (1.0 + jnp.exp(-value)) * acc[1]).astype(hidden.dtype)

    def contract(j, t, spot, credit, also):
        for r in range(2):
            d_whole(j, r, core).wait_send()
        if j >= 2:
            remote(x.at[j, s], x.at[j, s], y_send.at[j - 2], d_recv.at[j, 0], neighbour).wait_send()
        if credit:
            pl.semaphore_wait(pair_free, 1)
            pl.semaphore_wait(cross_free, 1)

        @pl.loop(0, chunks + 1)
        def _(q):
            @pl.when(q < chunks)
            def _():
                cols = columns(q)
                part = jnp.dot(hidden[spot], down[:, cols], preferred_element_type=jnp.float32)
                x[j, :, :, cols] = part.astype(x.dtype).reshape(SHARDS, cap, tile)
                rp_copy(j, t, q, 1 - row, diag_s).start()
                rp_copy(j, t, q, row, partner_s).start()
                for step in also:
                    step(q)

            @pl.when(q > 0)
            def _():
                cols = columns(q - 1)
                rp_copy(j, t, q - 1, 1 - row, diag_s).wait_recv()
                total = x[j, cross_s, :, cols].astype(jnp.float32)
                total += pair[t, 1 - row, :, cols].astype(jnp.float32)
                x[j, cross_s, :, cols] = total.astype(x.dtype)
                if j >= 2:
                    ry_copy(j, t, q - 1).start()
                else:
                    pl.when(~folded(q - 1))(lambda: ry_copy(j, t, q - 1).start())

                    @pl.when(folded(q - 1))
                    def _():
                        nx_copy(q - 1).start() if j == near_j else fold(q - 1)

    def finish(j, t):
        def step(q):
            cols = columns(q)
            with jax.named_scope("w_rp"):
                rp_copy(j, t, q, row, partner_s).wait_recv()
            total = x[j, s, :, cols].astype(jnp.float32) + pair[t, row, :, cols].astype(jnp.float32)

            def whole():
                with jax.named_scope("w_ry"):
                    ry_copy(j, t, q).wait_recv()
                x[j, s, :, cols] = (total + cross[t, :, cols].astype(jnp.float32)).astype(x.dtype)

            def column_sum():
                x[j, s, :, cols] = total.astype(x.dtype)

            if j >= 2:
                whole()
            else:
                pl.when(~folded(q))(whole)
                pl.when(folded(q))(column_sum)
            if j >= 2:
                @pl.when(outer)
                def _():
                    or_copy(j - 2, q).start()
            elif j == near_j:
                nr_copy(q).start()

        return step

    def release():
        pl.semaphore_signal(pair_free, inc=1, device_id={"expert": partner}, device_id_type=MESH)
        pl.semaphore_signal(cross_free, inc=1, device_id={"expert": neighbour}, device_id_type=MESH)

    def sent(src, dst, send):
        remote(src, dst, send, nr_recv.at[0], near).wait_send()

    def merge(i):
        def step(q):
            @pl.when(inner)
            def _():
                cols = columns(q)

                @pl.when(q == 0)
                def _():
                    sent(raw_f.at[i, pl.ds(0, cap)], near_ret, fwd_send.at[i])
                    with jax.named_scope("w_gate"):
                      if i == 0:
                        sent(near_stage.at[1], near_ret, near_send.at[1])

                with jax.named_scope("w_or"):
                    or_copy(i, q).wait_recv()
                total = mixed(1 + i, x[2 + i, s, :, cols], outer_ret[i, :, cols])
                raw_f[i, :, cols] = total.astype(raw_f.dtype)
                fr_copy(i, q).start()

        return step

    def early(j, t):
        def step(q):
            pl.when(q == chunks // 2)(lambda: finish(j, t)(0))
            pl.when(q == chunks - 1)(lambda: finish(j, t)(1))

        return step

    def ahead(j, t):
        def step(q):
            pl.when(q < chunks - 2)(lambda: finish(j, t)(q + 2))

        return step

    def merge_most(i):
        def step(q):
            pl.when(q < chunks - 2)(lambda: merge(i)(q))

        return step

    def merge_last(i):
        def step(q):
            pl.when(q < 2)(lambda: merge(i)(chunks - 2 + q))

        return step

    def near_nth(n):
        pl.when(n < chunks)(lambda: near_copy(0, n).start())
        pl.when(n >= chunks)(lambda: near_copy(1, n - chunks).start())

    def enter(i, q):
        cols = columns(q)

        @pl.when(inner)
        def _():
            with jax.named_scope("w_far"):
                far_copy(q, i).wait_recv()
            taken = select(2 + i, raw_f[i, :, cols])
            x[2 + i, s, :, cols] = taken[:cap]
            raw_f[i, 0:cap, cols] = taken[cap:]
            fwd_copy(i, q).start()

        @pl.when(outer)
        def _():
            with jax.named_scope("w_fwd"):
                fwd_copy(i, q).wait_recv()

        y_copy(i, q).start()
        d_copy(2 + i, row, q).start()

    def far_table(i):
        @pl.when(inner)
        def _():
            table_arrival(2 + i).wait_recv()
            set_pick(2 + i)
            set_mix(2 + i, 1 + i)

    with jax.named_scope("w_raw"):
        raw_load.wait()
    each(lambda q: cross_copy(q).start())
    each(lambda q: far_copy(q, 1 - kind).start())
    for load in loads:
        load.start()

    with jax.named_scope("take_own"):
        @each
        def _(q):
            cols = columns(q)
            taken = select(0, raw[:, cols])
            near_stage[0, :, cols] = taken[cap:]
            x[own_j, s, :, cols] = taken[:cap]
            d_copy(own_j, row, q).start()

            @pl.when(outer | (q < 2))
            def _():
                near_copy(0, q).start()

    with jax.named_scope("tables"):
        table_arrival(1).wait_recv()
        set_pick(1)
        set_mix(1, 3)

        far_table(0)

    with jax.named_scope("enter_b"):
        @each
        def _(q):
            cols = columns(q)
            with jax.named_scope("w_cross"):
                cross_copy(q).wait_recv()
            taken = select(1, raw_y[:, cols])
            near_stage[1, :, cols] = taken[cap:]
            x[own_j, cross_s, :, cols] = taken[:cap]
            d_copy(own_j, 1 - row, q).start()
            enter(0, q)

            pl.when(outer)(lambda: near_copy(1, q).start())
            pl.when(inner & (q % 2 == 1))(lambda: near_copy(0, 2 + q // 2).start())

    pl.when(inner)(lambda: near_nth(2 + chunks // 2))
    pl.when(inner)(lambda: near_nth(3 + chunks // 2))

    with jax.named_scope("wait_own"):
        loads[0].wait()
        loads[1].wait()
        gathered(own_j)
    with jax.named_scope("expand_own"):
        expand(own_j, 0)

    def enter_a(q):
        enter(1, q)
        y_arrival(0, q).wait_recv()
        d_copy(2, 1 - row, q).start()
        pl.when(inner & (q % 2 == 1))(lambda: near_nth(4 + chunks // 2 + q // 2))

    middle = chunks // 2 + 1
    with jax.named_scope("enter_a"):
        far_table(1)
        pl.loop(0, middle)(enter_a)

        @pl.loop(middle, chunks)
        def _(q):
            y_arrival(0, q).wait_recv()
            d_copy(2, 1 - row, q).start()

    with jax.named_scope("wait_b"):
        gathered(2)
    with jax.named_scope("expand_b"):
        expand(2, 1)
    with jax.named_scope("enter_a2"):
        @pl.loop(middle, chunks)
        def _(q):
            enter(1, q)

        @pl.when(inner)
        def _():
            pl.loop(4 + chunks // 2 + middle // 2, 2 * chunks)(near_nth)

    loads[2].wait()
    with jax.named_scope("contract_b"):
        contract(2, 0, 1, False, ())

    with jax.named_scope("wait_a"):
        @each
        def _(q):
            y_arrival(1, q).wait_recv()
            d_copy(3, 1 - row, q).start()

        gathered(3)
    with jax.named_scope("expand_a"):
        expand(3, 1, (early(2, 0),))
    def spread_near(q):
        @pl.when(q == chunks - 1)
        def _():
            for k, r in ((0, row), (1, 1 - row)):
                slot = r * 2 + core
                remote(near_stage.at[k], x.at[near_j, slot], near_send.at[k], near_recv.at[k], near).wait_recv()
                d_whole(near_j, r, core).start()

    with jax.named_scope("contract_a"):
        contract(3, 1, 1, False, (ahead(2, 0), merge_most(0), spread_near))
        release()

    with jax.named_scope("wait_near"):
        gathered(near_j)
    with jax.named_scope("expand_near"):
        expand(near_j, 1, (early(3, 1),))
    with jax.named_scope("contract_near"):
        contract(near_j, 0, 1, True, (merge_last(0), ahead(3, 1), merge_most(1)))
        release()
    def merge_late(q):
        pl.when(q >= chunks - 2)(lambda: merge(1)(q))

    sent(raw, raw_y, cross_send)
    sent(raw, raw_y, far_send)
    with jax.named_scope("contract_own"):
        contract(own_j, 1, 0, True, (finish(near_j, 0), merge_late))

    with jax.named_scope("combine"):
        @each
        def _(q):
            cols = columns(q)
            with jax.named_scope("w_own"):
                finish(own_j, 1)(q)
            with jax.named_scope("w_nr"):
                nr_copy(q).wait_recv()
            with jax.named_scope("w_fr"):
                fr_copy(0, q).wait_recv()
            total = mixed(0, x[own_j, s, :, cols], near_ret[:, cols])
            total += far_ret[:, cols].astype(jnp.float32)

            @pl.when(~folded(q))
            def _():
                far_ret[:, cols] = total.astype(far_ret.dtype)

            @pl.when(folded(q))
            def _():
                with jax.named_scope("w_fin"):
                    fin_copy(q).wait_recv()
                rest = raw_y[:, cols].astype(jnp.float32)
                far_ret[:, cols] = (total + rest).astype(far_ret.dtype)


    with jax.named_scope("tail_sends"):
        table_y.wait_send()
        table_f.wait_send()
        sent(near_stage.at[0], near_ret, near_send.at[0])
        sent(x.at[near_j, s], near_ret, nr_send)
        for j in range(4):
            sent(x.at[j, pl.ds(0, 2)], pair.at[0], rp_send.at[j])
            part = pl.ds(0, width if j >= 2 else width - folds * tile)
            sent(x.at[j, cross_s, :, part], near_ret.at[:, part], ry_send.at[j])
        sent(near_cross, near_cross, nx_send)
        part = pl.ds(0, folds * tile)
        sent(raw.at[:, part], far_ret.at[:, part], fin_send)

        @pl.when(inner)
        def _():
            for i in range(2):
                sent(raw_f.at[i], far_ret, fr_send.at[i])

        @pl.when(outer)
        def _():
            sent(near_stage.at[1], near_ret, near_send.at[1])
            for i in range(2):
                sent(x.at[2 + i, s], near_ret, or_send.at[i])


def routed(tokens, route_ids, levels, w_gate, w_up, w_down, cap):
    tok_rows, width = tokens.shape
    ff, dtype = w_gate.shape[2], tokens.dtype
    rows, chunks = SHARDS * cap, width // tile_of(width, 1024)
    folds = chunks * 3 // 7
    dma, vmem = pltpu.SemaphoreType.DMA, pltpu.VMEM
    anywhere, local = pl.BlockSpec(memory_space=pl.ANY), pl.BlockSpec(memory_space=pltpu.VMEM)
    return pl.pallas_call(
        routed_kernel,
        out_shape=pltpu.VMEM((tok_rows, width), dtype),
        in_specs=[anywhere, local, local, anywhere, anywhere, anywhere],
        out_specs=local,
        scratch_shapes=[
            vmem((4, SHARDS, cap, width), dtype),
            vmem((width, ff), dtype),
            vmem((width, ff), dtype),
            vmem((ff, width), dtype),
            vmem((2, rows, ff), jnp.float32),
            vmem((2, rows, ff), dtype),
            vmem((2, 2, cap, width), dtype),
            vmem((2, cap, width), dtype),
            vmem((tok_rows, width), dtype),
            vmem((tok_rows, width), dtype),
            vmem((2, tok_rows, width), dtype),
            vmem((2, cap, width), dtype),
            vmem((cap, width), dtype),
            vmem((folds, cap, width // chunks), dtype),
            vmem((2, cap, width), dtype),
            vmem((4, 16, tok_rows), jnp.float32),
            vmem((4, 2 * cap, tok_rows), dtype),
            vmem((4, 2, tok_rows, 2 * cap), dtype),
            dma((3,)), dma, dma((2,)), dma((3,)),
            dma, dma((chunks,)), dma, dma((2, chunks)),
            dma((2,)), dma((2,)),
            dma((2,)), dma((2, chunks)),
            dma((2,)), dma((2, chunks)),
            dma((4, 2)), dma((4, 2)),
            dma((4,)), dma((2, chunks, 2)),
            dma((4,)), dma((2, chunks)),
            dma, dma((chunks,)),
            dma((2,)), dma((2, chunks)),
            dma((2,)), dma((chunks,)),
            dma, dma((folds,)), dma, dma((folds,)),
            pltpu.SemaphoreType.REGULAR, pltpu.SemaphoreType.REGULAR,
        ],
        compiler_params=pltpu.CompilerParams(
            collective_id=0, has_side_effects=True, vmem_limit_bytes=65_200_000
        ),
    )(tokens, route_ids.T, levels.T, w_gate, w_up, w_down)


def combine_kernel(weight_ref, ret_ref, out_ref):
    weight = weight_ref[...]
    high = weight.astype(jnp.bfloat16)
    low = (weight - high.astype(jnp.float32)).astype(jnp.bfloat16)
    total = jnp.dot(high, ret_ref[...], preferred_element_type=jnp.float32)
    total += jnp.dot(low, ret_ref[...], preferred_element_type=jnp.float32)
    out_ref[...] = total.astype(out_ref.dtype)


def on_device(tokens, route_ids, levels, w_gate, w_up, w_down):
    tok_rows, width = tokens.shape
    top = route_ids.shape[1]
    ff = w_gate.shape[2]
    experts = lax.axis_size("expert") // SHARDS
    capacity = 5 * tok_rows * top // (4 * experts)
    cap = -(-capacity // 16) * 16
    slots = experts * cap
    dtype = tokens.dtype
    if experts == 4 and top == 2 and tok_rows < 2 * cap:
        return routed(tokens, route_ids, levels, w_gate, w_up, w_down, cap)

    chosen = route_ids[:, :, None] == jnp.arange(experts, dtype=jnp.int32)
    named = jnp.any(chosen, axis=1)
    index = jnp.arange(tok_rows, dtype=jnp.int32)
    earlier = (index[:, None] > index[None, :]).astype(jnp.bfloat16)
    rank = jnp.dot(earlier, named.astype(jnp.bfloat16), preferred_element_type=jnp.float32)
    place = jnp.where(named, rank.astype(jnp.int32), cap)
    level_f = levels.astype(jnp.float32)
    weights = level_f / jnp.sum(level_f, axis=1, keepdims=True)
    weight_e = jnp.sum(jnp.where(chosen, weights[:, :, None], 0.0), axis=1)
    spot = jnp.arange(cap, dtype=jnp.int32)
    pick = (place[:, :, None] == spot).reshape(tok_rows, slots)
    weight_m = jnp.where(pick, jnp.repeat(weight_e, cap, axis=1), 0.0)
    outgoing = lax.dot_general(
        pick.astype(dtype), tokens, (((0,), (0,)), ((), ())), preferred_element_type=jnp.float32
    ).astype(dtype).reshape(experts, cap, width)

    dma, anywhere = pltpu.SemaphoreType.DMA, pl.BlockSpec(memory_space=pl.ANY)
    rows, chunks = SHARDS * cap, width // tile_of(width, 1024)
    returned = pl.pallas_call(
        functools.partial(layer_kernel, experts),
        out_shape=jax.ShapeDtypeStruct((experts, cap, width), dtype),
        in_specs=[anywhere] * 4,
        out_specs=anywhere,
        scratch_shapes=[
            pltpu.VMEM((experts, SHARDS, cap, width), dtype),
            pltpu.VMEM((width, ff), dtype),
            pltpu.VMEM((width, ff), dtype),
            pltpu.VMEM((ff, width), dtype),
            pltpu.VMEM((2, rows, ff), jnp.float32),
            pltpu.VMEM((rows, ff), dtype),
            pltpu.VMEM((experts, 2, cap, width), dtype),
            pltpu.VMEM((experts, cap, width), dtype),
            dma((3,)),
            dma((experts,)), dma((experts,)),
            dma((experts,)), dma((experts,)),
            dma((experts, 2)), dma((experts, 2)),
            dma((experts, chunks, 2)), dma((experts, chunks, 2)),
            dma((experts, chunks)), dma((experts, chunks)),
            dma((experts, chunks)), dma((experts, chunks)),
        ],
        compiler_params=pltpu.CompilerParams(
            collective_id=0, has_side_effects=True, vmem_limit_bytes=67_000_000
        ),
    )(outgoing, w_gate, w_up, w_down)

    tile = tile_of(width, 1024)
    return pl.pallas_call(
        combine_kernel,
        out_shape=jax.ShapeDtypeStruct((tok_rows, width), dtype),
        grid=(width // tile,),
        in_specs=[
            pl.BlockSpec((tok_rows, slots), lambda n: (0, 0)),
            pl.BlockSpec((slots, tile), lambda n: (0, n)),
        ],
        out_specs=pl.BlockSpec((tok_rows, tile), lambda n: (0, n)),
    )(weight_m, returned.reshape(slots, width))


def solution(mesh):
    return jax.shard_map(
        on_device,
        mesh=mesh,
        in_specs=(
            P(("groups", "expert"), None),
            P(("groups", "expert"), None),
            P(("groups", "expert"), None),
            P("expert", None, None),
            P("expert", None, None),
            P("expert", None, None),
        ),
        out_specs=P(("groups", "expert"), None),
        check_vma=False,
    )
```

```python
import functools

import jax
import jax.numpy as jnp
from jax import lax
from jax.experimental import pallas as pl
from jax.experimental.pallas import tpu as pltpu
from jax.sharding import PartitionSpec as P

SHARDS = 4
MESH = pl.DeviceIdType.MESH


def tile_of(length, most):
    size = most
    while length % size:
        size //= 2
    return size


def xor(a, mask, count):
    total, bit = 0, 1
    while bit < count:
        total += (a // bit + mask // bit) % 2 * bit
        bit *= 2
    return total


def layer_kernel(
    planes, out_ref, gate_hbm, up_hbm, down_hbm, ret_ref,
    x, gate, up, down, acc, hidden, pair, cross,
    w_sem, z_send, z_recv, y_send, y_recv, p_send, p_recv,
    rp_send, rp_recv, ry_send, ry_recv, rz_send, rz_recv,
):
    me = lax.axis_index("expert")
    plane, s = me // SHARDS, me % SHARDS
    base = plane * SHARDS
    core, row = s % 2, s // 2
    partner_s = row * 2 + (1 - core)
    cross_s = (1 - row) * 2 + core
    diag_s = (1 - row) * 2 + (1 - core)
    partner, neighbour = base + partner_s, base + cross_s
    cap, width = x.shape[2], x.shape[3]
    rows = SHARDS * cap
    tile = tile_of(width, 1024)
    chunks = width // tile

    barrier = pltpu.get_barrier_semaphore()
    peers = [partner, neighbour]
    peers += [xor(plane, j, planes) * SHARDS + s for j in range(1, planes)]
    for peer in peers:
        pl.semaphore_signal(barrier, inc=1, device_id={"expert": peer}, device_id_type=MESH)
    pl.semaphore_wait(barrier, planes + 1)

    def remote(src, dst, send, recv, device):
        return pltpu.make_async_remote_copy(
            src_ref=src, dst_ref=dst, send_sem=send, recv_sem=recv,
            device_id={"expert": device}, device_id_type=MESH,
        )

    def columns(q):
        return pl.ds(pl.multiple_of(q * tile, tile), tile)

    def out_copy(j):
        to = xor(plane, j, planes)
        return remote(out_ref.at[to], x.at[j, s], z_send.at[j], z_recv.at[j], to * SHARDS + s)

    def own_copy():
        return pltpu.make_async_copy(out_ref.at[plane], x.at[0, s], z_recv.at[0])

    def y_copy(j):
        return remote(x.at[j, s], x.at[j, s], y_send.at[j], y_recv.at[j], neighbour)

    def y_arrival(j):
        return remote(x.at[j, cross_s], x.at[j, cross_s], y_send.at[j], y_recv.at[j], neighbour)

    def p_copy(j, k, slot):
        return remote(x.at[j, slot], x.at[j, slot], p_send.at[j, k], p_recv.at[j, k], partner)

    def rp_copy(j, q, k, slot):
        cols = columns(q)
        return remote(
            x.at[j, slot, :, cols], pair.at[j, k, :, cols],
            rp_send.at[j, q, k], rp_recv.at[j, q, k], partner,
        )

    def ry_copy(j, q):
        cols = columns(q)
        return remote(
            x.at[j, cross_s, :, cols], cross.at[j, :, cols],
            ry_send.at[j, q], ry_recv.at[j, q], neighbour,
        )

    def rz_copy(j, q):
        cols, to = columns(q), xor(plane, j, planes)
        return remote(
            x.at[j, s, :, cols], ret_ref.at[plane, :, cols],
            rz_send.at[j, q], rz_recv.at[j, q], to * SHARDS + s,
        )

    def keep_copy(q):
        cols = columns(q)
        return pltpu.make_async_copy(x.at[0, s, :, cols], ret_ref.at[plane, :, cols], rz_send.at[0, q])

    own_copy().start()
    for distance in range(1, planes):
        for to in (plane + distance, plane - distance):
            @pl.when((to >= 0) & (to < planes))
            def _():
                mask = xor(plane, to, planes)
                remote(
                    out_ref.at[to], x.at[mask, s], z_send.at[mask], z_recv.at[mask], to * SHARDS + s
                ).start()
    loads = [
        pltpu.make_async_copy(gate_hbm.at[0], gate, w_sem.at[0]),
        pltpu.make_async_copy(up_hbm.at[0], up, w_sem.at[1]),
        pltpu.make_async_copy(down_hbm.at[0], down, w_sem.at[2]),
    ]
    for load in loads:
        load.start()

    def arrive(j):
        if j == 0:
            own_copy().wait()
        else:
            out_copy(j).wait_recv()
        y_copy(j).start()
        p_copy(j, 0, s).start()

    def gather(j):
        y_arrival(j).wait_recv()
        p_copy(j, 1, cross_s).start()
        p_copy(j, 0, partner_s).wait_recv()
        p_copy(j, 1, diag_s).wait_recv()

    def expand(j):
        @pl.loop(0, chunks)
        def _(q):
            cols = columns(q)
            part = x[j, :, :, cols].reshape(rows, tile)

            @pl.when(q == 0)
            def _():
                acc[...] = jnp.zeros_like(acc)

            acc[0] += jnp.dot(part, gate[cols, :], preferred_element_type=jnp.float32)
            acc[1] += jnp.dot(part, up[cols, :], preferred_element_type=jnp.float32)

        value = acc[0]
        hidden[...] = (value / (1.0 + jnp.exp(-value)) * acc[1]).astype(hidden.dtype)

    def contract(j):
        y_copy(j).wait_send()
        p_copy(j, 0, s).wait_send()
        p_copy(j, 1, cross_s).wait_send()

        @pl.loop(0, chunks + 1)
        def _(q):
            @pl.when(q < chunks)
            def _():
                cols = columns(q)
                part = jnp.dot(hidden[...], down[:, cols], preferred_element_type=jnp.float32)
                x[j, :, :, cols] = part.astype(x.dtype).reshape(SHARDS, cap, tile)
                rp_copy(j, q, 1 - row, diag_s).start()
                rp_copy(j, q, row, partner_s).start()

            @pl.when(q > 0)
            def _():
                cols = columns(q - 1)
                rp_copy(j, q - 1, 1 - row, diag_s).wait_recv()
                total = x[j, cross_s, :, cols].astype(jnp.float32)
                total += pair[j, 1 - row, :, cols].astype(jnp.float32)
                x[j, cross_s, :, cols] = total.astype(x.dtype)
                ry_copy(j, q - 1).start()

    def finish(j):
        @pl.loop(0, chunks)
        def _(q):
            cols = columns(q)
            rp_copy(j, q, row, partner_s).wait_recv()
            total = x[j, s, :, cols].astype(jnp.float32) + pair[j, row, :, cols].astype(jnp.float32)
            ry_copy(j, q).wait_recv()
            x[j, s, :, cols] = (total + cross[j, :, cols].astype(jnp.float32)).astype(x.dtype)
            if j > 0:
                rz_copy(j, q).start()
            else:
                keep_copy(q).start()

    order = [0, *range(2, planes), 1]
    arrive(0)
    arrive(1)
    for i, j in enumerate(order):
        gather(j)
        if 0 < i < planes - 2:
            arrive(order[i + 1])
        if i == 0:
            for load in loads:
                load.wait()
        expand(j)
        contract(j)
        if i == 0:
            arrive(order[1])
        else:
            finish(order[i - 1])
    finish(order[-1])

    for j in range(planes):
        @pl.loop(0, chunks)
        def _(q):
            rp_copy(j, q, 1 - row, diag_s).wait_send()
            rp_copy(j, q, row, partner_s).wait_send()
            ry_copy(j, q).wait_send()
            if j > 0:
                rz_copy(j, q).wait()
            else:
                keep_copy(q).wait()
        if j > 0:
            out_copy(j).wait_send()


def routed_kernel(
    tokens, ids, levels, gate_hbm, up_hbm, down_hbm, far_ret,
    x, gate, up, down, acc, hidden, pair, cross, raw, raw_y, raw_f,
    near_stage, near_ret, near_cross, outer_ret, table, picks, mix,
    w_sem, raw_sem, table_send, table_recv,
    cross_send, cross_recv, far_send, far_recv, near_send, near_recv,
    fwd_send, fwd_recv, y_send, y_recv, d_send, d_recv,
    rp_send, rp_recv, ry_send, ry_recv,
    nr_send, nr_recv, or_send, or_recv, fr_send, fr_recv,
    nx_send, nx_recv, fin_send, fin_recv,
    pair_free, cross_free, entered,
):
    me = lax.axis_index("expert")
    plane, s = me // SHARDS, me % SHARDS
    core, row = s % 2, s // 2
    half, near_plane = plane // 2, xor(plane, 1, 4)
    far_plane = 2 * (1 - half) + half
    kind = (plane + half + 1) % 2
    inner, outer = kind == 0, kind == 1
    cross_s = (1 - row) * 2 + core
    partner_s = row * 2 + (1 - core)
    diag_s = (1 - row) * 2 + (1 - core)
    partner, neighbour = plane * SHARDS + partner_s, plane * SHARDS + cross_s
    near, far = near_plane * SHARDS + s, far_plane * SHARDS + s
    far_b = xor(far_plane, 1, 4) * SHARDS + s
    cap, width = x.shape[2], x.shape[3]
    tok_rows = raw.shape[0]
    rows = SHARDS * cap
    tile = tile_of(width, 1024)
    chunks = width // tile
    own_j, near_j = 0, 1
    folds = near_cross.shape[0]

    def columns(q):
        return pl.ds(pl.multiple_of(q * tile, tile), tile)

    def remote(src, dst, send, recv, device):
        return pltpu.make_async_remote_copy(
            src_ref=src, dst_ref=dst, send_sem=send, recv_sem=recv,
            device_id={"expert": device}, device_id_type=MESH,
        )

    def each(body):
        pl.loop(0, chunks)(body)

    raw_load = pltpu.make_async_copy(tokens, raw, raw_sem)
    loads = [
        pltpu.make_async_copy(gate_hbm.at[0], gate, w_sem.at[0]),
        pltpu.make_async_copy(up_hbm.at[0], up, w_sem.at[1]),
        pltpu.make_async_copy(down_hbm.at[0], down, w_sem.at[2]),
    ]
    raw_load.start()

    barrier = pltpu.get_barrier_semaphore()
    peers = [partner, neighbour, near]
    for peer in peers:
        pl.semaphore_signal(barrier, inc=1, device_id={"expert": peer}, device_id_type=MESH)

    @pl.when(inner)
    def _():
        pl.semaphore_signal(barrier, inc=1, device_id={"expert": far}, device_id_type=MESH)

    lane = lax.broadcasted_iota(jnp.int32, (tok_rows, tok_rows), 1)
    line = lax.broadcasted_iota(jnp.int32, (tok_rows, tok_rows), 0)
    expert_of = lax.broadcasted_iota(jnp.int32, (8, tok_rows), 0)
    first, second = ids[0:1, :] == expert_of, ids[1:2, :] == expert_of
    level_0, level_1 = levels[0:1, :].astype(jnp.float32), levels[1:2, :].astype(jnp.float32)
    named = jnp.where(first | second, 1.0, 0.0)
    earlier = jnp.where(line < lane, 1.0, 0.0).astype(jnp.bfloat16)
    rank = jnp.dot(named.astype(jnp.bfloat16), earlier, preferred_element_type=jnp.float32)
    share = jnp.where(first, level_0 / (level_0 + level_1), 0.0)
    share += jnp.where(second, level_1 / (level_0 + level_1), 0.0)
    table[0, 0:8, :] = jnp.where(named > 0.0, rank, 2.0 * tok_rows)
    table[0, 8:16, :] = share

    def matches(k, expert):
        spot = lax.broadcasted_iota(jnp.int32, (cap, tok_rows), 0).astype(jnp.float32)
        return table[k, pl.ds(expert, 1), :] == spot

    def set_pick(k):
        for i, expert in enumerate((plane, near_plane)):
            pick = jnp.where(matches(k, expert), 1.0, 0.0)
            picks[k, i * cap:(i + 1) * cap, :] = pick.astype(picks.dtype)

    def set_mix(k, spot):
        parts = []
        for expert in (plane, near_plane):
            weight = table[k, pl.ds(8 + expert, 1), :]
            parts.append(jnp.where(matches(k, expert), weight, 0.0))
        weight = jnp.transpose(jnp.concatenate(parts, axis=0))
        high = weight.astype(jnp.bfloat16)
        mix[spot, 0] = high
        mix[spot, 1] = (weight - high.astype(jnp.float32)).astype(jnp.bfloat16)

    def select(k, block):
        return jnp.dot(picks[k], block, preferred_element_type=jnp.float32).astype(x.dtype)

    def mixed(spot, own, other):
        both = jnp.concatenate([own, other], axis=0)
        total = jnp.dot(mix[spot, 0], both, preferred_element_type=jnp.float32)
        return total + jnp.dot(mix[spot, 1], both, preferred_element_type=jnp.float32)

    set_pick(0)
    set_mix(0, 0)
    with jax.named_scope("barrier"):
        pl.semaphore_wait(barrier, len(peers) + 1 - kind)

    table_y = remote(table.at[0], table.at[1], table_send.at[0], table_recv.at[0], neighbour)
    table_f = remote(table.at[0], table.at[3 - kind], table_send.at[1], table_recv.at[2 - kind], far)
    table_y.start()

    @pl.when(inner)
    def _():
        for peer in (near, far):
            pl.semaphore_signal(entered, inc=1, device_id={"expert": peer}, device_id_type=MESH)

    def table_arrival(k):
        return remote(table.at[0], table.at[k], table_send.at[0], table_recv.at[k - 1], far)

    def cross_copy(q):
        cols = columns(q)
        return remote(raw.at[:, cols], raw_y.at[:, cols], cross_send, cross_recv.at[q], neighbour)

    def far_copy(q, k):
        cols = columns(q)
        return remote(raw.at[:, cols], raw_f.at[k, :, cols], far_send, far_recv.at[k, q], far)

    def near_copy(k, q):
        cols, slot = columns(q), s if k == 0 else cross_s
        return remote(
            near_stage.at[k, :, cols], x.at[near_j, slot, :, cols],
            near_send.at[k], near_recv.at[k], near,
        )

    def fwd_copy(i, q):
        cols = columns(q)
        return remote(
            raw_f.at[i, pl.ds(0, cap), cols], x.at[2 + i, s, :, cols], fwd_send.at[i], fwd_recv.at[i, q], near
        )

    def y_copy(i, q):
        cols = columns(q)
        return remote(
            x.at[2 + i, s, :, cols], x.at[2 + i, s, :, cols], y_send.at[i], y_recv.at[i, q], neighbour
        )

    def y_arrival(i, q):
        cols = columns(q)
        return remote(
            x.at[2 + i, s, :, cols], x.at[2 + i, cross_s, :, cols],
            y_send.at[i], y_recv.at[i, q], neighbour,
        )

    def d_copy(j, r, q):
        cols, slot = columns(q), r * 2 + core
        return remote(
            x.at[j, slot, :, cols], x.at[j, slot, :, cols], d_send.at[j, r], d_recv.at[j, r], partner
        )

    def d_whole(j, r, lane_core):
        slot = r * 2 + lane_core
        return remote(x.at[j, slot], x.at[j, slot], d_send.at[j, r], d_recv.at[j, r], partner)

    def gathered(j):
        for r in range(2):
            d_whole(j, r, 1 - core).wait_recv()

    def rp_copy(j, t, q, k, slot):
        cols = columns(q)
        return remote(
            x.at[j, slot, :, cols], pair.at[t, k, :, cols],
            rp_send.at[j], rp_recv.at[t, q, k], partner,
        )

    def ry_copy(j, t, q):
        cols = columns(q)
        return remote(
            x.at[j, cross_s, :, cols], cross.at[t, :, cols],
            ry_send.at[j], ry_recv.at[t, q], neighbour,
        )

    def nr_copy(q):
        cols = columns(q)
        return remote(x.at[near_j, s, :, cols], near_ret.at[:, cols], nr_send, nr_recv.at[q], near)

    def or_copy(i, q):
        cols = columns(q)
        return remote(
            x.at[2 + i, s, :, cols], outer_ret.at[i, :, cols], or_send.at[i], or_recv.at[i, q], near
        )

    def fr_copy(i, q):
        cols = columns(q)
        return remote(
            raw_f.at[i, :, cols], far_ret.at[:, cols], fr_send.at[i], fr_recv.at[q],
            far_b if i == 0 else far,
        )

    def folded(q):
        return (q >= 2) & (q < 2 + folds)

    def nx_copy(q):
        return remote(
            x.at[near_j, cross_s, :, columns(q)], near_cross.at[q - 2], nx_send, nx_recv.at[q - 2], near
        )

    def fin_copy(q):
        return remote(
            raw.at[:, columns(q)], raw_y.at[:, columns(q)],
            fin_send, fin_recv.at[q - 2], neighbour,
        )

    def fold(q):
        cols = columns(q)
        with jax.named_scope("w_nx"):
            nx_copy(q).wait_recv()
        total = mixed(3, x[own_j, cross_s, :, cols], near_cross[q - 2])
        raw[:, cols] = total.astype(raw.dtype)
        fin_copy(q).start()

    def expand(j, spot, also=()):
        @each
        def _(q):
            cols = columns(q)
            part = x[j, :, :, cols].reshape(rows, tile)

            @pl.when(q == 0)
            def _():
                acc[...] = jnp.zeros_like(acc)

            acc[0] += jnp.dot(part, gate[cols, :], preferred_element_type=jnp.float32)
            acc[1] += jnp.dot(part, up[cols, :], preferred_element_type=jnp.float32)
            for step in also:
                step(q)

        value = acc[0]
        hidden[spot] = (value / (1.0 + jnp.exp(-value)) * acc[1]).astype(hidden.dtype)

    def contract(j, t, spot, credit, also):
        for r in range(2):
            d_whole(j, r, core).wait_send()
        if j >= 2:
            remote(x.at[j, s], x.at[j, s], y_send.at[j - 2], d_recv.at[j, 0], neighbour).wait_send()
        if credit:
            pl.semaphore_wait(pair_free, 1)
            pl.semaphore_wait(cross_free, 1)

        @pl.loop(0, chunks + 1)
        def _(q):
            @pl.when(q < chunks)
            def _():
                cols = columns(q)
                part = jnp.dot(hidden[spot], down[:, cols], preferred_element_type=jnp.float32)
                x[j, :, :, cols] = part.astype(x.dtype).reshape(SHARDS, cap, tile)
                rp_copy(j, t, q, 1 - row, diag_s).start()
                rp_copy(j, t, q, row, partner_s).start()
                for step in also:
                    step(q)

            @pl.when(q > 0)
            def _():
                cols = columns(q - 1)
                rp_copy(j, t, q - 1, 1 - row, diag_s).wait_recv()
                total = x[j, cross_s, :, cols].astype(jnp.float32)
                total += pair[t, 1 - row, :, cols].astype(jnp.float32)
                x[j, cross_s, :, cols] = total.astype(x.dtype)
                if j >= 2:
                    ry_copy(j, t, q - 1).start()
                else:
                    pl.when(~folded(q - 1))(lambda: ry_copy(j, t, q - 1).start())

                    @pl.when(folded(q - 1))
                    def _():
                        nx_copy(q - 1).start() if j == near_j else fold(q - 1)

    def finish(j, t):
        def step(q):
            cols = columns(q)
            with jax.named_scope("w_rp"):
                rp_copy(j, t, q, row, partner_s).wait_recv()
            total = x[j, s, :, cols].astype(jnp.float32) + pair[t, row, :, cols].astype(jnp.float32)

            def whole():
                with jax.named_scope("w_ry"):
                    ry_copy(j, t, q).wait_recv()
                x[j, s, :, cols] = (total + cross[t, :, cols].astype(jnp.float32)).astype(x.dtype)

            def column_sum():
                x[j, s, :, cols] = total.astype(x.dtype)

            if j >= 2:
                whole()
            else:
                pl.when(~folded(q))(whole)
                pl.when(folded(q))(column_sum)
            if j >= 2:
                @pl.when(outer)
                def _():
                    or_copy(j - 2, q).start()
            elif j == near_j:
                nr_copy(q).start()

        return step

    def release():
        pl.semaphore_signal(pair_free, inc=1, device_id={"expert": partner}, device_id_type=MESH)
        pl.semaphore_signal(cross_free, inc=1, device_id={"expert": neighbour}, device_id_type=MESH)

    def sent(src, dst, send):
        remote(src, dst, send, nr_recv.at[0], near).wait_send()

    def merge(i):
        def step(q):
            @pl.when(inner)
            def _():
                cols = columns(q)

                @pl.when(q == 0)
                def _():
                    sent(raw_f.at[i, pl.ds(0, cap)], near_ret, fwd_send.at[i])
                    with jax.named_scope("w_gate"):
                      if i == 0:
                        sent(near_stage.at[1], near_ret, near_send.at[1])

                with jax.named_scope("w_or"):
                    or_copy(i, q).wait_recv()
                total = mixed(1 + i, x[2 + i, s, :, cols], outer_ret[i, :, cols])
                raw_f[i, :, cols] = total.astype(raw_f.dtype)
                fr_copy(i, q).start()

        return step

    def early(j, t):
        def step(q):
            pl.when(q == chunks // 2 - kind)(lambda: finish(j, t)(0))
            pl.when(q == chunks - 1 - kind)(lambda: finish(j, t)(1))

        return step

    def ahead(j, t):
        def step(q):
            pl.when(q < chunks - 2)(lambda: finish(j, t)(q + 2))

        return step

    def merge_most(i):
        def step(q):
            pl.when(q < chunks - 2)(lambda: merge(i)(q))

        return step

    def merge_last(i):
        def step(q):
            pl.when(q < 2)(lambda: merge(i)(chunks - 2 + q))

        return step

    def near_nth(n):
        pl.when(n < chunks)(lambda: near_copy(0, n).start())
        pl.when(n >= chunks)(lambda: near_copy(1, n - chunks).start())

    def enter(i, q):
        cols = columns(q)

        @pl.when(inner)
        def _():
            with jax.named_scope("w_far"):
                far_copy(q, i).wait_recv()
            taken = select(2 + i, raw_f[i, :, cols])
            x[2 + i, s, :, cols] = taken[:cap]
            raw_f[i, 0:cap, cols] = taken[cap:]
            fwd_copy(i, q).start()

        @pl.when(outer)
        def _():
            with jax.named_scope("w_fwd"):
                fwd_copy(i, q).wait_recv()

        y_copy(i, q).start()
        d_copy(2 + i, row, q).start()

    def far_table(i):
        @pl.when(inner)
        def _():
            table_arrival(2 + i).wait_recv()
            set_pick(2 + i)
            set_mix(2 + i, 1 + i)

    with jax.named_scope("w_raw"):
        raw_load.wait()
    each(lambda q: cross_copy(q).start())
    pl.when(outer)(lambda: pl.semaphore_wait(entered, 1))
    table_f.start()
    each(lambda q: far_copy(q, 1 - kind).start())
    for load in loads:
        load.start()

    with jax.named_scope("take_own"):
        @each
        def _(q):
            cols = columns(q)
            taken = select(0, raw[:, cols])
            near_stage[0, :, cols] = taken[cap:]
            x[own_j, s, :, cols] = taken[:cap]
            d_copy(own_j, row, q).start()

            @pl.when(outer | (q < 2))
            def _():
                near_copy(0, q).start()

    with jax.named_scope("tables"):
        pl.when(inner)(lambda: pl.semaphore_wait(entered, 1))
        table_arrival(1).wait_recv()
        set_pick(1)
        set_mix(1, 3)

        far_table(0)

    with jax.named_scope("enter_b"):
        @each
        def _(q):
            cols = columns(q)
            with jax.named_scope("w_cross"):
                cross_copy(q).wait_recv()
            taken = select(1, raw_y[:, cols])
            near_stage[1, :, cols] = taken[cap:]
            x[own_j, cross_s, :, cols] = taken[:cap]
            d_copy(own_j, 1 - row, q).start()
            enter(0, q)

            pl.when(outer)(lambda: near_copy(1, q).start())
            pl.when(inner & (q % 2 == 1))(lambda: near_copy(0, 2 + q // 2).start())

    pl.when(inner)(lambda: near_nth(2 + chunks // 2))
    pl.when(inner)(lambda: near_nth(3 + chunks // 2))

    with jax.named_scope("wait_own"):
        loads[0].wait()
        loads[1].wait()
        gathered(own_j)
    with jax.named_scope("expand_own"):
        expand(own_j, 0)

    def enter_a(q):
        enter(1, q)
        y_arrival(0, q).wait_recv()
        d_copy(2, 1 - row, q).start()
        pl.when(inner & (q % 2 == 1))(lambda: near_nth(4 + chunks // 2 + q // 2))

    middle = chunks // 2 + 1
    with jax.named_scope("enter_a"):
        far_table(1)
        pl.loop(0, middle)(enter_a)

        @pl.loop(middle, chunks)
        def _(q):
            y_arrival(0, q).wait_recv()
            d_copy(2, 1 - row, q).start()

    with jax.named_scope("wait_b"):
        gathered(2)
    with jax.named_scope("expand_b"):
        expand(2, 1)
    with jax.named_scope("enter_a2"):
        @pl.loop(middle, chunks)
        def _(q):
            enter(1, q)

        @pl.when(inner)
        def _():
            pl.loop(4 + chunks // 2 + middle // 2, 2 * chunks)(near_nth)

    loads[2].wait()
    def spread_a(q):
        y_arrival(1, q).wait_recv()
        d_copy(3, 1 - row, q).start()

    with jax.named_scope("contract_b"):
        contract(2, 0, 1, False, (spread_a,))

    with jax.named_scope("wait_a"):
        gathered(3)
    with jax.named_scope("expand_a"):
        expand(3, 1, (early(2, 0),))
    def spread_near(q):
        @pl.when(q == chunks - 1)
        def _():
            for k, r in ((0, row), (1, 1 - row)):
                slot = r * 2 + core
                remote(near_stage.at[k], x.at[near_j, slot], near_send.at[k], near_recv.at[k], near).wait_recv()
                d_whole(near_j, r, core).start()

    with jax.named_scope("contract_a"):
        contract(3, 1, 1, False, (ahead(2, 0), merge_most(0), spread_near))
        release()

    with jax.named_scope("wait_near"):
        gathered(near_j)
    with jax.named_scope("expand_near"):
        expand(near_j, 1, (early(3, 1),))
    with jax.named_scope("contract_near"):
        contract(near_j, 0, 1, True, (merge_last(0), ahead(3, 1), merge_most(1)))
        release()
    def merge_late(q):
        pl.when(q >= chunks - 2)(lambda: merge(1)(q))

    sent(raw, raw_y, cross_send)
    sent(raw, raw_y, far_send)
    with jax.named_scope("contract_own"):
        contract(own_j, 1, 0, True, (finish(near_j, 0), merge_late))

    with jax.named_scope("combine"):
        @each
        def _(q):
            cols = columns(q)
            with jax.named_scope("w_own"):
                finish(own_j, 1)(q)
            with jax.named_scope("w_nr"):
                nr_copy(q).wait_recv()
            with jax.named_scope("w_fr"):
                fr_copy(0, q).wait_recv()
            total = mixed(0, x[own_j, s, :, cols], near_ret[:, cols])
            total += far_ret[:, cols].astype(jnp.float32)

            @pl.when(~folded(q))
            def _():
                far_ret[:, cols] = total.astype(far_ret.dtype)

            @pl.when(folded(q))
            def _():
                with jax.named_scope("w_fin"):
                    fin_copy(q).wait_recv()
                rest = raw_y[:, cols].astype(jnp.float32)
                far_ret[:, cols] = (total + rest).astype(far_ret.dtype)


    with jax.named_scope("tail_sends"):
        table_y.wait_send()
        table_f.wait_send()
        sent(near_stage.at[0], near_ret, near_send.at[0])
        sent(x.at[near_j, s], near_ret, nr_send)
        for j in range(4):
            sent(x.at[j, pl.ds(0, 2)], pair.at[0], rp_send.at[j])
            part = pl.ds(0, width if j >= 2 else width - folds * tile)
            sent(x.at[j, cross_s, :, part], near_ret.at[:, part], ry_send.at[j])
        sent(near_cross, near_cross, nx_send)
        part = pl.ds(0, folds * tile)
        sent(raw.at[:, part], far_ret.at[:, part], fin_send)

        @pl.when(inner)
        def _():
            for i in range(2):
                sent(raw_f.at[i], far_ret, fr_send.at[i])

        @pl.when(outer)
        def _():
            sent(near_stage.at[1], near_ret, near_send.at[1])
            for i in range(2):
                sent(x.at[2 + i, s], near_ret, or_send.at[i])


def routed(tokens, route_ids, levels, w_gate, w_up, w_down, cap):
    tok_rows, width = tokens.shape
    ff, dtype = w_gate.shape[2], tokens.dtype
    rows, chunks = SHARDS * cap, width // tile_of(width, 1024)
    folds = chunks * 3 // 7
    dma, vmem = pltpu.SemaphoreType.DMA, pltpu.VMEM
    anywhere, local = pl.BlockSpec(memory_space=pl.ANY), pl.BlockSpec(memory_space=pltpu.VMEM)
    return pl.pallas_call(
        routed_kernel,
        out_shape=pltpu.VMEM((tok_rows, width), dtype),
        in_specs=[anywhere, local, local, anywhere, anywhere, anywhere],
        out_specs=local,
        scratch_shapes=[
            vmem((4, SHARDS, cap, width), dtype),
            vmem((width, ff), dtype),
            vmem((width, ff), dtype),
            vmem((ff, width), dtype),
            vmem((2, rows, ff), jnp.float32),
            vmem((2, rows, ff), dtype),
            vmem((2, 2, cap, width), dtype),
            vmem((2, cap, width), dtype),
            vmem((tok_rows, width), dtype),
            vmem((tok_rows, width), dtype),
            vmem((2, tok_rows, width), dtype),
            vmem((2, cap, width), dtype),
            vmem((cap, width), dtype),
            vmem((folds, cap, width // chunks), dtype),
            vmem((2, cap, width), dtype),
            vmem((4, 16, tok_rows), jnp.float32),
            vmem((4, 2 * cap, tok_rows), dtype),
            vmem((4, 2, tok_rows, 2 * cap), dtype),
            dma((3,)), dma, dma((2,)), dma((3,)),
            dma, dma((chunks,)), dma, dma((2, chunks)),
            dma((2,)), dma((2,)),
            dma((2,)), dma((2, chunks)),
            dma((2,)), dma((2, chunks)),
            dma((4, 2)), dma((4, 2)),
            dma((4,)), dma((2, chunks, 2)),
            dma((4,)), dma((2, chunks)),
            dma, dma((chunks,)),
            dma((2,)), dma((2, chunks)),
            dma((2,)), dma((chunks,)),
            dma, dma((folds,)), dma, dma((folds,)),
            pltpu.SemaphoreType.REGULAR, pltpu.SemaphoreType.REGULAR,
            pltpu.SemaphoreType.REGULAR,
        ],
        compiler_params=pltpu.CompilerParams(
            collective_id=0, has_side_effects=True, vmem_limit_bytes=65_200_000
        ),
    )(tokens, route_ids.T, levels.T, w_gate, w_up, w_down)


def combine_kernel(weight_ref, ret_ref, out_ref):
    weight = weight_ref[...]
    high = weight.astype(jnp.bfloat16)
    low = (weight - high.astype(jnp.float32)).astype(jnp.bfloat16)
    total = jnp.dot(high, ret_ref[...], preferred_element_type=jnp.float32)
    total += jnp.dot(low, ret_ref[...], preferred_element_type=jnp.float32)
    out_ref[...] = total.astype(out_ref.dtype)


def on_device(tokens, route_ids, levels, w_gate, w_up, w_down):
    tok_rows, width = tokens.shape
    top = route_ids.shape[1]
    ff = w_gate.shape[2]
    experts = lax.axis_size("expert") // SHARDS
    capacity = 5 * tok_rows * top // (4 * experts)
    cap = -(-capacity // 16) * 16
    slots = experts * cap
    dtype = tokens.dtype
    if experts == 4 and top == 2 and tok_rows < 2 * cap:
        return routed(tokens, route_ids, levels, w_gate, w_up, w_down, cap)

    chosen = route_ids[:, :, None] == jnp.arange(experts, dtype=jnp.int32)
    named = jnp.any(chosen, axis=1)
    index = jnp.arange(tok_rows, dtype=jnp.int32)
    earlier = (index[:, None] > index[None, :]).astype(jnp.bfloat16)
    rank = jnp.dot(earlier, named.astype(jnp.bfloat16), preferred_element_type=jnp.float32)
    place = jnp.where(named, rank.astype(jnp.int32), cap)
    level_f = levels.astype(jnp.float32)
    weights = level_f / jnp.sum(level_f, axis=1, keepdims=True)
    weight_e = jnp.sum(jnp.where(chosen, weights[:, :, None], 0.0), axis=1)
    spot = jnp.arange(cap, dtype=jnp.int32)
    pick = (place[:, :, None] == spot).reshape(tok_rows, slots)
    weight_m = jnp.where(pick, jnp.repeat(weight_e, cap, axis=1), 0.0)
    outgoing = lax.dot_general(
        pick.astype(dtype), tokens, (((0,), (0,)), ((), ())), preferred_element_type=jnp.float32
    ).astype(dtype).reshape(experts, cap, width)

    dma, anywhere = pltpu.SemaphoreType.DMA, pl.BlockSpec(memory_space=pl.ANY)
    rows, chunks = SHARDS * cap, width // tile_of(width, 1024)
    returned = pl.pallas_call(
        functools.partial(layer_kernel, experts),
        out_shape=jax.ShapeDtypeStruct((experts, cap, width), dtype),
        in_specs=[anywhere] * 4,
        out_specs=anywhere,
        scratch_shapes=[
            pltpu.VMEM((experts, SHARDS, cap, width), dtype),
            pltpu.VMEM((width, ff), dtype),
            pltpu.VMEM((width, ff), dtype),
            pltpu.VMEM((ff, width), dtype),
            pltpu.VMEM((2, rows, ff), jnp.float32),
            pltpu.VMEM((rows, ff), dtype),
            pltpu.VMEM((experts, 2, cap, width), dtype),
            pltpu.VMEM((experts, cap, width), dtype),
            dma((3,)),
            dma((experts,)), dma((experts,)),
            dma((experts,)), dma((experts,)),
            dma((experts, 2)), dma((experts, 2)),
            dma((experts, chunks, 2)), dma((experts, chunks, 2)),
            dma((experts, chunks)), dma((experts, chunks)),
            dma((experts, chunks)), dma((experts, chunks)),
        ],
        compiler_params=pltpu.CompilerParams(
            collective_id=0, has_side_effects=True, vmem_limit_bytes=67_000_000
        ),
    )(outgoing, w_gate, w_up, w_down)

    tile = tile_of(width, 1024)
    return pl.pallas_call(
        combine_kernel,
        out_shape=jax.ShapeDtypeStruct((tok_rows, width), dtype),
        grid=(width // tile,),
        in_specs=[
            pl.BlockSpec((tok_rows, slots), lambda n: (0, 0)),
            pl.BlockSpec((slots, tile), lambda n: (0, n)),
        ],
        out_specs=pl.BlockSpec((tok_rows, tile), lambda n: (0, n)),
    )(weight_m, returned.reshape(slots, width))


def solution(mesh):
    return jax.shard_map(
        on_device,
        mesh=mesh,
        in_specs=(
            P(("groups", "expert"), None),
            P(("groups", "expert"), None),
            P(("groups", "expert"), None),
            P("expert", None, None),
            P("expert", None, None),
            P("expert", None, None),
        ),
        out_specs=P(("groups", "expert"), None),
        check_vma=False,
    )
```

```python
import functools

import jax
import jax.numpy as jnp
from jax import lax
from jax.experimental import pallas as pl
from jax.experimental.pallas import tpu as pltpu
from jax.sharding import PartitionSpec as P

SHARDS = 4
MESH = pl.DeviceIdType.MESH


def tile_of(length, most):
    size = most
    while length % size:
        size //= 2
    return size


def xor(a, mask, count):
    total, bit = 0, 1
    while bit < count:
        total += (a // bit + mask // bit) % 2 * bit
        bit *= 2
    return total


def layer_kernel(
    planes, out_ref, gate_hbm, up_hbm, down_hbm, ret_ref,
    x, gate, up, down, acc, hidden, pair, cross,
    w_sem, z_send, z_recv, y_send, y_recv, p_send, p_recv,
    rp_send, rp_recv, ry_send, ry_recv, rz_send, rz_recv,
):
    me = lax.axis_index("expert")
    plane, s = me // SHARDS, me % SHARDS
    base = plane * SHARDS
    core, row = s % 2, s // 2
    partner_s = row * 2 + (1 - core)
    cross_s = (1 - row) * 2 + core
    diag_s = (1 - row) * 2 + (1 - core)
    partner, neighbour = base + partner_s, base + cross_s
    cap, width = x.shape[2], x.shape[3]
    rows = SHARDS * cap
    tile = tile_of(width, 1024)
    chunks = width // tile

    barrier = pltpu.get_barrier_semaphore()
    peers = [partner, neighbour]
    peers += [xor(plane, j, planes) * SHARDS + s for j in range(1, planes)]
    for peer in peers:
        pl.semaphore_signal(barrier, inc=1, device_id={"expert": peer}, device_id_type=MESH)
    pl.semaphore_wait(barrier, planes + 1)

    def remote(src, dst, send, recv, device):
        return pltpu.make_async_remote_copy(
            src_ref=src, dst_ref=dst, send_sem=send, recv_sem=recv,
            device_id={"expert": device}, device_id_type=MESH,
        )

    def columns(q):
        return pl.ds(pl.multiple_of(q * tile, tile), tile)

    def out_copy(j):
        to = xor(plane, j, planes)
        return remote(out_ref.at[to], x.at[j, s], z_send.at[j], z_recv.at[j], to * SHARDS + s)

    def own_copy():
        return pltpu.make_async_copy(out_ref.at[plane], x.at[0, s], z_recv.at[0])

    def y_copy(j):
        return remote(x.at[j, s], x.at[j, s], y_send.at[j], y_recv.at[j], neighbour)

    def y_arrival(j):
        return remote(x.at[j, cross_s], x.at[j, cross_s], y_send.at[j], y_recv.at[j], neighbour)

    def p_copy(j, k, slot):
        return remote(x.at[j, slot], x.at[j, slot], p_send.at[j, k], p_recv.at[j, k], partner)

    def rp_copy(j, q, k, slot):
        cols = columns(q)
        return remote(
            x.at[j, slot, :, cols], pair.at[j, k, :, cols],
            rp_send.at[j, q, k], rp_recv.at[j, q, k], partner,
        )

    def ry_copy(j, q):
        cols = columns(q)
        return remote(
            x.at[j, cross_s, :, cols], cross.at[j, :, cols],
            ry_send.at[j, q], ry_recv.at[j, q], neighbour,
        )

    def rz_copy(j, q):
        cols, to = columns(q), xor(plane, j, planes)
        return remote(
            x.at[j, s, :, cols], ret_ref.at[plane, :, cols],
            rz_send.at[j, q], rz_recv.at[j, q], to * SHARDS + s,
        )

    def keep_copy(q):
        cols = columns(q)
        return pltpu.make_async_copy(x.at[0, s, :, cols], ret_ref.at[plane, :, cols], rz_send.at[0, q])

    own_copy().start()
    for distance in range(1, planes):
        for to in (plane + distance, plane - distance):
            @pl.when((to >= 0) & (to < planes))
            def _():
                mask = xor(plane, to, planes)
                remote(
                    out_ref.at[to], x.at[mask, s], z_send.at[mask], z_recv.at[mask], to * SHARDS + s
                ).start()
    loads = [
        pltpu.make_async_copy(gate_hbm.at[0], gate, w_sem.at[0]),
        pltpu.make_async_copy(up_hbm.at[0], up, w_sem.at[1]),
        pltpu.make_async_copy(down_hbm.at[0], down, w_sem.at[2]),
    ]
    for load in loads:
        load.start()

    def arrive(j):
        if j == 0:
            own_copy().wait()
        else:
            out_copy(j).wait_recv()
        y_copy(j).start()
        p_copy(j, 0, s).start()

    def gather(j):
        y_arrival(j).wait_recv()
        p_copy(j, 1, cross_s).start()
        p_copy(j, 0, partner_s).wait_recv()
        p_copy(j, 1, diag_s).wait_recv()

    def expand(j):
        @pl.loop(0, chunks)
        def _(q):
            cols = columns(q)
            part = x[j, :, :, cols].reshape(rows, tile)

            @pl.when(q == 0)
            def _():
                acc[...] = jnp.zeros_like(acc)

            acc[0] += jnp.dot(part, gate[cols, :], preferred_element_type=jnp.float32)
            acc[1] += jnp.dot(part, up[cols, :], preferred_element_type=jnp.float32)

        value = acc[0]
        hidden[...] = (value / (1.0 + jnp.exp(-value)) * acc[1]).astype(hidden.dtype)

    def contract(j):
        y_copy(j).wait_send()
        p_copy(j, 0, s).wait_send()
        p_copy(j, 1, cross_s).wait_send()

        @pl.loop(0, chunks + 1)
        def _(q):
            @pl.when(q < chunks)
            def _():
                cols = columns(q)
                part = jnp.dot(hidden[...], down[:, cols], preferred_element_type=jnp.float32)
                x[j, :, :, cols] = part.astype(x.dtype).reshape(SHARDS, cap, tile)
                rp_copy(j, q, 1 - row, diag_s).start()
                rp_copy(j, q, row, partner_s).start()

            @pl.when(q > 0)
            def _():
                cols = columns(q - 1)
                rp_copy(j, q - 1, 1 - row, diag_s).wait_recv()
                total = x[j, cross_s, :, cols].astype(jnp.float32)
                total += pair[j, 1 - row, :, cols].astype(jnp.float32)
                x[j, cross_s, :, cols] = total.astype(x.dtype)
                ry_copy(j, q - 1).start()

    def finish(j):
        @pl.loop(0, chunks)
        def _(q):
            cols = columns(q)
            rp_copy(j, q, row, partner_s).wait_recv()
            total = x[j, s, :, cols].astype(jnp.float32) + pair[j, row, :, cols].astype(jnp.float32)
            ry_copy(j, q).wait_recv()
            x[j, s, :, cols] = (total + cross[j, :, cols].astype(jnp.float32)).astype(x.dtype)
            if j > 0:
                rz_copy(j, q).start()
            else:
                keep_copy(q).start()

    order = [0, *range(2, planes), 1]
    arrive(0)
    arrive(1)
    for i, j in enumerate(order):
        gather(j)
        if 0 < i < planes - 2:
            arrive(order[i + 1])
        if i == 0:
            for load in loads:
                load.wait()
        expand(j)
        contract(j)
        if i == 0:
            arrive(order[1])
        else:
            finish(order[i - 1])
    finish(order[-1])

    for j in range(planes):
        @pl.loop(0, chunks)
        def _(q):
            rp_copy(j, q, 1 - row, diag_s).wait_send()
            rp_copy(j, q, row, partner_s).wait_send()
            ry_copy(j, q).wait_send()
            if j > 0:
                rz_copy(j, q).wait()
            else:
                keep_copy(q).wait()
        if j > 0:
            out_copy(j).wait_send()


def routed_kernel(
    tokens, ids, levels, gate_hbm, up_hbm, down_hbm, far_ret,
    x, gate, up, down, acc, hidden, pair, cross, raw, raw_y, raw_f,
    near_stage, near_ret, near_cross, outer_ret, table, picks, mix,
    w_sem, raw_sem, table_send, table_recv,
    cross_send, cross_recv, far_send, far_recv, near_send, near_recv,
    fwd_send, fwd_recv, y_send, y_recv, d_send, d_recv,
    rp_send, rp_recv, ry_send, ry_recv,
    nr_send, nr_recv, or_send, or_recv, fr_send, fr_recv,
    nx_send, nx_recv, fin_send, fin_recv,
    pair_free, cross_free, entered,
):
    me = lax.axis_index("expert")
    plane, s = me // SHARDS, me % SHARDS
    core, row = s % 2, s // 2
    half, near_plane = plane // 2, xor(plane, 1, 4)
    far_plane = 2 * (1 - half) + half
    kind = (plane + half + 1) % 2
    inner, outer = kind == 0, kind == 1
    cross_s = (1 - row) * 2 + core
    partner_s = row * 2 + (1 - core)
    diag_s = (1 - row) * 2 + (1 - core)
    partner, neighbour = plane * SHARDS + partner_s, plane * SHARDS + cross_s
    near, far = near_plane * SHARDS + s, far_plane * SHARDS + s
    far_b = xor(far_plane, 1, 4) * SHARDS + s
    cap, width = x.shape[2], x.shape[3]
    tok_rows = raw.shape[0]
    rows = SHARDS * cap
    tile = tile_of(width, 1024)
    chunks = width // tile
    own_j, near_j = 0, 1
    folds = near_cross.shape[0]

    def columns(q):
        return pl.ds(pl.multiple_of(q * tile, tile), tile)

    def remote(src, dst, send, recv, device):
        return pltpu.make_async_remote_copy(
            src_ref=src, dst_ref=dst, send_sem=send, recv_sem=recv,
            device_id={"expert": device}, device_id_type=MESH,
        )

    def each(body):
        pl.loop(0, chunks)(body)

    raw_load = pltpu.make_async_copy(tokens, raw, raw_sem)
    loads = [
        pltpu.make_async_copy(gate_hbm.at[0], gate, w_sem.at[0]),
        pltpu.make_async_copy(up_hbm.at[0], up, w_sem.at[1]),
        pltpu.make_async_copy(down_hbm.at[0], down, w_sem.at[2]),
    ]
    raw_load.start()

    barrier = pltpu.get_barrier_semaphore()
    peers = [partner, neighbour, near]
    for peer in peers:
        pl.semaphore_signal(barrier, inc=1, device_id={"expert": peer}, device_id_type=MESH)

    @pl.when(inner)
    def _():
        pl.semaphore_signal(barrier, inc=1, device_id={"expert": far}, device_id_type=MESH)

    lane = lax.broadcasted_iota(jnp.int32, (tok_rows, tok_rows), 1)
    line = lax.broadcasted_iota(jnp.int32, (tok_rows, tok_rows), 0)
    expert_of = lax.broadcasted_iota(jnp.int32, (8, tok_rows), 0)
    first, second = ids[0:1, :] == expert_of, ids[1:2, :] == expert_of
    level_0, level_1 = levels[0:1, :].astype(jnp.float32), levels[1:2, :].astype(jnp.float32)
    named = jnp.where(first | second, 1.0, 0.0)
    earlier = jnp.where(line < lane, 1.0, 0.0).astype(jnp.bfloat16)
    rank = jnp.dot(named.astype(jnp.bfloat16), earlier, preferred_element_type=jnp.float32)
    share = jnp.where(first, level_0 / (level_0 + level_1), 0.0)
    share += jnp.where(second, level_1 / (level_0 + level_1), 0.0)
    table[0, 0:8, :] = jnp.where(named > 0.0, rank, 2.0 * tok_rows)
    table[0, 8:16, :] = share

    def matches(k, expert):
        spot = lax.broadcasted_iota(jnp.int32, (cap, tok_rows), 0).astype(jnp.float32)
        return table[k, pl.ds(expert, 1), :] == spot

    def set_pick(k):
        for i, expert in enumerate((plane, near_plane)):
            pick = jnp.where(matches(k, expert), 1.0, 0.0)
            picks[k, i * cap:(i + 1) * cap, :] = pick.astype(picks.dtype)

    def set_mix(k, spot):
        parts = []
        for expert in (plane, near_plane):
            weight = table[k, pl.ds(8 + expert, 1), :]
            parts.append(jnp.where(matches(k, expert), weight, 0.0))
        weight = jnp.transpose(jnp.concatenate(parts, axis=0))
        high = weight.astype(jnp.bfloat16)
        mix[spot, 0] = high
        mix[spot, 1] = (weight - high.astype(jnp.float32)).astype(jnp.bfloat16)

    def select(k, block):
        return jnp.dot(picks[k], block, preferred_element_type=jnp.float32).astype(x.dtype)

    def mixed(spot, own, other):
        both = jnp.concatenate([own, other], axis=0)
        total = jnp.dot(mix[spot, 0], both, preferred_element_type=jnp.float32)
        return total + jnp.dot(mix[spot, 1], both, preferred_element_type=jnp.float32)

    set_pick(0)
    set_mix(0, 0)
    with jax.named_scope("barrier"):
        pl.semaphore_wait(barrier, len(peers) + 1 - kind)

    table_y = remote(table.at[0], table.at[1], table_send.at[0], table_recv.at[0], neighbour)
    table_f = remote(table.at[0], table.at[3 - kind], table_send.at[1], table_recv.at[2 - kind], far)
    table_y.start()

    @pl.when(inner)
    def _():
        for peer in (near, far):
            pl.semaphore_signal(entered, inc=1, device_id={"expert": peer}, device_id_type=MESH)

    def table_arrival(k):
        return remote(table.at[0], table.at[k], table_send.at[0], table_recv.at[k - 1], far)

    def cross_copy(q):
        cols = columns(q)
        return remote(raw.at[:, cols], raw_y.at[:, cols], cross_send, cross_recv.at[q], neighbour)

    def far_copy(q, k):
        cols = columns(q)
        return remote(raw.at[:, cols], raw_f.at[k, :, cols], far_send, far_recv.at[k, q], far)

    def near_copy(k, q):
        cols, slot = columns(q), s if k == 0 else cross_s
        return remote(
            near_stage.at[k, :, cols], x.at[near_j, slot, :, cols],
            near_send.at[k], near_recv.at[k], near,
        )

    def fwd_copy(i, q):
        cols = columns(q)
        return remote(
            raw_f.at[i, pl.ds(0, cap), cols], x.at[2 + i, s, :, cols], fwd_send.at[i], fwd_recv.at[i, q], near
        )

    def y_copy(i, q):
        cols = columns(q)
        return remote(
            x.at[2 + i, s, :, cols], x.at[2 + i, s, :, cols], y_send.at[i], y_recv.at[i, q], neighbour
        )

    def y_arrival(i, q):
        cols = columns(q)
        return remote(
            x.at[2 + i, s, :, cols], x.at[2 + i, cross_s, :, cols],
            y_send.at[i], y_recv.at[i, q], neighbour,
        )

    def d_copy(j, r, q):
        cols, slot = columns(q), r * 2 + core
        return remote(
            x.at[j, slot, :, cols], x.at[j, slot, :, cols], d_send.at[j, r], d_recv.at[j, r], partner
        )

    def d_whole(j, r, lane_core):
        slot = r * 2 + lane_core
        return remote(x.at[j, slot], x.at[j, slot], d_send.at[j, r], d_recv.at[j, r], partner)

    def gathered(j):
        for r in range(2):
            d_whole(j, r, 1 - core).wait_recv()

    def rp_copy(j, t, q, k, slot):
        cols = columns(q)
        return remote(
            x.at[j, slot, :, cols], pair.at[t, k, :, cols],
            rp_send.at[j], rp_recv.at[t, q, k], partner,
        )

    def ry_copy(j, t, q):
        cols = columns(q)
        return remote(
            x.at[j, cross_s, :, cols], cross.at[t, :, cols],
            ry_send.at[j], ry_recv.at[t, q], neighbour,
        )

    def nr_copy(q):
        cols = columns(q)
        return remote(x.at[near_j, s, :, cols], near_ret.at[:, cols], nr_send, nr_recv.at[q], near)

    def or_copy(i, q):
        cols = columns(q)
        return remote(
            x.at[2 + i, s, :, cols], outer_ret.at[i, :, cols], or_send.at[i], or_recv.at[i, q], near
        )

    def fr_copy(i, q):
        cols = columns(q)
        return remote(
            raw_f.at[i, :, cols], far_ret.at[:, cols], fr_send.at[i], fr_recv.at[q],
            far_b if i == 0 else far,
        )

    def folded(q):
        return (q >= 2) & (q < 2 + folds)

    def nx_copy(q):
        return remote(
            x.at[near_j, cross_s, :, columns(q)], near_cross.at[q - 2], nx_send, nx_recv.at[q - 2], near
        )

    def fin_copy(q):
        return remote(
            raw.at[:, columns(q)], raw_y.at[:, columns(q)],
            fin_send, fin_recv.at[q - 2], neighbour,
        )

    def fold(q):
        cols = columns(q)
        with jax.named_scope("w_nx"):
            nx_copy(q).wait_recv()
        total = mixed(3, x[own_j, cross_s, :, cols], near_cross[q - 2])
        raw[:, cols] = total.astype(raw.dtype)
        fin_copy(q).start()

    def expand(j, spot, also=()):
        @each
        def _(q):
            cols = columns(q)
            part = x[j, :, :, cols].reshape(rows, tile)

            @pl.when(q == 0)
            def _():
                acc[...] = jnp.zeros_like(acc)

            acc[0] += jnp.dot(part, gate[cols, :], preferred_element_type=jnp.float32)
            acc[1] += jnp.dot(part, up[cols, :], preferred_element_type=jnp.float32)
            for step in also:
                step(q)

        value = acc[0]
        hidden[spot] = (value / (1.0 + jnp.exp(-value)) * acc[1]).astype(hidden.dtype)

    def contract(j, t, spot, credit, also):
        for r in range(2):
            d_whole(j, r, core).wait_send()
        if j >= 2:
            remote(x.at[j, s], x.at[j, s], y_send.at[j - 2], d_recv.at[j, 0], neighbour).wait_send()
        if credit:
            pl.semaphore_wait(pair_free, 1)
            pl.semaphore_wait(cross_free, 1)

        @pl.loop(0, chunks + 1)
        def _(q):
            @pl.when(q < chunks)
            def _():
                cols = columns(q)
                part = jnp.dot(hidden[spot], down[:, cols], preferred_element_type=jnp.float32)
                x[j, :, :, cols] = part.astype(x.dtype).reshape(SHARDS, cap, tile)
                rp_copy(j, t, q, 1 - row, diag_s).start()
                rp_copy(j, t, q, row, partner_s).start()
                for step in also:
                    step(q)

            @pl.when(q > 0)
            def _():
                cols = columns(q - 1)
                rp_copy(j, t, q - 1, 1 - row, diag_s).wait_recv()
                total = x[j, cross_s, :, cols].astype(jnp.float32)
                total += pair[t, 1 - row, :, cols].astype(jnp.float32)
                x[j, cross_s, :, cols] = total.astype(x.dtype)
                if j >= 2:
                    ry_copy(j, t, q - 1).start()
                else:
                    pl.when(~folded(q - 1))(lambda: ry_copy(j, t, q - 1).start())

                    @pl.when(folded(q - 1))
                    def _():
                        nx_copy(q - 1).start() if j == near_j else fold(q - 1)

    def finish(j, t):
        def step(q):
            cols = columns(q)
            with jax.named_scope("w_rp"):
                rp_copy(j, t, q, row, partner_s).wait_recv()
            total = x[j, s, :, cols].astype(jnp.float32) + pair[t, row, :, cols].astype(jnp.float32)

            def whole():
                with jax.named_scope("w_ry"):
                    ry_copy(j, t, q).wait_recv()
                x[j, s, :, cols] = (total + cross[t, :, cols].astype(jnp.float32)).astype(x.dtype)

            def column_sum():
                x[j, s, :, cols] = total.astype(x.dtype)

            if j >= 2:
                whole()
            else:
                pl.when(~folded(q))(whole)
                pl.when(folded(q))(column_sum)
            if j >= 2:
                @pl.when(outer)
                def _():
                    or_copy(j - 2, q).start()
            elif j == near_j:
                nr_copy(q).start()

        return step

    def release():
        pl.semaphore_signal(pair_free, inc=1, device_id={"expert": partner}, device_id_type=MESH)
        pl.semaphore_signal(cross_free, inc=1, device_id={"expert": neighbour}, device_id_type=MESH)

    def sent(src, dst, send):
        remote(src, dst, send, nr_recv.at[0], near).wait_send()

    def merge(i):
        def step(q):
            @pl.when(inner)
            def _():
                cols = columns(q)

                @pl.when(q == 0)
                def _():
                    sent(raw_f.at[i, pl.ds(0, cap)], near_ret, fwd_send.at[i])
                    with jax.named_scope("w_gate"):
                        if i == 0:
                            sent(near_stage.at[1], near_ret, near_send.at[1])

                with jax.named_scope("w_or"):
                    or_copy(i, q).wait_recv()
                total = mixed(1 + i, x[2 + i, s, :, cols], outer_ret[i, :, cols])
                raw_f[i, :, cols] = total.astype(raw_f.dtype)
                fr_copy(i, q).start()

        return step

    def early(j, t):
        def step(q):
            pl.when(q == chunks // 2 - kind)(lambda: finish(j, t)(0))
            pl.when(q == chunks - 1 - kind)(lambda: finish(j, t)(1))

        return step

    def ahead(j, t):
        def step(q):
            pl.when(q < chunks - 2)(lambda: finish(j, t)(q + 2))

        return step

    def merge_most(i):
        def step(q):
            pl.when(q < chunks - 2)(lambda: merge(i)(q))

        return step

    def merge_last(i):
        def step(q):
            pl.when(q < 2)(lambda: merge(i)(chunks - 2 + q))

        return step

    def near_nth(n):
        pl.when(n < chunks)(lambda: near_copy(0, n).start())
        pl.when(n >= chunks)(lambda: near_copy(1, n - chunks).start())

    def enter(i, q):
        cols = columns(q)

        @pl.when(inner)
        def _():
            with jax.named_scope("w_far"):
                far_copy(q, i).wait_recv()
            taken = select(2 + i, raw_f[i, :, cols])
            x[2 + i, s, :, cols] = taken[:cap]
            raw_f[i, 0:cap, cols] = taken[cap:]
            fwd_copy(i, q).start()

        @pl.when(outer)
        def _():
            with jax.named_scope("w_fwd"):
                fwd_copy(i, q).wait_recv()

        y_copy(i, q).start()
        d_copy(2 + i, row, q).start()

    def far_table(i):
        @pl.when(inner)
        def _():
            table_arrival(2 + i).wait_recv()
            set_pick(2 + i)
            set_mix(2 + i, 1 + i)

    with jax.named_scope("w_raw"):
        raw_load.wait()
    each(lambda q: cross_copy(q).start())
    pl.when(outer)(lambda: pl.semaphore_wait(entered, 1))
    table_f.start()
    each(lambda q: far_copy(q, 1 - kind).start())
    for load in loads:
        load.start()

    with jax.named_scope("take_own"):
        @each
        def _(q):
            cols = columns(q)
            taken = select(0, raw[:, cols])
            near_stage[0, :, cols] = taken[cap:]
            x[own_j, s, :, cols] = taken[:cap]
            d_copy(own_j, row, q).start()

            @pl.when(outer | (q < 4))
            def _():
                near_copy(0, q).start()

    with jax.named_scope("tables"):
        pl.when(inner)(lambda: pl.semaphore_wait(entered, 1))
        table_arrival(1).wait_recv()
        set_pick(1)
        set_mix(1, 3)

        far_table(0)

    with jax.named_scope("enter_b"):
        @each
        def _(q):
            cols = columns(q)
            with jax.named_scope("w_cross"):
                cross_copy(q).wait_recv()
            taken = select(1, raw_y[:, cols])
            near_stage[1, :, cols] = taken[cap:]
            x[own_j, cross_s, :, cols] = taken[:cap]
            d_copy(own_j, 1 - row, q).start()
            enter(0, q)

            pl.when(outer)(lambda: near_copy(1, q).start())
            pl.when(inner & (q % 2 == 1))(lambda: near_copy(0, 4 + q // 2).start())


    with jax.named_scope("wait_own"):
        loads[0].wait()
        loads[1].wait()
        gathered(own_j)
    with jax.named_scope("expand_own"):
        expand(own_j, 0)

    def enter_a(q):
        enter(1, q)
        y_arrival(0, q).wait_recv()
        d_copy(2, 1 - row, q).start()
        pl.when(inner & (q % 2 == 1))(lambda: near_nth(4 + chunks // 2 + q // 2))

    middle = chunks // 2 + 1
    with jax.named_scope("enter_a"):
        far_table(1)
        pl.loop(0, middle)(enter_a)

        @pl.loop(middle, chunks)
        def _(q):
            y_arrival(0, q).wait_recv()
            d_copy(2, 1 - row, q).start()

    with jax.named_scope("wait_b"):
        gathered(2)
    with jax.named_scope("expand_b"):
        expand(2, 1)
    with jax.named_scope("enter_a2"):
        @pl.loop(middle, chunks)
        def _(q):
            enter(1, q)

        @pl.when(inner)
        def _():
            pl.loop(4 + chunks // 2 + middle // 2, 2 * chunks)(near_nth)

    loads[2].wait()
    def spread_a(q):
        y_arrival(1, q).wait_recv()
        d_copy(3, 1 - row, q).start()

    with jax.named_scope("contract_b"):
        contract(2, 0, 1, False, (spread_a,))

    with jax.named_scope("wait_a"):
        gathered(3)
    with jax.named_scope("expand_a"):
        expand(3, 1, (early(2, 0),))
    def spread_near(q):
        @pl.when(q == chunks - 1)
        def _():
            for k, r in ((0, row), (1, 1 - row)):
                slot = r * 2 + core
                remote(near_stage.at[k], x.at[near_j, slot], near_send.at[k], near_recv.at[k], near).wait_recv()
                d_whole(near_j, r, core).start()

    with jax.named_scope("contract_a"):
        contract(3, 1, 1, False, (ahead(2, 0), merge_most(0), spread_near))
        release()

    with jax.named_scope("wait_near"):
        gathered(near_j)
    with jax.named_scope("expand_near"):
        expand(near_j, 1, (early(3, 1),))
    with jax.named_scope("contract_near"):
        contract(near_j, 0, 1, True, (merge_last(0), ahead(3, 1), merge_most(1)))
        release()
    def merge_late(q):
        pl.when(q >= chunks - 2)(lambda: merge(1)(q))

    sent(raw, raw_y, cross_send)
    sent(raw, raw_y, far_send)
    with jax.named_scope("contract_own"):
        contract(own_j, 1, 0, True, (finish(near_j, 0), merge_late))

    with jax.named_scope("combine"):
        @each
        def _(q):
            cols = columns(q)
            with jax.named_scope("w_own"):
                finish(own_j, 1)(q)
            with jax.named_scope("w_nr"):
                nr_copy(q).wait_recv()
            with jax.named_scope("w_fr"):
                fr_copy(0, q).wait_recv()
            total = mixed(0, x[own_j, s, :, cols], near_ret[:, cols])
            total += far_ret[:, cols].astype(jnp.float32)

            @pl.when(~folded(q))
            def _():
                far_ret[:, cols] = total.astype(far_ret.dtype)

            @pl.when(folded(q))
            def _():
                with jax.named_scope("w_fin"):
                    fin_copy(q).wait_recv()
                rest = raw_y[:, cols].astype(jnp.float32)
                far_ret[:, cols] = (total + rest).astype(far_ret.dtype)


    with jax.named_scope("tail_sends"):
        table_y.wait_send()
        table_f.wait_send()
        sent(near_stage.at[0], near_ret, near_send.at[0])
        sent(x.at[near_j, s], near_ret, nr_send)
        for j in range(4):
            sent(x.at[j, pl.ds(0, 2)], pair.at[0], rp_send.at[j])
            part = pl.ds(0, width if j >= 2 else width - folds * tile)
            sent(x.at[j, cross_s, :, part], near_ret.at[:, part], ry_send.at[j])
        sent(near_cross, near_cross, nx_send)
        part = pl.ds(0, folds * tile)
        sent(raw.at[:, part], far_ret.at[:, part], fin_send)

        @pl.when(inner)
        def _():
            for i in range(2):
                sent(raw_f.at[i], far_ret, fr_send.at[i])

        @pl.when(outer)
        def _():
            sent(near_stage.at[1], near_ret, near_send.at[1])
            for i in range(2):
                sent(x.at[2 + i, s], near_ret, or_send.at[i])


def routed(tokens, route_ids, levels, w_gate, w_up, w_down, cap):
    tok_rows, width = tokens.shape
    ff, dtype = w_gate.shape[2], tokens.dtype
    rows, chunks = SHARDS * cap, width // tile_of(width, 1024)
    folds = chunks * 3 // 7
    dma, vmem = pltpu.SemaphoreType.DMA, pltpu.VMEM
    anywhere, local = pl.BlockSpec(memory_space=pl.ANY), pl.BlockSpec(memory_space=pltpu.VMEM)
    return pl.pallas_call(
        routed_kernel,
        out_shape=pltpu.VMEM((tok_rows, width), dtype),
        in_specs=[anywhere, local, local, anywhere, anywhere, anywhere],
        out_specs=local,
        scratch_shapes=[
            vmem((4, SHARDS, cap, width), dtype),
            vmem((width, ff), dtype),
            vmem((width, ff), dtype),
            vmem((ff, width), dtype),
            vmem((2, rows, ff), jnp.float32),
            vmem((2, rows, ff), dtype),
            vmem((2, 2, cap, width), dtype),
            vmem((2, cap, width), dtype),
            vmem((tok_rows, width), dtype),
            vmem((tok_rows, width), dtype),
            vmem((2, tok_rows, width), dtype),
            vmem((2, cap, width), dtype),
            vmem((cap, width), dtype),
            vmem((folds, cap, width // chunks), dtype),
            vmem((2, cap, width), dtype),
            vmem((4, 16, tok_rows), jnp.float32),
            vmem((4, 2 * cap, tok_rows), dtype),
            vmem((4, 2, tok_rows, 2 * cap), dtype),
            dma((3,)), dma, dma((2,)), dma((3,)),
            dma, dma((chunks,)), dma, dma((2, chunks)),
            dma((2,)), dma((2,)),
            dma((2,)), dma((2, chunks)),
            dma((2,)), dma((2, chunks)),
            dma((4, 2)), dma((4, 2)),
            dma((4,)), dma((2, chunks, 2)),
            dma((4,)), dma((2, chunks)),
            dma, dma((chunks,)),
            dma((2,)), dma((2, chunks)),
            dma((2,)), dma((chunks,)),
            dma, dma((folds,)), dma, dma((folds,)),
            pltpu.SemaphoreType.REGULAR, pltpu.SemaphoreType.REGULAR,
            pltpu.SemaphoreType.REGULAR,
        ],
        compiler_params=pltpu.CompilerParams(
            collective_id=0, has_side_effects=True, vmem_limit_bytes=65_200_000
        ),
    )(tokens, route_ids.T, levels.T, w_gate, w_up, w_down)


def combine_kernel(weight_ref, ret_ref, out_ref):
    weight = weight_ref[...]
    high = weight.astype(jnp.bfloat16)
    low = (weight - high.astype(jnp.float32)).astype(jnp.bfloat16)
    total = jnp.dot(high, ret_ref[...], preferred_element_type=jnp.float32)
    total += jnp.dot(low, ret_ref[...], preferred_element_type=jnp.float32)
    out_ref[...] = total.astype(out_ref.dtype)


def on_device(tokens, route_ids, levels, w_gate, w_up, w_down):
    tok_rows, width = tokens.shape
    top = route_ids.shape[1]
    ff = w_gate.shape[2]
    experts = lax.axis_size("expert") // SHARDS
    capacity = 5 * tok_rows * top // (4 * experts)
    cap = -(-capacity // 16) * 16
    slots = experts * cap
    dtype = tokens.dtype
    if experts == 4 and top == 2 and tok_rows < 2 * cap:
        return routed(tokens, route_ids, levels, w_gate, w_up, w_down, cap)

    chosen = route_ids[:, :, None] == jnp.arange(experts, dtype=jnp.int32)
    named = jnp.any(chosen, axis=1)
    index = jnp.arange(tok_rows, dtype=jnp.int32)
    earlier = (index[:, None] > index[None, :]).astype(jnp.bfloat16)
    rank = jnp.dot(earlier, named.astype(jnp.bfloat16), preferred_element_type=jnp.float32)
    place = jnp.where(named, rank.astype(jnp.int32), cap)
    level_f = levels.astype(jnp.float32)
    weights = level_f / jnp.sum(level_f, axis=1, keepdims=True)
    weight_e = jnp.sum(jnp.where(chosen, weights[:, :, None], 0.0), axis=1)
    spot = jnp.arange(cap, dtype=jnp.int32)
    pick = (place[:, :, None] == spot).reshape(tok_rows, slots)
    weight_m = jnp.where(pick, jnp.repeat(weight_e, cap, axis=1), 0.0)
    outgoing = lax.dot_general(
        pick.astype(dtype), tokens, (((0,), (0,)), ((), ())), preferred_element_type=jnp.float32
    ).astype(dtype).reshape(experts, cap, width)

    dma, anywhere = pltpu.SemaphoreType.DMA, pl.BlockSpec(memory_space=pl.ANY)
    rows, chunks = SHARDS * cap, width // tile_of(width, 1024)
    returned = pl.pallas_call(
        functools.partial(layer_kernel, experts),
        out_shape=jax.ShapeDtypeStruct((experts, cap, width), dtype),
        in_specs=[anywhere] * 4,
        out_specs=anywhere,
        scratch_shapes=[
            pltpu.VMEM((experts, SHARDS, cap, width), dtype),
            pltpu.VMEM((width, ff), dtype),
            pltpu.VMEM((width, ff), dtype),
            pltpu.VMEM((ff, width), dtype),
            pltpu.VMEM((2, rows, ff), jnp.float32),
            pltpu.VMEM((rows, ff), dtype),
            pltpu.VMEM((experts, 2, cap, width), dtype),
            pltpu.VMEM((experts, cap, width), dtype),
            dma((3,)),
            dma((experts,)), dma((experts,)),
            dma((experts,)), dma((experts,)),
            dma((experts, 2)), dma((experts, 2)),
            dma((experts, chunks, 2)), dma((experts, chunks, 2)),
            dma((experts, chunks)), dma((experts, chunks)),
            dma((experts, chunks)), dma((experts, chunks)),
        ],
        compiler_params=pltpu.CompilerParams(
            collective_id=0, has_side_effects=True, vmem_limit_bytes=67_000_000
        ),
    )(outgoing, w_gate, w_up, w_down)

    tile = tile_of(width, 1024)
    return pl.pallas_call(
        combine_kernel,
        out_shape=jax.ShapeDtypeStruct((tok_rows, width), dtype),
        grid=(width // tile,),
        in_specs=[
            pl.BlockSpec((tok_rows, slots), lambda n: (0, 0)),
            pl.BlockSpec((slots, tile), lambda n: (0, n)),
        ],
        out_specs=pl.BlockSpec((tok_rows, tile), lambda n: (0, n)),
    )(weight_m, returned.reshape(slots, width))


def solution(mesh):
    return jax.shard_map(
        on_device,
        mesh=mesh,
        in_specs=(
            P(("groups", "expert"), None),
            P(("groups", "expert"), None),
            P(("groups", "expert"), None),
            P("expert", None, None),
            P("expert", None, None),
            P("expert", None, None),
        ),
        out_specs=P(("groups", "expert"), None),
        check_vma=False,
    )
```
